32 devices in a mesh: ctx: 8 (over z, x), dp: 4 (over y, core).
Axes of the slice: x: 2, y: 2, z: 4, core: 2. Of those that a mesh axis runs over, the one named last changes fastest.
Arguments:
- head_input: bfloat16 [8192, 4096], P(('dp', 'ctx')), parts along dimension 0, may hold values from -6 to 6
- gate_input: bfloat16 [8192, 4096], P(('dp', 'ctx')), parts along dimension 0, may hold values from -6 to 6
- write_vector: bfloat16 [8192, 128], P(('dp', 'ctx')), parts along dimension 0, may hold values from -2.5 to 2.5
- read_vector: bfloat16 [8192, 128], P(('dp', 'ctx')), parts along dimension 0, may hold values from -2.5 to 2.5
- increment_preactivation: bfloat16 [8192, 64], P(('dp', 'ctx')), parts along dimension 0, may hold values from -2 to 8
- step_bias: float32 [64], replicated, may hold values from -1 to 0.5
- decay_log: float32 [64], replicated, may hold values from -9.3 to -2.3
- skip_gain: float32 [64], replicated, may hold values from 0.5 to 1.5
- norm_weight: float32 [4096], replicated, may hold values from 0.5 to 1.5
- doc_starts: int32 [64], P(('dp', 'ctx')), parts along dimension 0, may hold values from 0 to 1, as said below
- block_order: int32 [64], P(('dp', 'ctx')), parts along dimension 0, may hold values from 0 to 15, as said below
Outputs:
- packed_out: bfloat16 [8192, 4096], P(('dp', 'ctx')), parts along dimension 0
The draws below stay inside these ranges and needn't reach their ends.
There are 4 independent parts, one for each index of `dp`. The reference program is written for one: setup_inputs(seed, part) draws one part's arguments, and reference() takes and returns one part's arrays. A program takes and returns all parts, laid end to end along the dimension named above; an argument that names none is the same for every part. Nothing has to cross between parts.
Inputs may be any that keep to these rules, and one draw needn't show every extreme that they name: `doc_starts`: block 0 starts a document; no document is longer than 128 blocks. `block_order`: a permutation of the block indices that keeps each document's blocks together and in their order.
All inputs are finite; a program needn't handle non-finite values.
Results may differ from the reference program's by a relative error of at most 0.0085.
Values may be sent and summed in bfloat16 or wider, within the bound.
A program may use at most 128 MiB of HBM per device.

```python
import math
import jax
import jax.numpy as jnp
from jax import lax

HEADS = 64
HEAD_DIM = 64
STATE = 128
GROUP = 128
DOC_MOST = 128
JOINED_TERMS = 2048


def doc_tables(key):
    key_baseline = jax.random.fold_in(key, 7)
    key_start, key_rank, key_extra = jax.random.split(key_baseline, 3)
    block_count = JOINED_TERMS // GROUP
    positions = jnp.arange(block_count, dtype=jnp.int32)
    chosen = jax.random.randint(key_start, (block_count,), 0, 64) == 0
    extra_at = jax.random.randint(key_extra, (4,), 1, block_count)
    hit_extra = jnp.any(positions[:, None] == extra_at[None, :], axis=1)
    forced = jnp.logical_or(positions % DOC_MOST == 0, hit_extra)
    starts = jnp.logical_or(chosen, forced).astype(jnp.int32)
    segment_number = jnp.cumsum(starts) - 1
    ranks = jax.random.randint(key_rank, (block_count,), 0, 1 << 20)
    priority = ranks[segment_number] * block_count + positions
    permuted = jnp.argsort(priority, stable=True).astype(jnp.int32)
    return (starts, permuted)


def draw_doc_starts(key, part):
    return doc_tables(key)[0]


def draw_block_order(key, part):
    return doc_tables(key)[1]


def draw_increment_preactivation(key, part):
    key_baseline = jax.random.fold_in(key, 11)
    key_value_product, lookup_jump = jax.random.split(key_baseline)
    spike_series = (jax.random.randint(lookup_jump, (JOINED_TERMS, 1), 0, 64) == 0).astype(jnp.float32)
    payload_reference_level = jnp.clip(0.5 * jax.random.normal(key_value_product, (JOINED_TERMS, HEADS), jnp.float32), -2.0, 2.0)
    return (payload_reference_level + 6.0 * spike_series).astype(jnp.bfloat16)


def draw_decay_log(key, part):
    key_baseline = jax.random.fold_in(key, 13)
    return jax.random.uniform(key_baseline, (HEADS,), jnp.float32, math.log(0.0003), math.log(0.1))


def levels(own_key, dims, shards, low, largest):
    gain = 1.0
    for axis_at, blocks in shards:
        steps = jax.random.uniform(jax.random.fold_in(jax.random.fold_in(own_key, 6), axis_at), (blocks,), jnp.float32, low / len(shards), largest / len(shards))
        gain = gain * jnp.repeat(jnp.exp(steps), dims[axis_at] // blocks).reshape((-1,) + (1,) * (len(dims) - 1 - axis_at))
    return gain


def noise(stream_key, extent, scale, reach, cuts=(), kind=jnp.bfloat16):
    entries = scale * jax.random.normal(stream_key, extent, jnp.float32)
    if cuts:
        entries = entries * levels(stream_key, extent, cuts, -0.22, 0.18)
    return jnp.clip(entries, -reach, reach).astype(kind)


def setup_inputs(seed: int = 0, part: int = 0) -> dict:
    streams_of = jax.random.split(jax.random.key(seed), 12)
    part_keys = jax.random.split(jax.random.fold_in(streams_of[11], part), 12)
    return {
        "head_input": noise(part_keys[0], (JOINED_TERMS, HEADS * HEAD_DIM), 1.0, 6.0, ((0, 8),)),
        "gate_input": noise(part_keys[1], (JOINED_TERMS, HEADS * HEAD_DIM), 1.0, 6.0, ((0, 8),)),
        "write_vector": noise(part_keys[2], (JOINED_TERMS, STATE), 0.3, 2.5, ((0, 8),)),
        "read_vector": noise(part_keys[3], (JOINED_TERMS, STATE), 0.3, 2.5, ((0, 8),)),
        "increment_preactivation": draw_increment_preactivation(jax.random.fold_in(jax.random.fold_in(streams_of[11], part), 71), part),
        "step_bias": jnp.clip(jax.random.uniform(streams_of[5], (HEADS,), jnp.float32, -1.0, 0.5), -1.0, 0.5),
        "decay_log": draw_decay_log(jax.random.fold_in(streams_of[11], 71), part),
        "skip_gain": jnp.clip(jax.random.uniform(streams_of[7], (HEADS,), jnp.float32, 0.5, 1.5), 0.5, 1.5),
        "norm_weight": jnp.clip(1.0 + 0.1 * jax.random.normal(streams_of[8], (HEADS * HEAD_DIM,), jnp.float32), 0.5, 1.5),
        "doc_starts": draw_doc_starts(jax.random.fold_in(jax.random.fold_in(streams_of[11], part), 71), part),
        "block_order": draw_block_order(jax.random.fold_in(jax.random.fold_in(streams_of[11], part), 71), part),
    }


highest = lax.Precision.HIGHEST

def product(form, left, right):
    return jnp.einsum(form, left.astype(jnp.float32), right.astype(jnp.float32), precision=highest)

def link_maps(earlier, current):
    decay_one, state_one = earlier
    decay_two, state_two = current
    return (decay_one * decay_two, decay_two[..., None, None] * state_one + state_two)

def group_terms(inputs, step_size, decay_speed, scores, write_vector, keep_mask, group_size):
    length, local_heads, head_width = inputs.shape
    group_count = length // group_size
    blocked = inputs.reshape(group_count, group_size, local_heads, head_width)
    steps_blocked = step_size.reshape(group_count, group_size, local_heads).transpose(0, 2, 1)
    cumulative = jnp.cumsum(-steps_blocked * decay_speed[None, :, None], axis=2)
    row_labels = lax.broadcasted_iota(jnp.int32, (group_size, group_size), 0)
    col_ids = lax.broadcasted_iota(jnp.int32, (group_size, group_size), 1)
    gap_log = cumulative[:, :, :, None] - cumulative[:, :, None, :]
    decays = jnp.exp(jnp.where(row_labels >= col_ids, gap_log, -jnp.inf))
    weight = (scores[:, None, :, :] * decays * steps_blocked[:, :, None, :]).astype(jnp.bfloat16)
    local_out = product('chij,cjhp->cihp', weight, blocked)
    last_cum = cumulative[:, :, -1]
    tail_decay = jnp.exp(last_cum[:, :, None] - cumulative) * steps_blocked
    scaled = (blocked.astype(jnp.float32) * tail_decay.transpose(0, 2, 1)[..., None]).astype(jnp.bfloat16)
    write_blocked = write_vector.reshape(group_count, group_size, -1)
    states = product('cjhp,cjn->chpn', scaled, write_blocked)
    factor = jnp.exp(last_cum) * keep_mask[:, None]
    scan_decay, scan_state = lax.associative_scan(link_maps, (factor, states))
    return (local_out, cumulative, scan_decay, scan_state)

def finish_groups(local_out, cumulative, scan_decay, scan_state, keep_mask, read_vector, starting_entry, inputs, skip_gain):
    group_count, group_size, local_heads, head_width = local_out.shape
    prior_decay = jnp.concatenate([jnp.ones((1, local_heads), jnp.float32), scan_decay[:-1]], 0)
    prior_state = jnp.concatenate([jnp.zeros((1,) + scan_state.shape[1:], jnp.float32), scan_state[:-1]], 0)
    entering = keep_mask[:, None, None, None] * (prior_decay[:, :, None, None] * starting_entry[None] + prior_state)
    read_blocked = read_vector.reshape(group_count, group_size, -1)
    carried = product('cin,chpn->cihp', read_blocked, entering)
    carried = carried * jnp.exp(cumulative).transpose(0, 2, 1)[..., None]
    blocked = inputs.reshape(local_out.shape).astype(jnp.float32)
    result = local_out + carried + skip_gain[None, None, :, None] * blocked
    return result.reshape(group_count * group_size, local_heads * head_width)

def gated_norm(gated, norm_weight):
    values = gated.astype(jnp.float32)
    mean_square = lax.optimization_barrier(jnp.mean(values * values, axis=-1, keepdims=True))
    return (values * lax.rsqrt(mean_square + 1e-05) * norm_weight).astype(jnp.bfloat16)

def reference(head_input, gate_input, write_vector, read_vector, increment_preactivation, step_bias, decay_log, skip_gain, norm_weight, doc_starts, block_order):
    step_size = jax.nn.softplus(increment_preactivation.astype(jnp.float32) + step_bias)
    decay_speed = jnp.exp(decay_log)
    keep_mask = 1.0 - doc_starts.astype(jnp.float32)
    group_count = JOINED_TERMS // GROUP
    scores = product('cin,cjn->cij', read_vector.reshape(group_count, GROUP, -1), write_vector.reshape(group_count, GROUP, -1))
    per_head = head_input.reshape(JOINED_TERMS, HEADS, HEAD_DIM).transpose(1, 0, 2)[:, :, None, :]

    def one_head(pieces):
        inputs, head_steps, attention_forgetting, head_gain = pieces
        local_out, cumulative, scan_decay, scan_state = group_terms(inputs, head_steps[:, None], attention_forgetting[None], scores, write_vector, keep_mask, GROUP)
        starting_entry = jnp.zeros((1, HEAD_DIM, STATE), jnp.float32)
        return finish_groups(local_out, cumulative, scan_decay, scan_state, keep_mask, read_vector, starting_entry, inputs, head_gain[None])
    outputs = lax.map(one_head, (per_head, step_size.T, decay_speed, skip_gain))
    combined = outputs.transpose(1, 0, 2).reshape(JOINED_TERMS, HEADS * HEAD_DIM)
    gated = (combined * jax.nn.silu(gate_input.astype(jnp.float32))).astype(jnp.bfloat16)
    normed = gated_norm(gated, norm_weight)
    return normed.reshape(group_count, GROUP, -1)[block_order].reshape(JOINED_TERMS, HEADS * HEAD_DIM)
```

```python
import functools

import jax
import jax.numpy as jnp
from jax import lax
from jax.experimental import pallas as pl
from jax.experimental.pallas import tpu as pltpu
from jax.sharding import PartitionSpec as P

HEAD_DIM = 64
GROUP = 128
CHUNK = 8
WIDE = CHUNK * HEAD_DIM
EXTRA = 16
PARTS = 4

highest = lax.Precision.HIGHEST
VM = pl.BlockSpec(memory_space=pltpu.VMEM)
SM = pl.BlockSpec(memory_space=pltpu.SMEM)
ANY = pl.BlockSpec(memory_space=pl.ANY)


def transposed(v):
    rows, cols = v.shape
    if cols < 128:
        v = jnp.concatenate([v, jnp.zeros((rows, 128 - cols), v.dtype)], axis=1)
    return v.T[:cols]


def upright(v):
    rows, cols = v.shape
    if rows < 128:
        v = jnp.concatenate([v, jnp.zeros((128 - rows, cols), v.dtype)], axis=0)
    return v.T[:, :rows]


def lower_mask():
    row = lax.broadcasted_iota(jnp.int32, (GROUP, GROUP), 0)
    col = lax.broadcasted_iota(jnp.int32, (GROUP, GROUP), 1)
    return row >= col


def step_terms(logit_ref, bias_ref, dlog_ref):
    raw = logit_ref[...].astype(jnp.float32)
    raw = jnp.concatenate([upright(raw[:, k : k + GROUP]) for k in range(0, raw.shape[1], GROUP)], axis=0)
    v = raw + bias_ref[...]
    dt = jnp.maximum(v, 0.0) + jnp.log(1.0 + jnp.exp(-jnp.abs(v)))
    return dt, -dt * jnp.exp(dlog_ref[...])


def spread(v):
    rows = v.shape[0]
    first = lax.broadcasted_iota(jnp.int32, (rows, 128), 1) < HEAD_DIM
    return jnp.concatenate(
        [
            jnp.where(first, v[:, k : k + 1], v[:, k + 1 : k + 2])
            for k in range(0, CHUNK, 2)
        ],
        axis=1,
    )


def prepare(logit_ref, bias_ref, dlog_ref, write_ref, cum_s, dt_s, write_t):
    heads = bias_ref.shape[1]
    dt, fall = step_terms(logit_ref, bias_ref, dlog_ref)
    tri = lower_mask().astype(jnp.float32)
    cums = []
    for g in range(write_t.shape[0]):
        rows = slice(g * GROUP, (g + 1) * GROUP)
        cum = jnp.dot(tri, fall[rows], precision=highest, preferred_element_type=jnp.float32)
        cums.append(cum)
        for c in range(heads // CHUNK):
            cum_s[g, c] = cum[:, c * CHUNK : (c + 1) * CHUNK]
            dt_s[g, c] = dt[rows, c * CHUNK : (c + 1) * CHUNK]
        write_t[g] = write_ref[rows, :].astype(jnp.float32).T.astype(jnp.bfloat16)
    return dt, cums


def group_state(g, c, x, cum_s, dt_s, write_t):
    cum = cum_s[g, c]
    last = cum[GROUP - 1 : GROUP]
    tail = jnp.exp(last - cum) * dt_s[g, c]
    scaled = (x.astype(jnp.float32) * spread(tail)).astype(jnp.bfloat16)
    state = jnp.dot(write_t[g], scaled, preferred_element_type=jnp.float32)
    return state, spread(jnp.exp(last))


def state_kernel(
    x_ref, logit_ref, write_ref, bias_ref, dlog_ref, starts_ref, order_ref, out_ref, cum_s, dt_s, write_t
):
    groups = write_t.shape[0]
    prepare(logit_ref, bias_ref, dlog_ref, write_ref, cum_s, dt_s, write_t)
    parts, _, width = out_ref.shape
    chunks = cum_s.shape[1]
    per = width // WIDE

    def one(c, carry):
        cols = pl.ds(pl.multiple_of(c * WIDE, WIDE), WIDE)
        total, decay = None, None
        for g in range(groups):
            x = x_ref[g * GROUP : (g + 1) * GROUP, cols]
            state, last = group_state(g, c, x, cum_s, dt_s, write_t)
            keep = 1.0 - starts_ref[g].astype(jnp.float32)
            factor = keep * last
            total = state if total is None else factor * total + state
            decay = factor if decay is None else factor * decay
        coarse = decay.astype(jnp.bfloat16)
        fine = (decay - coarse.astype(jnp.float32)).astype(jnp.bfloat16)
        row = lax.broadcasted_iota(jnp.int32, (EXTRA, WIDE), 0)
        lane = lax.broadcasted_iota(jnp.int32, (EXTRA, WIDE), 1)
        order = jnp.zeros((EXTRA, WIDE), jnp.float32)
        for g in range(groups):
            order = jnp.where(lane == g, order_ref[g].astype(jnp.float32), order)
        extra = jnp.where(
            row == 0,
            coarse.astype(jnp.float32),
            jnp.where(row == 1, fine.astype(jnp.float32), order),
        )
        full = jnp.concatenate([total, extra], axis=0).astype(jnp.bfloat16)
        if parts == 1:
            out_ref[0, :, cols] = full
        else:
            into = pl.ds(pl.multiple_of((c % per) * WIDE, WIDE), WIDE)
            out_ref[c // per, :, into] = full
        return carry

    lax.fori_loop(0, chunks, one, 0)


def scan_kernel(in_ref, out_ref):
    parts, _, width = in_ref.shape
    state = jnp.zeros((GROUP, width), jnp.float32)
    for s in range(parts):
        out_ref[s] = state.astype(jnp.bfloat16)
        extra = in_ref[s, GROUP : GROUP + EXTRA, :].astype(jnp.float32)
        decay = extra[0:1] + extra[1:2]
        state = decay * state + in_ref[s, :GROUP, :].astype(jnp.float32)


def gated_setup(
    logit_ref, bias_ref, dlog_ref, write_ref, read_ref, gain_ref, cum_s, dt_s, write_t, cum_t, dt_t, gain_s, score_s
):
    groups, chunks = cum_s.shape[:2]
    dt, cums = prepare(logit_ref, bias_ref, dlog_ref, write_ref, cum_s, dt_s, write_t)
    mask = lower_mask()
    for g in range(groups):
        rows = slice(g * GROUP, (g + 1) * GROUP)
        ct = transposed(cums[g])
        dtt = transposed(dt[rows])
        for c in range(chunks):
            cum_t[g, c] = ct[c * CHUNK : (c + 1) * CHUNK]
            dt_t[g, c] = dtt[c * CHUNK : (c + 1) * CHUNK]
        score = jnp.dot(read_ref[rows, :], write_t[g], preferred_element_type=jnp.float32)
        score_s[g] = jnp.where(mask, score, 0.0)
    for c in range(chunks):
        gain_s[c] = jnp.broadcast_to(gain_ref[:, c * CHUNK : (c + 1) * CHUNK], (8, CHUNK))


def gated_chunk(
    c, state, put, x_ref, gate_ref, read_ref, starts_ref, cum_s, dt_s, write_t, cum_t, dt_t, gain_s, score_s
):
    groups = cum_s.shape[0]
    first = lax.broadcasted_iota(jnp.int32, (GROUP, 128), 1) < HEAD_DIM
    cols = pl.ds(pl.multiple_of(c * WIDE, WIDE), WIDE)
    gain = spread(gain_s[c][0:1])
    for g in range(groups):
        rows = slice(g * GROUP, (g + 1) * GROUP)
        x = x_ref[rows, cols]
        keep = 1.0 - starts_ref[g].astype(jnp.float32)
        entering = (keep * state).astype(jnp.bfloat16)
        cum = cum_s[g, c]
        carried = jnp.dot(read_ref[rows, :], entering, preferred_element_type=jnp.float32)
        mixed = carried * spread(jnp.exp(cum)) + gain * x.astype(jnp.float32)
        score = score_s[g]
        ct, dtt = cum_t[g, c], dt_t[g, c]
        pieces = []
        for k in range(0, CHUNK, 2):
            pair = x[:, k * HEAD_DIM : (k + 2) * HEAD_DIM]
            both = []
            for h in (k, k + 1):
                gap = cum[:, h : h + 1] - ct[h : h + 1]
                weight = score * jnp.exp(jnp.minimum(gap, 0.0)) * dtt[h : h + 1]
                both.append(
                    jnp.dot(weight.astype(jnp.bfloat16), pair, preferred_element_type=jnp.float32)
                )
            pieces.append(jnp.where(first, both[0], both[1]))
        mixed = mixed + jnp.concatenate(pieces, axis=1)
        gate = gate_ref[rows, cols].astype(jnp.float32)
        put(g, (mixed * (gate / (1.0 + jnp.exp(-gate)))).astype(jnp.bfloat16))
        if g + 1 < groups:
            own, last = group_state(g, c, x, cum_s, dt_s, write_t)
            state = keep * last * state + own


def gated_kernel(
    x_ref,
    gate_ref,
    logit_ref,
    write_ref,
    read_ref,
    entry_ref,
    bias_ref,
    dlog_ref,
    gain_ref,
    starts_ref,
    out_ref,
    *scratch,
):
    gated_setup(logit_ref, bias_ref, dlog_ref, write_ref, read_ref, gain_ref, *scratch)
    parts, _, width = out_ref.shape
    chunks = scratch[0].shape[1]
    per = width // WIDE

    def one(c, carry):
        cols = pl.ds(pl.multiple_of(c * WIDE, WIDE), WIDE)
        into = pl.ds(pl.multiple_of((c % per) * WIDE, WIDE), WIDE)
        if parts == 1:
            state = entry_ref[0, :, cols].astype(jnp.float32)
        else:
            state = entry_ref[c // per, :, into].astype(jnp.float32)

        def put(g, value):
            rows = slice(g * GROUP, (g + 1) * GROUP)
            if parts == 1:
                out_ref[0, rows, cols] = value
            else:
                out_ref[c // per, rows, into] = value

        gated_chunk(c, state, put, x_ref, gate_ref, read_ref, starts_ref, *scratch)
        return carry

    lax.fori_loop(0, chunks, one, 0)


def fused_kernel(
    n,
    parts,
    x_hbm,
    gate_hbm,
    logit_ref,
    write_ref,
    read_ref,
    bias_ref,
    dlog_ref,
    gain_ref,
    weight_ref,
    starts_ref,
    order_ref,
    out_ref,
    x_ref,
    gate_ref,
    pair_out,
    pair_in,
    total_s,
    decay_s,
    e_in,
    f_out,
    back,
    entry,
    made,
    stage,
    final,
    squares,
    order_own,
    order_all,
    order_s,
    load_sem,
    pair_send,
    pair_recv,
    chain_send,
    chain_recv,
    back_send,
    back_recv,
    send1,
    recv1,
    send2,
    recv2,
    send3,
    recv3,
    order_sem,
    *rest,
):
    got, scratch = rest[:parts], rest[parts:]
    cum_s, dt_s, write_t = scratch[:3]
    groups, chunks = cum_s.shape[:2]
    piece = stage.shape[-1]
    per = WIDE // piece
    steps = chunks // parts
    state_size = write_t.shape[1]
    me = lax.axis_index("ctx")
    side = me % 2
    level = me // 2
    levels = n // 2
    buddy = me + 1 - 2 * side
    half = n // 2
    mine = (me // half) * half
    other = half - mine
    span = chunks // parts * WIDE

    def partner(k):
        far = 1 - k % 2
        return far * other + (1 - far) * mine + lax.rem(me + k // 2, half)

    def send(source, target, sends, recvs, there):
        return pltpu.make_async_remote_copy(
            src_ref=source,
            dst_ref=target,
            send_sem=sends,
            recv_sem=recvs,
            device_id={"ctx": there},
            device_id_type=pl.DeviceIdType.MESH,
        )

    def load(which, j):
        cols = pl.ds(j * span, span)
        source, target = ((x_hbm, x_ref), (gate_hbm, gate_ref))[which]
        return pltpu.make_async_copy(source.at[:, cols], target.at[:, cols], load_sem.at[which, j])

    def pair(c):
        return send(pair_out.at[c], pair_in.at[c], pair_send.at[c], pair_recv.at[c], buddy)

    def chain(c):
        return send(f_out.at[c], e_in.at[c], chain_send.at[c], chain_recv.at[c], lax.rem(me + 2, n))

    def give(c):
        return send(back.at[c], entry.at[c], back_send.at[c], back_recv.at[c], buddy)

    def order_to(there, slot):
        return send(order_own, order_all.at[slot], send3.at[there], recv3.at[slot], there)

    def first(there, slot, j):
        return send(
            made.at[there, j],
            got[j].at[pl.ds(slot * groups, groups)],
            send1.at[there, j],
            recv1.at[slot, j],
            there,
        )

    def second(there, slot, j):
        return send(stage.at[there, j], final.at[slot, j], send2.at[there, j], recv2.at[slot, j], there)

    for j in range(parts):
        load(0, j).start()
    for j in range(parts):
        load(1, j).start()
    barrier = pltpu.get_barrier_semaphore()
    for off in range(1, n):
        pl.semaphore_signal(
            barrier, inc=1, device_id={"ctx": lax.rem(me + off, n)}, device_id_type=pl.DeviceIdType.MESH
        )
    lane = lax.broadcasted_iota(jnp.int32, order_own.shape, 1)
    held = jnp.zeros(order_own.shape, jnp.int32)
    for g in range(groups):
        held = jnp.where(lane == g, order_ref[g], held)
    order_own[...] = held
    order_all[me] = held
    gated_setup(logit_ref, bias_ref, dlog_ref, write_ref, read_ref, gain_ref, *scratch)

    @pl.when(level == 0)
    def _():
        e_in[...] = jnp.zeros_like(e_in)

    pl.semaphore_wait(barrier, n - 1)

    def ends(c, carry):
        cols = pl.ds(pl.multiple_of(c * WIDE, WIDE), WIDE)
        total, decay = None, None
        for g in range(groups):
            x = x_ref[g * GROUP : (g + 1) * GROUP, cols]
            state, last = group_state(g, c, x, cum_s, dt_s, write_t)
            factor = (1.0 - starts_ref[g].astype(jnp.float32)) * last
            total = state if total is None else factor * total + state
            decay = factor if decay is None else factor * decay
        total_s[c] = total
        decay_s[c] = jnp.broadcast_to(decay, (8, WIDE))

        @pl.when(c % 2 != side)
        def _():
            coarse = decay.astype(jnp.bfloat16).astype(jnp.float32)
            row = lax.broadcasted_iota(jnp.int32, (EXTRA, WIDE), 0)
            extra = jnp.where(row == 0, coarse, decay - coarse)
            pair_out[c] = jnp.concatenate([total, extra], axis=0).astype(jnp.bfloat16)
            pair(c).start()

        return carry

    for j in range(parts):
        load(0, j).wait()
        lax.fori_loop(j * steps, (j + 1) * steps, ends, 0)
    for off in range(1, n):
        order_to(lax.rem(me + off, n), me).start()

    def relay(c):
        pair(c).wait_recv()

        @pl.when(level > 0)
        def _():
            chain(c).wait_recv()

        state = e_in[c].astype(jnp.float32)
        their = pair_in[c, :state_size].astype(jnp.float32)
        tail = pair_in[c, state_size : state_size + EXTRA].astype(jnp.float32)
        fade = tail[0:1] + tail[1:2]
        total, decay = total_s[c], decay_s[c][0:1]
        early = side == 0
        middle = jnp.where(early, decay, fade) * state + jnp.where(early, total, their)

        @pl.when(level < levels - 1)
        def _():
            end = jnp.where(early, fade, decay) * middle + jnp.where(early, their, total)
            f_out[c] = end.astype(jnp.bfloat16)
            chain(c).start()

        back[c] = jnp.where(early, middle, state).astype(jnp.bfloat16)
        give(c).start()
        entry[c] = jnp.where(early, state, middle).astype(jnp.bfloat16)

    def part(j, carry):
        def links(i, inner):
            relay(j * steps + 2 * i + side)
            return inner

        lax.fori_loop(0, steps // 2, links, 0)
        for s in range(parts):

            @pl.when(j == s)
            def _():
                load(1, s).wait()

        def one(t, inner):
            i = lax.rem(t + me, steps)
            c = j * steps + i

            @pl.when(c % 2 != side)
            def _():
                give(c).wait_recv()

            def put(g, value):
                for p in range(per):
                    made[p * steps + i, j, g] = value[:, p * piece : (p + 1) * piece]

            gated_chunk(
                c, entry[c].astype(jnp.float32), put, x_ref, gate_ref, read_ref, starts_ref, *scratch
            )
            for p in range(per):
                there = p * steps + i
                for s in range(parts):

                    @pl.when(jnp.logical_and(j == s, there != me))
                    def _():
                        first(there, me, s).start()

                    @pl.when(jnp.logical_and(j == s, there == me))
                    def _():
                        for g in range(groups):
                            got[s][me * groups + g] = made[there, s, g]

            return inner

        lax.fori_loop(0, steps, one, 0)
        return carry

    lax.fori_loop(0, parts, part, 0)
    for off in range(1, n):
        there = lax.rem(me + off, n)
        order_to(there, there).wait_recv()
    fetch = pltpu.make_async_copy(order_all, order_s, order_sem)
    fetch.start()
    fetch.wait()
    for j in range(parts):
        for off in range(1, n):
            there = lax.rem(me + off, n)
            first(there, there, j).wait_recv()

        def pick(k, carry, j=j):
            there = partner(k)

            @pl.when(there != me)
            def _():
                for g in range(groups):
                    stage[there, j, g] = got[j][order_s[there, 0, g]]
                second(there, me, j).start()

            @pl.when(there == me)
            def _():
                for g in range(groups):
                    final[me, j, g] = got[j][order_s[me, 0, g]]

            return carry

        lax.fori_loop(0, n, pick, 0)
    squares[...] = jnp.zeros_like(squares)
    tile = 32
    for j in range(parts):
        for off in range(1, n):
            there = lax.rem(me + off, n)
            second(there, there, j).wait_recv()
        for g in range(groups):

            def add(r, carry, j=j, g=g):
                at = pl.ds(pl.multiple_of(r * tile, tile), tile)
                total = squares[g, at, :]
                for s in range(n):
                    v = final[s, j, g, at, :].astype(jnp.float32)
                    v = v * v
                    for q in range(0, piece, 128):
                        total = total + v[:, q : q + 128]
                squares[g, at, :] = total
                return carry

            lax.fori_loop(0, GROUP // tile, add, 0)
    for g in range(groups):

        def norm(r, carry, g=g):
            at = pl.ds(pl.multiple_of(r * tile, tile), tile)
            into = pl.ds(pl.multiple_of(g * GROUP + r * tile, tile), tile)
            total = jnp.sum(squares[g, at, :], axis=1, keepdims=True)
            scale = lax.rsqrt(total * (1.0 / out_ref.shape[1]) + 1e-05)
            for j in range(parts):
                for s in range(n):
                    v = final[s, j, g, at, :].astype(jnp.float32)
                    low = (j * steps + s % steps) * WIDE + s // steps * piece
                    w = weight_ref[:, low : low + piece]
                    out_ref[into, low : low + piece] = (v * scale * w).astype(jnp.bfloat16)
            return carry

        lax.fori_loop(0, GROUP // tile, norm, 0)

    def settle(c, carry):
        @pl.when(c % 2 != side)
        def _():
            pair(c).wait_send()

        @pl.when(c % 2 == side)
        def _():
            give(c).wait_send()

            @pl.when(level < levels - 1)
            def _():
                chain(c).wait_send()

        return carry

    lax.fori_loop(0, chunks, settle, 0)
    for off in range(1, n):
        there = lax.rem(me + off, n)
        order_to(there, there).wait_send()
        for j in range(parts):
            first(there, there, j).wait_send()
            second(there, there, j).wait_send()


def norm_kernel(in_ref, weight_ref, out_ref):
    parts, rows, width = in_ref.shape
    tile = 32

    def one(r, carry):
        at = pl.ds(pl.multiple_of(r * tile, tile), tile)
        total = jnp.zeros((tile, 1), jnp.float32)
        for s in range(parts):
            v = in_ref[s, at, :].astype(jnp.float32)
            total = total + jnp.sum(v * v, axis=1, keepdims=True)
        scale = lax.rsqrt(total * (1.0 / (parts * width)) + 1e-05)
        for s in range(parts):
            v = in_ref[s, at, :].astype(jnp.float32)
            w = weight_ref[:, s * width : (s + 1) * width]
            out_ref[at, s * width : (s + 1) * width] = (v * scale * w).astype(jnp.bfloat16)
        return carry

    lax.fori_loop(0, rows // tile, one, 0)


def local(
    head_input,
    gate_input,
    write_vector,
    read_vector,
    increment_preactivation,
    step_bias,
    decay_log,
    skip_gain,
    norm_weight,
    doc_starts,
    block_order,
):
    devices = lax.axis_size("ctx")
    rows, features = head_input.shape
    heads = step_bias.shape[0]
    groups = rows // GROUP
    chunks = heads // CHUNK
    width = features // devices
    state_size = write_vector.shape[1]
    direct = width % WIDE == 0
    parts = devices if direct else 1
    limit = pltpu.CompilerParams(vmem_limit_bytes=48 * 1024 * 1024)
    common = [
        pltpu.VMEM((groups, chunks, GROUP, CHUNK), jnp.float32),
        pltpu.VMEM((groups, chunks, GROUP, CHUNK), jnp.float32),
        pltpu.VMEM((groups, state_size, GROUP), jnp.bfloat16),
    ]
    more = [
        pltpu.VMEM((groups, chunks, CHUNK, GROUP), jnp.float32),
        pltpu.VMEM((groups, chunks, CHUNK, GROUP), jnp.float32),
        pltpu.VMEM((chunks, 8, CHUNK), jnp.float32),
        pltpu.VMEM((groups, GROUP, GROUP), jnp.float32),
    ]
    bias, dlog, gain = (v.reshape(1, -1) for v in (step_bias, decay_log, skip_gain))

    def to_owners(v):
        if not direct:
            v = v.reshape(v.shape[1], devices, width).transpose(1, 0, 2)
        return lax.all_to_all(v, "ctx", split_axis=0, concat_axis=0, tiled=True)

    def joined(v):
        if not direct:
            v = v.transpose(1, 0, 2).reshape(1, v.shape[1], features)
        return v

    piece = width // PARTS
    per = max(WIDE // max(piece, 1), 1)
    if width == 512 and devices % (2 * per) == 0:
        slab = (devices, PARTS, groups, GROUP, piece)
        state = (chunks, state_size, WIDE)
        sems = pltpu.SemaphoreType.DMA
        return pl.pallas_call(
            functools.partial(fused_kernel, devices, PARTS),
            out_shape=jax.ShapeDtypeStruct((rows, features), jnp.bfloat16),
            in_specs=[ANY] * 2 + [VM] * 7 + [SM] * 2,
            out_specs=VM,
            scratch_shapes=[
                pltpu.VMEM((rows, features), jnp.bfloat16),
                pltpu.VMEM((rows, features), jnp.bfloat16),
                pltpu.VMEM((chunks, state_size + EXTRA, WIDE), jnp.bfloat16),
                pltpu.VMEM((chunks, state_size + EXTRA, WIDE), jnp.bfloat16),
                pltpu.VMEM(state, jnp.float32),
                pltpu.VMEM((chunks, 8, WIDE), jnp.float32),
                pltpu.VMEM(state, jnp.bfloat16),
                pltpu.VMEM(state, jnp.bfloat16),
                pltpu.VMEM(state, jnp.bfloat16),
                pltpu.VMEM(state, jnp.bfloat16),
                pltpu.VMEM(slab, jnp.bfloat16),
                pltpu.VMEM(slab, jnp.bfloat16),
                pltpu.VMEM(slab, jnp.bfloat16),
                pltpu.VMEM((groups, GROUP, 128), jnp.float32),
                pltpu.VMEM((8, 128), jnp.int32),
                pltpu.VMEM((devices, 8, 128), jnp.int32),
                pltpu.SMEM((devices, 8, 128), jnp.int32),
                sems((2, PARTS)),
            ]
            + [sems((chunks,))] * 6
            + [sems((devices, PARTS))] * 4
            + [sems((devices,))] * 2
            + [sems]
            + [pltpu.VMEM((devices * groups, GROUP, piece), jnp.bfloat16)] * PARTS
            + common
            + more,
            compiler_params=pltpu.CompilerParams(
                collective_id=0, has_side_effects=True, vmem_limit_bytes=60 * 1024 * 1024
            ),
            name="fused",
        )(
            head_input,
            gate_input,
            increment_preactivation.T,
            write_vector,
            read_vector,
            bias,
            dlog,
            gain,
            norm_weight.reshape(1, -1),
            doc_starts,
            block_order,
        )

    ends = pl.pallas_call(
        state_kernel,
        out_shape=jax.ShapeDtypeStruct((parts, state_size + EXTRA, features // parts), jnp.bfloat16),
        in_specs=[VM] * 5 + [SM] * 2,
        out_specs=VM,
        scratch_shapes=common,
        compiler_params=limit,
        name="end_states",
    )(head_input, increment_preactivation.T, write_vector, bias, dlog, doc_starts, block_order)
    ends = to_owners(ends)
    all_order = ends[:, state_size + 2, :groups].astype(jnp.int32).reshape(-1)
    entry = pl.pallas_call(
        scan_kernel,
        out_shape=jax.ShapeDtypeStruct((devices, state_size, width), jnp.bfloat16),
        in_specs=[VM],
        out_specs=VM,
        compiler_params=limit,
        name="scan_states",
    )(ends)
    entry = joined(lax.all_to_all(entry, "ctx", split_axis=0, concat_axis=0, tiled=True))
    gated = pl.pallas_call(
        gated_kernel,
        out_shape=jax.ShapeDtypeStruct((parts, rows, features // parts), jnp.bfloat16),
        in_specs=[VM] * 9 + [SM],
        out_specs=VM,
        scratch_shapes=common
        + more,
        compiler_params=limit,
        name="gated",
    )(
        head_input,
        gate_input,
        increment_preactivation.T,
        write_vector,
        read_vector,
        entry,
        bias,
        dlog,
        gain,
        doc_starts,
    )
    gated = to_owners(gated)
    blocks = gated.reshape(devices * groups, GROUP, width)[all_order]
    packed = lax.all_to_all(
        blocks.reshape(devices, rows, width), "ctx", split_axis=0, concat_axis=0, tiled=True
    )
    return pl.pallas_call(
        norm_kernel,
        out_shape=jax.ShapeDtypeStruct((rows, features), jnp.bfloat16),
        in_specs=[VM] * 2,
        out_specs=VM,
        compiler_params=limit,
        name="norm",
    )(joined(packed), norm_weight.reshape(1, -1))


def solution(mesh):
    return jax.shard_map(
        local,
        mesh=mesh,
        in_specs=(
            P(("dp", "ctx"), None),
            P(("dp", "ctx"), None),
            P(("dp", "ctx"), None),
            P(("dp", "ctx"), None),
            P(("dp", "ctx"), None),
            P(),
            P(),
            P(),
            P(),
            P(("dp", "ctx")),
            P(("dp", "ctx")),
        ),
        out_specs=P(("dp", "ctx"), None),
        check_vma=False,
    )
```

```python
import functools

import jax
import jax.numpy as jnp
from jax import lax
from jax.experimental import pallas as pl
from jax.experimental.pallas import tpu as pltpu
from jax.sharding import PartitionSpec as P

HEAD_DIM = 64
GROUP = 128
CHUNK = 8
WIDE = CHUNK * HEAD_DIM
EXTRA = 16
PARTS = 4
LIMIT = 61 * 1024 * 1024
UNIT = 256

highest = lax.Precision.HIGHEST
VM = pl.BlockSpec(memory_space=pltpu.VMEM)
SM = pl.BlockSpec(memory_space=pltpu.SMEM)
ANY = pl.BlockSpec(memory_space=pltpu.HBM)


def transposed(v):
    rows, cols = v.shape
    if cols < 128:
        v = jnp.concatenate([v, jnp.zeros((rows, 128 - cols), v.dtype)], axis=1)
    return v.T[:cols]


def upright(v):
    rows, cols = v.shape
    if rows < 128:
        v = jnp.concatenate([v, jnp.zeros((128 - rows, cols), v.dtype)], axis=0)
    return v.T[:, :rows]


def lower_mask():
    row = lax.broadcasted_iota(jnp.int32, (GROUP, GROUP), 0)
    col = lax.broadcasted_iota(jnp.int32, (GROUP, GROUP), 1)
    return row >= col


def step_terms(logit_ref, bias_ref, dlog_ref):
    raw = logit_ref[...].astype(jnp.float32)
    raw = jnp.concatenate([upright(raw[:, k : k + GROUP]) for k in range(0, raw.shape[1], GROUP)], axis=0)
    v = raw + bias_ref[...]
    dt = jnp.maximum(v, 0.0) + jnp.log(1.0 + jnp.exp(-jnp.abs(v)))
    return dt, -dt * jnp.exp(dlog_ref[...])


def spread(v):
    rows = v.shape[0]
    first = lax.broadcasted_iota(jnp.int32, (rows, 128), 1) < HEAD_DIM
    return jnp.concatenate(
        [
            jnp.where(first, v[:, k : k + 1], v[:, k + 1 : k + 2])
            for k in range(0, CHUNK, 2)
        ],
        axis=1,
    )


def prepare(logit_ref, bias_ref, dlog_ref, write_ref, cum_s, dt_s, write_t):
    heads = bias_ref.shape[1]
    dt, fall = step_terms(logit_ref, bias_ref, dlog_ref)
    tri = lower_mask().astype(jnp.float32)
    cums = []
    for g in range(write_t.shape[0]):
        rows = slice(g * GROUP, (g + 1) * GROUP)
        cum = jnp.dot(tri, fall[rows], precision=highest, preferred_element_type=jnp.float32)
        cums.append(cum)
        for c in range(heads // CHUNK):
            cum_s[g, c] = cum[:, c * CHUNK : (c + 1) * CHUNK]
            dt_s[g, c] = dt[rows, c * CHUNK : (c + 1) * CHUNK]
        write_t[g] = write_ref[rows, :].astype(jnp.float32).T.astype(jnp.bfloat16)
    return dt, cums


def group_state(g, c, x, cum_s, dt_s, write_t):
    cum = cum_s[g, c]
    last = cum[GROUP - 1 : GROUP]
    tail = jnp.exp(last - cum) * dt_s[g, c]
    scaled = (x.astype(jnp.float32) * spread(tail)).astype(jnp.bfloat16)
    state = jnp.dot(write_t[g], scaled, preferred_element_type=jnp.float32)
    return state, spread(jnp.exp(last))


def state_kernel(
    x_ref, logit_ref, write_ref, bias_ref, dlog_ref, starts_ref, order_ref, out_ref, cum_s, dt_s, write_t
):
    groups = write_t.shape[0]
    prepare(logit_ref, bias_ref, dlog_ref, write_ref, cum_s, dt_s, write_t)
    parts, _, width = out_ref.shape
    chunks = cum_s.shape[1]
    per = width // WIDE

    def one(c, carry):
        cols = pl.ds(pl.multiple_of(c * WIDE, WIDE), WIDE)
        total, decay = None, None
        for g in range(groups):
            x = x_ref[g * GROUP : (g + 1) * GROUP, cols]
            state, last = group_state(g, c, x, cum_s, dt_s, write_t)
            keep = 1.0 - starts_ref[g].astype(jnp.float32)
            factor = keep * last
            total = state if total is None else factor * total + state
            decay = factor if decay is None else factor * decay
        coarse = decay.astype(jnp.bfloat16)
        fine = (decay - coarse.astype(jnp.float32)).astype(jnp.bfloat16)
        row = lax.broadcasted_iota(jnp.int32, (EXTRA, WIDE), 0)
        lane = lax.broadcasted_iota(jnp.int32, (EXTRA, WIDE), 1)
        order = jnp.zeros((EXTRA, WIDE), jnp.float32)
        for g in range(groups):
            order = jnp.where(lane == g, order_ref[g].astype(jnp.float32), order)
        extra = jnp.where(
            row == 0,
            coarse.astype(jnp.float32),
            jnp.where(row == 1, fine.astype(jnp.float32), order),
        )
        full = jnp.concatenate([total, extra], axis=0).astype(jnp.bfloat16)
        if parts == 1:
            out_ref[0, :, cols] = full
        else:
            into = pl.ds(pl.multiple_of((c % per) * WIDE, WIDE), WIDE)
            out_ref[c // per, :, into] = full
        return carry

    lax.fori_loop(0, chunks, one, 0)


def scan_kernel(in_ref, out_ref):
    parts, _, width = in_ref.shape
    state = jnp.zeros((GROUP, width), jnp.float32)
    for s in range(parts):
        out_ref[s] = state.astype(jnp.bfloat16)
        extra = in_ref[s, GROUP : GROUP + EXTRA, :].astype(jnp.float32)
        decay = extra[0:1] + extra[1:2]
        state = decay * state + in_ref[s, :GROUP, :].astype(jnp.float32)


def gated_setup(
    logit_ref, bias_ref, dlog_ref, write_ref, read_ref, gain_ref, cum_s, dt_s, write_t, cum_t, dt_t, gain_s, score_s
):
    groups, chunks = cum_s.shape[:2]
    dt, cums = prepare(logit_ref, bias_ref, dlog_ref, write_ref, cum_s, dt_s, write_t)
    mask = lower_mask()
    for g in range(groups):
        rows = slice(g * GROUP, (g + 1) * GROUP)
        ct = transposed(cums[g])
        dtt = transposed(dt[rows])
        for c in range(chunks):
            cum_t[g, c] = ct[c * CHUNK : (c + 1) * CHUNK]
            dt_t[g, c] = dtt[c * CHUNK : (c + 1) * CHUNK]
        score = jnp.dot(read_ref[rows, :], write_t[g], preferred_element_type=jnp.float32)
        score_s[g] = jnp.where(mask, score, 0.0)
    for c in range(chunks):
        gain_s[c] = jnp.broadcast_to(gain_ref[:, c * CHUNK : (c + 1) * CHUNK], (8, CHUNK))


def gated_chunk(
    c, state, put, x_ref, gate_ref, read_ref, starts_ref, cum_s, dt_s, write_t, cum_t, dt_t, gain_s, score_s
):
    groups = cum_s.shape[0]
    first = lax.broadcasted_iota(jnp.int32, (GROUP, 128), 1) < HEAD_DIM
    cols = pl.ds(pl.multiple_of(c * WIDE, WIDE), WIDE)
    gain = spread(gain_s[c][0:1])
    for g in range(groups):
        rows = slice(g * GROUP, (g + 1) * GROUP)
        x = x_ref[rows, cols]
        keep = 1.0 - starts_ref[g].astype(jnp.float32)
        entering = (keep * state).astype(jnp.bfloat16)
        cum = cum_s[g, c]
        carried = jnp.dot(read_ref[rows, :], entering, preferred_element_type=jnp.float32)
        mixed = carried * spread(jnp.exp(cum)) + gain * x.astype(jnp.float32)
        score = score_s[g]
        ct, dtt = cum_t[g, c], dt_t[g, c]
        pieces = []
        for k in range(0, CHUNK, 2):
            pair = x[:, k * HEAD_DIM : (k + 2) * HEAD_DIM]
            both = []
            for h in (k, k + 1):
                gap = cum[:, h : h + 1] - ct[h : h + 1]
                weight = score * jnp.exp(jnp.minimum(gap, 0.0)) * dtt[h : h + 1]
                both.append(
                    jnp.dot(weight.astype(jnp.bfloat16), pair, preferred_element_type=jnp.float32)
                )
            pieces.append(jnp.where(first, both[0], both[1]))
        mixed = mixed + jnp.concatenate(pieces, axis=1)
        gate = gate_ref[rows, cols].astype(jnp.float32)
        put(g, (mixed * (gate / (1.0 + jnp.exp(-gate)))).astype(jnp.bfloat16))
        if g + 1 < groups:
            own, last = group_state(g, c, x, cum_s, dt_s, write_t)
            state = keep * last * state + own


def gated_kernel(
    x_ref,
    gate_ref,
    logit_ref,
    write_ref,
    read_ref,
    entry_ref,
    bias_ref,
    dlog_ref,
    gain_ref,
    starts_ref,
    out_ref,
    *scratch,
):
    gated_setup(logit_ref, bias_ref, dlog_ref, write_ref, read_ref, gain_ref, *scratch)
    parts, _, width = out_ref.shape
    chunks = scratch[0].shape[1]
    per = width // WIDE

    def one(c, carry):
        cols = pl.ds(pl.multiple_of(c * WIDE, WIDE), WIDE)
        into = pl.ds(pl.multiple_of((c % per) * WIDE, WIDE), WIDE)
        if parts == 1:
            state = entry_ref[0, :, cols].astype(jnp.float32)
        else:
            state = entry_ref[c // per, :, into].astype(jnp.float32)

        def put(g, value):
            rows = slice(g * GROUP, (g + 1) * GROUP)
            if parts == 1:
                out_ref[0, rows, cols] = value
            else:
                out_ref[c // per, rows, into] = value

        gated_chunk(c, state, put, x_ref, gate_ref, read_ref, starts_ref, *scratch)
        return carry

    lax.fori_loop(0, chunks, one, 0)


def fused_kernel(
    n,
    parts,
    x_hbm,
    gate_hbm,
    logit_ref,
    write_ref,
    read_ref,
    bias_ref,
    dlog_ref,
    gain_ref,
    starts_ref,
    order_ref,
    out_ref,
    squares,
    x_ref,
    gate_ref,
    pair_out,
    pair_in,
    total_s,
    decay_s,
    e_in,
    f_out,
    back,
    entry,
    made,
    stage,
    final,
    order_own,
    order_all,
    order_s,
    load_sem,
    pair_send,
    pair_recv,
    chain_send,
    chain_recv,
    back_send,
    back_recv,
    send1,
    recv1,
    send2,
    recv2,
    send3,
    recv3,
    order_sem,
    gate_sem,
    *rest,
):
    got, scratch = rest[:parts], rest[parts:]
    cum_s, dt_s, write_t = scratch[:3]
    groups, chunks = cum_s.shape[:2]
    piece = stage.shape[-1]
    per = WIDE // piece
    steps = chunks // parts
    state_size = write_t.shape[1]
    me = lax.axis_index("ctx")
    side = me % 2
    level = me // 2
    levels = n // 2
    buddy = me + 1 - 2 * side
    span = chunks // parts * WIDE
    units = WIDE // UNIT

    def send(source, target, sends, recvs, there):
        return pltpu.make_async_remote_copy(
            src_ref=source,
            dst_ref=target,
            send_sem=sends,
            recv_sem=recvs,
            device_id={"ctx": there},
            device_id_type=pl.DeviceIdType.MESH,
        )

    def load(which, j):
        cols = pl.ds(j * span, span)
        source, target = ((x_hbm, x_ref), (gate_hbm, gate_ref))[which]
        return pltpu.make_async_copy(source.at[:, cols], target.at[:, cols], load_sem.at[which, j])

    def pair(c):
        return send(pair_out.at[c], pair_in.at[c], pair_send.at[c], pair_recv.at[c], buddy)

    def chain(c):
        return send(f_out.at[c], e_in.at[c], chain_send.at[c], chain_recv.at[c], lax.rem(me + 2, n))

    def give(c):
        return send(back.at[c], entry.at[c], back_send.at[c], back_recv.at[c], buddy)

    def order_to(there, slot):
        return send(order_own, order_all.at[slot], send3.at[there], recv3.at[slot], there)

    def first(there, slot, j):
        return send(
            made.at[there, j],
            got[j].at[pl.ds(slot * groups, groups)],
            send1.at[there, j],
            recv1.at[slot, j],
            there,
        )

    def second(there, slot, j):
        return send(stage.at[there, j], final.at[slot, j], send2.at[there, j], recv2.at[slot, j], there)

    for j in range(parts):
        load(0, j).start()
    for j in range(parts):
        load(1, j).start()
    barrier = pltpu.get_barrier_semaphore()
    for off in range(1, n):
        pl.semaphore_signal(
            barrier, inc=1, device_id={"ctx": lax.rem(me + off, n)}, device_id_type=pl.DeviceIdType.MESH
        )
    lane = lax.broadcasted_iota(jnp.int32, order_own.shape, 1)
    held = jnp.zeros(order_own.shape, jnp.int32)
    for g in range(groups):
        held = jnp.where(lane == g, order_ref[g], held)
    order_own[...] = held
    order_all[me] = held
    with jax.named_scope("setup"):
        gated_setup(logit_ref, bias_ref, dlog_ref, write_ref, read_ref, gain_ref, *scratch)

    @pl.when(level == 0)
    def _():
        e_in[...] = jnp.zeros_like(e_in)

    @pl.when(me == 0)
    def _():
        entry[...] = jnp.zeros_like(entry)

    def ends(c, carry):
        cols = pl.ds(pl.multiple_of(c * WIDE, WIDE), WIDE)
        total, decay = None, None
        for g in range(groups):
            x = x_ref[g * GROUP : (g + 1) * GROUP, cols]
            state, last = group_state(g, c, x, cum_s, dt_s, write_t)
            factor = (1.0 - starts_ref[g].astype(jnp.float32)) * last
            total = state if total is None else factor * total + state
            decay = factor if decay is None else factor * decay
        for u in range(units):
            cut = slice(u * UNIT, (u + 1) * UNIT)
            total_s[c * units + u] = total[:, cut]
            decay_s[c * units + u] = jnp.broadcast_to(decay[:, cut], (8, UNIT))

        @pl.when(c % 2 != side)
        def _():
            coarse = decay.astype(jnp.bfloat16).astype(jnp.float32)
            row = lax.broadcasted_iota(jnp.int32, (EXTRA, WIDE), 0)
            extra = jnp.where(row == 0, coarse, decay - coarse)
            full = jnp.concatenate([total, extra], axis=0).astype(jnp.bfloat16)
            for u in range(units):
                pair_out[c * units + u] = full[:, u * UNIT : (u + 1) * UNIT]

        return carry

    def offer(i, carry):
        c = 2 * i + 1 - side
        for u in range(units):
            pair(c * units + u).start()
        return carry

    for j in range(parts):
        with jax.named_scope("loadx"):
            load(0, j).wait()
        with jax.named_scope("ends"):
            lax.fori_loop(j * steps, (j + 1) * steps, ends, 0)
        if j == 0:
            with jax.named_scope("barrier"):
                pl.semaphore_wait(barrier, n - 1)
            for off in range(1, n):
                order_to(lax.rem(me + off, n), me).start()
        lax.fori_loop(j * steps // 2, (j + 1) * steps // 2, offer, 0)

    def relay(q):
        pair(q).wait_recv()

        @pl.when(level > 0)
        def _():
            chain(q).wait_recv()

        state = e_in[q].astype(jnp.float32)
        their = pair_in[q, :state_size].astype(jnp.float32)
        tail = pair_in[q, state_size : state_size + EXTRA].astype(jnp.float32)
        fade = tail[0:1] + tail[1:2]
        total, decay = total_s[q], decay_s[q][0:1]
        early = side == 0
        middle = jnp.where(early, decay, fade) * state + jnp.where(early, total, their)

        @pl.when(level < levels - 1)
        def _():
            end = jnp.where(early, fade, decay) * middle + jnp.where(early, their, total)
            f_out[q] = end.astype(jnp.bfloat16)
            chain(q).start()

        @pl.when(me != 1)
        def _():
            back[q] = jnp.where(early, middle, state).astype(jnp.bfloat16)
            give(q).start()

        entry[q] = jnp.where(early, state, middle).astype(jnp.bfloat16)

    def links(i, carry):
        q = (2 * (i // units) + side) * units + i % units
        relay(q)
        return carry

    inward = steps // 2 * units

    low = level < levels // 2

    def by_distance(k):
        return jnp.where(low, levels - 1 - k, k)

    def gate_ready(j):
        for s in range(parts):

            @pl.when(j == s)
            def _():
                load(1, s).wait()

    def compute(j, i):
        c = j * steps + i

        def put(g, value):
            for p in range(per):
                made[p * steps + i, j, g] = value[:, p * piece : (p + 1) * piece]

        with jax.named_scope("gated"):
            state = jnp.concatenate([entry[c * units + u].astype(jnp.float32) for u in range(units)], axis=1)
            gated_chunk(c, state, put, x_ref, gate_ref, read_ref, starts_ref, *scratch)

    def outward(j, there, wanted):
        for s in range(parts):

            @pl.when(jnp.logical_and(j == s, jnp.logical_and(there != me, wanted)))
            def _():
                first(there, me, s).start()

    def keep(j, i):
        for s in range(parts):

            @pl.when(jnp.logical_and(j == s, lax.rem(me, steps) == i))
            def _():
                for g in range(groups):
                    got[s][me * groups + g] = made[me, s, g]

    def near_column(j, carry):
        with jax.named_scope("links"):
            lax.fori_loop(j * inward, (j + 1) * inward, links, 0)
        gate_ready(j)

        def one(t, inner):
            i = 2 * t + side
            compute(j, i)
            for k in range(per):
                there = by_distance(k) * steps + i
                outward(j, there, there // 2 < level)
            keep(j, i)
            return inner

        lax.fori_loop(0, steps // 2, one, 0)
        return carry

    def postponed(far):
        def some(j, carry):
            def one(t, inner):
                i = 2 * t + side
                for k in range(per):
                    there = by_distance(k) * steps + i
                    high = there // 2
                    outward(j, there, jnp.logical_and(high >= level, (high >= levels // 2) == far))
                return inner

            lax.fori_loop(0, steps // 2, one, 0)
            return carry

        lax.fori_loop(0, parts, some, 0)

    def far_column(j, carry):
        def one(t, inner):
            i = 2 * t + 1 - side
            c = j * steps + i

            @pl.when(me > 0)
            def _():
                with jax.named_scope("waitgive"):
                    for u in range(units):
                        give(c * units + u).wait_recv()

            compute(j, i)
            for k in range(per):
                outward(j, by_distance(k) * steps + i, True)
            keep(j, i)
            return inner

        lax.fori_loop(0, steps // 2, one, 0)
        return carry

    lax.fori_loop(0, parts, near_column, 0)
    for far in (False, True):
        postponed(far)
    lax.fori_loop(0, parts, far_column, 0)

    def crossed(j, carry):
        for k in range(n // 2):
            there = jnp.where(low, n // 2, 0) + k
            first(there, there, j).wait_send()
        return carry

    lower_inner = jnp.logical_and(level == levels // 2 - 1, level > 0)
    upper_inner = jnp.logical_and(level == levels // 2, level < levels - 1)

    @pl.when(jnp.logical_or(lower_inner, upper_inner))
    def _():
        with jax.named_scope("crossed"):
            for j in range(parts):
                crossed(j, 0)
        pl.semaphore_signal(
            gate_sem,
            inc=1,
            device_id={"ctx": jnp.where(low, me - 2, lax.rem(me + 2, n))},
            device_id_type=pl.DeviceIdType.MESH,
        )

    for off in range(1, n):
        there = lax.rem(me + off, n)
        order_to(there, there).wait_recv()
    fetch = pltpu.make_async_copy(order_all, order_s, order_sem)
    fetch.start()
    fetch.wait()
    if levels > 2:

        @pl.when(jnp.logical_or(level == levels // 2 - 2, level == levels // 2 + 1))
        def _():
            with jax.named_scope("gate"):
                pl.semaphore_wait(gate_sem, 1)

    for j in range(parts):
        with jax.named_scope("waitfirst"):
            for off in range(1, n):
                there = lax.rem(me + off, n)
                first(there, there, j).wait_recv()

        def pick(k, carry, j=j):
            there = 2 * by_distance(k // 2) + lax.rem(k + me, 2)

            @pl.when(there != me)
            def _():
                for g in range(groups):
                    stage[there, j, g] = got[j][order_s[there, 0, g]]
                second(there, me, j).start()

            @pl.when(there == me)
            def _():
                for g in range(groups):
                    final[me, j, g] = got[j][order_s[me, 0, g]]

            return carry

        with jax.named_scope("pick"):
            lax.fori_loop(0, n, pick, 0)
    tile = 32
    for j in range(parts):
        with jax.named_scope("waitsecond"):
            for off in range(1, n):
                there = lax.rem(me + off, n)
                second(there, there, j).wait_recv()

        def add(r, carry, j=j):
            for g in range(groups):
                at = pl.ds(pl.multiple_of(r * tile, tile), tile)
                into = pl.ds(pl.multiple_of(g * GROUP + r * tile, tile), tile)
                total = jnp.zeros((tile, 128), jnp.float32) if j == 0 else squares[into, :]
                for s in range(n):
                    raw = final[s, j, g, at, :]
                    left = (j * steps + s % steps) * WIDE + s // steps * piece
                    out_ref[into, left : left + piece] = raw
                    v = raw.astype(jnp.float32)
                    v = v * v
                    for q in range(0, piece, 128):
                        total = total + v[:, q : q + 128]
                squares[into, :] = total
            return carry

        with jax.named_scope("add"):
            lax.fori_loop(0, GROUP // tile, add, 0)

    def settle(i, carry):
        pair((2 * (i // units) + 1 - side) * units + i % units).wait_send()
        q = (2 * (i // units) + side) * units + i % units

        @pl.when(me != 1)
        def _():
            give(q).wait_send()

        @pl.when(level < levels - 1)
        def _():
            chain(q).wait_send()

        return carry

    with jax.named_scope("settle"):
        lax.fori_loop(0, parts * inward, settle, 0)
    with jax.named_scope("sent"):
        for off in range(1, n):
            there = lax.rem(me + off, n)
            order_to(there, there).wait_send()
            waited = jnp.logical_and(jnp.logical_or(lower_inner, upper_inner), (there < n // 2) != low)
            for j in range(parts):
                second(there, there, j).wait_send()

                @pl.when(jnp.logical_not(waited))
                def _():
                    first(there, there, j).wait_send()


def scale_kernel(in_ref, squares_ref, weight_ref, out_ref):
    total = jnp.sum(squares_ref[...], axis=1, keepdims=True)
    scale = lax.rsqrt(total * (1.0 / in_ref.shape[1]) + 1e-05)
    for q in range(0, in_ref.shape[1], WIDE):
        cols = slice(q, q + WIDE)
        v = in_ref[:, cols].astype(jnp.float32)
        out_ref[:, cols] = (v * scale * weight_ref[:, cols]).astype(jnp.bfloat16)


def norm_kernel(in_ref, weight_ref, out_ref):
    parts, rows, width = in_ref.shape
    tile = 32

    def one(r, carry):
        at = pl.ds(pl.multiple_of(r * tile, tile), tile)
        total = jnp.zeros((tile, 1), jnp.float32)
        for s in range(parts):
            v = in_ref[s, at, :].astype(jnp.float32)
            total = total + jnp.sum(v * v, axis=1, keepdims=True)
        scale = lax.rsqrt(total * (1.0 / (parts * width)) + 1e-05)
        for s in range(parts):
            v = in_ref[s, at, :].astype(jnp.float32)
            w = weight_ref[:, s * width : (s + 1) * width]
            out_ref[at, s * width : (s + 1) * width] = (v * scale * w).astype(jnp.bfloat16)
        return carry

    lax.fori_loop(0, rows // tile, one, 0)


def local(
    head_input,
    gate_input,
    write_vector,
    read_vector,
    increment_preactivation,
    step_bias,
    decay_log,
    skip_gain,
    norm_weight,
    doc_starts,
    block_order,
):
    devices = lax.axis_size("ctx")
    rows, features = head_input.shape
    heads = step_bias.shape[0]
    groups = rows // GROUP
    chunks = heads // CHUNK
    width = features // devices
    state_size = write_vector.shape[1]
    direct = width % WIDE == 0
    parts = devices if direct else 1
    limit = pltpu.CompilerParams(vmem_limit_bytes=48 * 1024 * 1024)
    common = [
        pltpu.VMEM((groups, chunks, GROUP, CHUNK), jnp.float32),
        pltpu.VMEM((groups, chunks, GROUP, CHUNK), jnp.float32),
        pltpu.VMEM((groups, state_size, GROUP), jnp.bfloat16),
    ]
    more = [
        pltpu.VMEM((groups, chunks, CHUNK, GROUP), jnp.float32),
        pltpu.VMEM((groups, chunks, CHUNK, GROUP), jnp.float32),
        pltpu.VMEM((chunks, 8, CHUNK), jnp.float32),
        pltpu.VMEM((groups, GROUP, GROUP), jnp.float32),
    ]
    bias, dlog, gain = (v.reshape(1, -1) for v in (step_bias, decay_log, skip_gain))

    def to_owners(v):
        if not direct:
            v = v.reshape(v.shape[1], devices, width).transpose(1, 0, 2)
        return lax.all_to_all(v, "ctx", split_axis=0, concat_axis=0, tiled=True)

    def joined(v):
        if not direct:
            v = v.transpose(1, 0, 2).reshape(1, v.shape[1], features)
        return v

    piece = width // PARTS
    per = max(WIDE // max(piece, 1), 1)
    if width == 512 and devices == 2 * per:
        slab = (devices, PARTS, groups, GROUP, piece)
        links = features // UNIT
        state = (links, state_size, UNIT)
        sems = pltpu.SemaphoreType.DMA
        packed, squares = pl.pallas_call(
            functools.partial(fused_kernel, devices, PARTS),
            out_shape=[
                pltpu.VMEM((rows, features), jnp.bfloat16),
                pltpu.VMEM((rows, 128), jnp.float32),
            ],
            in_specs=[ANY] * 2 + [VM] * 6 + [SM] * 2,
            out_specs=[VM] * 2,
            scratch_shapes=[
                pltpu.VMEM((rows, features), jnp.bfloat16),
                pltpu.VMEM((rows, features), jnp.bfloat16),
                pltpu.VMEM((links, state_size + EXTRA, UNIT), jnp.bfloat16),
                pltpu.VMEM((links, state_size + EXTRA, UNIT), jnp.bfloat16),
                pltpu.VMEM(state, jnp.float32),
                pltpu.VMEM((links, 8, UNIT), jnp.float32),
                pltpu.VMEM(state, jnp.bfloat16),
                pltpu.VMEM(state, jnp.bfloat16),
                pltpu.VMEM(state, jnp.bfloat16),
                pltpu.VMEM(state, jnp.bfloat16),
                pltpu.VMEM(slab, jnp.bfloat16),
                pltpu.VMEM(slab, jnp.bfloat16),
                pltpu.VMEM(slab, jnp.bfloat16),
                pltpu.VMEM((8, 128), jnp.int32),
                pltpu.VMEM((devices, 8, 128), jnp.int32),
                pltpu.SMEM((devices, 8, 128), jnp.int32),
                sems((2, PARTS)),
            ]
            + [sems((links,))] * 6
            + [sems((devices, PARTS))] * 4
            + [sems((devices,))] * 2
            + [sems, pltpu.SemaphoreType.REGULAR]
            + [pltpu.VMEM((devices * groups, GROUP, piece), jnp.bfloat16)] * PARTS
            + common
            + more,
            compiler_params=pltpu.CompilerParams(
                collective_id=0, has_side_effects=True, vmem_limit_bytes=LIMIT
            ),
            name="fused",
        )(
            head_input,
            gate_input,
            increment_preactivation.T,
            write_vector,
            read_vector,
            bias,
            dlog,
            gain,
            doc_starts,
            block_order,
        )
        tile = 64
        return pl.pallas_call(
            scale_kernel,
            grid=(rows // tile,),
            out_shape=jax.ShapeDtypeStruct((rows, features), jnp.bfloat16),
            in_specs=[
                pl.BlockSpec((tile, features), lambda r: (r, 0)),
                pl.BlockSpec((tile, 128), lambda r: (r, 0)),
                pl.BlockSpec((1, features), lambda r: (0, 0)),
            ],
            out_specs=pl.BlockSpec((tile, features), lambda r: (r, 0)),
            compiler_params=pltpu.CompilerParams(vmem_limit_bytes=8 * 1024 * 1024),
            name="scale",
        )(packed, squares, norm_weight.reshape(1, -1))

    ends = pl.pallas_call(
        state_kernel,
        out_shape=jax.ShapeDtypeStruct((parts, state_size + EXTRA, features // parts), jnp.bfloat16),
        in_specs=[VM] * 5 + [SM] * 2,
        out_specs=VM,
        scratch_shapes=common,
        compiler_params=limit,
        name="end_states",
    )(head_input, increment_preactivation.T, write_vector, bias, dlog, doc_starts, block_order)
    ends = to_owners(ends)
    all_order = ends[:, state_size + 2, :groups].astype(jnp.int32).reshape(-1)
    entry = pl.pallas_call(
        scan_kernel,
        out_shape=jax.ShapeDtypeStruct((devices, state_size, width), jnp.bfloat16),
        in_specs=[VM],
        out_specs=VM,
        compiler_params=limit,
        name="scan_states",
    )(ends)
    entry = joined(lax.all_to_all(entry, "ctx", split_axis=0, concat_axis=0, tiled=True))
    gated = pl.pallas_call(
        gated_kernel,
        out_shape=jax.ShapeDtypeStruct((parts, rows, features // parts), jnp.bfloat16),
        in_specs=[VM] * 9 + [SM],
        out_specs=VM,
        scratch_shapes=common
        + more,
        compiler_params=limit,
        name="gated",
    )(
        head_input,
        gate_input,
        increment_preactivation.T,
        write_vector,
        read_vector,
        entry,
        bias,
        dlog,
        gain,
        doc_starts,
    )
    gated = to_owners(gated)
    blocks = gated.reshape(devices * groups, GROUP, width)[all_order]
    packed = lax.all_to_all(
        blocks.reshape(devices, rows, width), "ctx", split_axis=0, concat_axis=0, tiled=True
    )
    return pl.pallas_call(
        norm_kernel,
        out_shape=jax.ShapeDtypeStruct((rows, features), jnp.bfloat16),
        in_specs=[VM] * 2,
        out_specs=VM,
        compiler_params=limit,
        name="norm",
    )(joined(packed), norm_weight.reshape(1, -1))


def solution(mesh):
    return jax.shard_map(
        local,
        mesh=mesh,
        in_specs=(
            P(("dp", "ctx"), None),
            P(("dp", "ctx"), None),
            P(("dp", "ctx"), None),
            P(("dp", "ctx"), None),
            P(("dp", "ctx"), None),
            P(),
            P(),
            P(),
            P(),
            P(("dp", "ctx")),
            P(("dp", "ctx")),
        ),
        out_specs=P(("dp", "ctx"), None),
        check_vma=False,
    )
```

```python
import functools

import jax
import jax.numpy as jnp
from jax import lax
from jax.experimental import pallas as pl
from jax.experimental.pallas import tpu as pltpu
from jax.sharding import PartitionSpec as P

HEAD_DIM = 64
GROUP = 128
CHUNK = 8
WIDE = CHUNK * HEAD_DIM
EXTRA = 16
PARTS = 4
LIMIT = 61 * 1024 * 1024
UNIT = 128

highest = lax.Precision.HIGHEST
VM = pl.BlockSpec(memory_space=pltpu.VMEM)
SM = pl.BlockSpec(memory_space=pltpu.SMEM)
ANY = pl.BlockSpec(memory_space=pltpu.HBM)


def transposed(v):
    rows, cols = v.shape
    if cols < 128:
        v = jnp.concatenate([v, jnp.zeros((rows, 128 - cols), v.dtype)], axis=1)
    return v.T[:cols]


def upright(v):
    rows, cols = v.shape
    if rows < 128:
        v = jnp.concatenate([v, jnp.zeros((128 - rows, cols), v.dtype)], axis=0)
    return v.T[:, :rows]


def lower_mask():
    row = lax.broadcasted_iota(jnp.int32, (GROUP, GROUP), 0)
    col = lax.broadcasted_iota(jnp.int32, (GROUP, GROUP), 1)
    return row >= col


def step_terms(logit_ref, bias_ref, dlog_ref):
    raw = logit_ref[...].astype(jnp.float32)
    raw = jnp.concatenate([upright(raw[:, k : k + GROUP]) for k in range(0, raw.shape[1], GROUP)], axis=0)
    v = raw + bias_ref[...]
    dt = jnp.maximum(v, 0.0) + jnp.log(1.0 + jnp.exp(-jnp.abs(v)))
    return dt, -dt * jnp.exp(dlog_ref[...])


def spread(v):
    rows = v.shape[0]
    first = lax.broadcasted_iota(jnp.int32, (rows, 128), 1) < HEAD_DIM
    return jnp.concatenate(
        [
            jnp.where(first, v[:, k : k + 1], v[:, k + 1 : k + 2])
            for k in range(0, CHUNK, 2)
        ],
        axis=1,
    )


def prepare(logit_ref, bias_ref, dlog_ref, write_ref, cum_s, dt_s, write_t):
    heads = bias_ref.shape[1]
    dt, fall = step_terms(logit_ref, bias_ref, dlog_ref)
    tri = lower_mask().astype(jnp.float32)
    cums = []
    for g in range(write_t.shape[0]):
        rows = slice(g * GROUP, (g + 1) * GROUP)
        cum = jnp.dot(tri, fall[rows], precision=highest, preferred_element_type=jnp.float32)
        cums.append(cum)
        for c in range(heads // CHUNK):
            cum_s[g, c] = cum[:, c * CHUNK : (c + 1) * CHUNK]
            dt_s[g, c] = dt[rows, c * CHUNK : (c + 1) * CHUNK]
        write_t[g] = write_ref[rows, :].astype(jnp.float32).T.astype(jnp.bfloat16)
    return dt, cums


def group_state(g, c, x, cum_s, dt_s, write_t):
    cum = cum_s[g, c]
    last = cum[GROUP - 1 : GROUP]
    tail = jnp.exp(last - cum) * dt_s[g, c]
    scaled = (x.astype(jnp.float32) * spread(tail)).astype(jnp.bfloat16)
    state = jnp.dot(write_t[g], scaled, preferred_element_type=jnp.float32)
    return state, spread(jnp.exp(last))


def state_kernel(
    x_ref, logit_ref, write_ref, bias_ref, dlog_ref, starts_ref, order_ref, out_ref, cum_s, dt_s, write_t
):
    groups = write_t.shape[0]
    prepare(logit_ref, bias_ref, dlog_ref, write_ref, cum_s, dt_s, write_t)
    parts, _, width = out_ref.shape
    chunks = cum_s.shape[1]
    per = width // WIDE

    def one(c, carry):
        cols = pl.ds(pl.multiple_of(c * WIDE, WIDE), WIDE)
        total, decay = None, None
        for g in range(groups):
            x = x_ref[g * GROUP : (g + 1) * GROUP, cols]
            state, last = group_state(g, c, x, cum_s, dt_s, write_t)
            keep = 1.0 - starts_ref[g].astype(jnp.float32)
            factor = keep * last
            total = state if total is None else factor * total + state
            decay = factor if decay is None else factor * decay
        coarse = decay.astype(jnp.bfloat16)
        fine = (decay - coarse.astype(jnp.float32)).astype(jnp.bfloat16)
        row = lax.broadcasted_iota(jnp.int32, (EXTRA, WIDE), 0)
        lane = lax.broadcasted_iota(jnp.int32, (EXTRA, WIDE), 1)
        order = jnp.zeros((EXTRA, WIDE), jnp.float32)
        for g in range(groups):
            order = jnp.where(lane == g, order_ref[g].astype(jnp.float32), order)
        extra = jnp.where(
            row == 0,
            coarse.astype(jnp.float32),
            jnp.where(row == 1, fine.astype(jnp.float32), order),
        )
        full = jnp.concatenate([total, extra], axis=0).astype(jnp.bfloat16)
        if parts == 1:
            out_ref[0, :, cols] = full
        else:
            into = pl.ds(pl.multiple_of((c % per) * WIDE, WIDE), WIDE)
            out_ref[c // per, :, into] = full
        return carry

    lax.fori_loop(0, chunks, one, 0)


def scan_kernel(in_ref, out_ref):
    parts, _, width = in_ref.shape
    state = jnp.zeros((GROUP, width), jnp.float32)
    for s in range(parts):
        out_ref[s] = state.astype(jnp.bfloat16)
        extra = in_ref[s, GROUP : GROUP + EXTRA, :].astype(jnp.float32)
        decay = extra[0:1] + extra[1:2]
        state = decay * state + in_ref[s, :GROUP, :].astype(jnp.float32)


def gated_setup(
    logit_ref, bias_ref, dlog_ref, write_ref, read_ref, gain_ref, cum_s, dt_s, write_t, cum_t, dt_t, gain_s, score_s
):
    groups, chunks = cum_s.shape[:2]
    dt, cums = prepare(logit_ref, bias_ref, dlog_ref, write_ref, cum_s, dt_s, write_t)
    mask = lower_mask()
    for g in range(groups):
        rows = slice(g * GROUP, (g + 1) * GROUP)
        ct = transposed(cums[g])
        dtt = transposed(dt[rows])
        for c in range(chunks):
            cum_t[g, c] = ct[c * CHUNK : (c + 1) * CHUNK]
            dt_t[g, c] = dtt[c * CHUNK : (c + 1) * CHUNK]
        score = jnp.dot(read_ref[rows, :], write_t[g], preferred_element_type=jnp.float32)
        score_s[g] = jnp.where(mask, score, 0.0)
    for c in range(chunks):
        gain_s[c] = jnp.broadcast_to(gain_ref[:, c * CHUNK : (c + 1) * CHUNK], (8, CHUNK))
    return cums


def gated_chunk(
    c, state, put, x_ref, gate_ref, read_ref, starts_ref, cum_s, dt_s, write_t, cum_t, dt_t, gain_s, score_s
):
    groups = cum_s.shape[0]
    first = lax.broadcasted_iota(jnp.int32, (GROUP, 128), 1) < HEAD_DIM
    cols = pl.ds(pl.multiple_of(c * WIDE, WIDE), WIDE)
    gain = spread(gain_s[c][0:1])
    for g in range(groups):
        rows = slice(g * GROUP, (g + 1) * GROUP)
        x = x_ref[rows, cols]
        keep = 1.0 - starts_ref[g].astype(jnp.float32)
        entering = (keep * state).astype(jnp.bfloat16)
        cum = cum_s[g, c]
        carried = jnp.dot(read_ref[rows, :], entering, preferred_element_type=jnp.float32)
        mixed = carried * spread(jnp.exp(cum)) + gain * x.astype(jnp.float32)
        score = score_s[g]
        ct, dtt = cum_t[g, c], dt_t[g, c]
        pieces = []
        for k in range(0, CHUNK, 2):
            pair = x[:, k * HEAD_DIM : (k + 2) * HEAD_DIM]
            both = []
            for h in (k, k + 1):
                gap = cum[:, h : h + 1] - ct[h : h + 1]
                weight = score * jnp.exp(jnp.minimum(gap, 0.0)) * dtt[h : h + 1]
                both.append(
                    jnp.dot(weight.astype(jnp.bfloat16), pair, preferred_element_type=jnp.float32)
                )
            pieces.append(jnp.where(first, both[0], both[1]))
        mixed = mixed + jnp.concatenate(pieces, axis=1)
        gate = gate_ref[rows, cols].astype(jnp.float32)
        put(g, (mixed * (gate / (1.0 + jnp.exp(-gate)))).astype(jnp.bfloat16))
        if g + 1 < groups:
            own, last = group_state(g, c, x, cum_s, dt_s, write_t)
            state = keep * last * state + own


def gated_kernel(
    x_ref,
    gate_ref,
    logit_ref,
    write_ref,
    read_ref,
    entry_ref,
    bias_ref,
    dlog_ref,
    gain_ref,
    starts_ref,
    out_ref,
    *scratch,
):
    gated_setup(logit_ref, bias_ref, dlog_ref, write_ref, read_ref, gain_ref, *scratch)
    parts, _, width = out_ref.shape
    chunks = scratch[0].shape[1]
    per = width // WIDE

    def one(c, carry):
        cols = pl.ds(pl.multiple_of(c * WIDE, WIDE), WIDE)
        into = pl.ds(pl.multiple_of((c % per) * WIDE, WIDE), WIDE)
        if parts == 1:
            state = entry_ref[0, :, cols].astype(jnp.float32)
        else:
            state = entry_ref[c // per, :, into].astype(jnp.float32)

        def put(g, value):
            rows = slice(g * GROUP, (g + 1) * GROUP)
            if parts == 1:
                out_ref[0, rows, cols] = value
            else:
                out_ref[c // per, rows, into] = value

        gated_chunk(c, state, put, x_ref, gate_ref, read_ref, starts_ref, *scratch)
        return carry

    lax.fori_loop(0, chunks, one, 0)


def fused_kernel(
    n,
    parts,
    x_hbm,
    gate_hbm,
    logit_ref,
    write_ref,
    read_ref,
    bias_ref,
    dlog_ref,
    gain_ref,
    starts_ref,
    order_ref,
    out_ref,
    squares,
    x_ref,
    gate_ref,
    pair_out,
    pair_in,
    fade_out,
    fade_in,
    fade_s,
    total_s,
    decay_s,
    e_in,
    f_out,
    back,
    near_entry,
    far_entry,
    made,
    stage,
    final,
    order_own,
    order_all,
    order_s,
    load_sem,
    link_recv,
    link_send,
    fade_send,
    fade_recv,
    send1,
    recv1,
    send2,
    recv2,
    send3,
    recv3,
    order_sem,
    gate_sem,
    *rest,
):
    got, scratch = rest[:parts], rest[parts:]
    cum_s, dt_s, write_t = scratch[:3]
    groups, chunks = cum_s.shape[:2]
    piece = stage.shape[-1]
    per = WIDE // piece
    units = WIDE // UNIT
    span = 2 * WIDE
    me = lax.axis_index("ctx")
    side = me % 2
    level = me // 2
    levels = n // 2
    half = n // 2
    buddy = me + 1 - 2 * side
    low = level < levels // 2

    def send(source, target, sends, recvs, there):
        return pltpu.make_async_remote_copy(
            src_ref=source,
            dst_ref=target,
            send_sem=sends,
            recv_sem=recvs,
            device_id={"ctx": there},
            device_id_type=pl.DeviceIdType.MESH,
        )

    def landed(ref, sem):
        send(ref, ref, sem, sem, buddy).wait_recv()

    def left(ref, sem):
        send(ref, ref, sem, sem, buddy).wait_send()

    def load(which, j):
        cols = pl.ds(j * span, span)
        source, target = ((x_hbm, x_ref), (gate_hbm, gate_ref))[which]
        return pltpu.make_async_copy(source.at[:, cols], target.at[:, cols], load_sem.at[which, j])

    def pair(r):
        return send(pair_out.at[r], pair_in.at[r], link_send.at[0], link_recv.at[0, r], buddy)

    def chain(r):
        return send(f_out.at[r], e_in.at[r], link_send.at[1], link_recv.at[1, r], lax.rem(me + 2, n))

    def give(r):
        return send(back.at[r], far_entry.at[r], link_send.at[2], link_recv.at[2, r], buddy)

    def fade():
        return send(fade_out, fade_in, fade_send, fade_recv, buddy)

    def first(there, j):
        far = ((there < half) != low).astype(jnp.int32)
        return send(
            made.at[there, j], got[j].at[pl.ds(me * groups, groups)], send1.at[far], recv1.at[j], there
        )

    def second(there, j):
        return send(stage.at[there, j], final.at[me, j], send2, recv2.at[j], there)

    for j in range(parts):
        load(0, j).start()
    for j in range(parts):
        load(1, j).start()
    barrier = pltpu.get_barrier_semaphore()
    for off in range(1, n):
        pl.semaphore_signal(
            barrier, inc=1, device_id={"ctx": lax.rem(me + off, n)}, device_id_type=pl.DeviceIdType.MESH
        )
    with jax.named_scope("setup"):
        lane = lax.broadcasted_iota(jnp.int32, order_own.shape, 1)
        held = jnp.zeros(order_own.shape, jnp.int32)
        for g in range(groups):
            held = jnp.where(lane == g, order_ref[g], held)
        order_own[...] = held
        order_all[me] = held
        cums = gated_setup(logit_ref, bias_ref, dlog_ref, write_ref, read_ref, gain_ref, *scratch)
        heads = bias_ref.shape[1]
        whole = None
        for g in range(groups):
            factor = (1.0 - starts_ref[g].astype(jnp.float32)) * jnp.exp(cums[g][GROUP - 1 : GROUP])
            whole = factor if whole is None else whole * factor
        whole = jnp.concatenate([whole, jnp.zeros((1, 128 - heads), jnp.float32)], axis=1)
        fade_out[...] = jnp.broadcast_to(whole, (8, 128))

    @pl.when(level == 0)
    def _():
        e_in[...] = jnp.zeros_like(e_in)

    @pl.when(me == 0)
    def _():
        far_entry[...] = jnp.zeros_like(far_entry)

    def ends(c, carry):
        cols = pl.ds(pl.multiple_of(c * WIDE, WIDE), WIDE)
        total, decay = None, None
        for g in range(groups):
            x = x_ref[g * GROUP : (g + 1) * GROUP, cols]
            state, last = group_state(g, c, x, cum_s, dt_s, write_t)
            factor = (1.0 - starts_ref[g].astype(jnp.float32)) * last
            total = state if total is None else factor * total + state
            decay = factor if decay is None else factor * decay
        base = c // 2 * units

        @pl.when(c % 2 == side)
        def _():
            for u in range(units):
                cut = slice(u * UNIT, (u + 1) * UNIT)
                total_s[base + u] = total[:, cut]
                decay_s[base + u] = jnp.broadcast_to(decay[:, cut], (8, UNIT))

        @pl.when(c % 2 != side)
        def _():
            for u in range(units):
                pair_out[base + u] = total[:, u * UNIT : (u + 1) * UNIT].astype(jnp.bfloat16)

        return carry

    def relay(r, carry):
        pair(r).wait_recv()

        @pl.when(level > 0)
        def _():
            chain(r).wait_recv()

        state = e_in[r].astype(jnp.float32)
        their = pair_in[r].astype(jnp.float32)
        theirs = fade_s[r][0:1]
        total, decay = total_s[r], decay_s[r][0:1]
        early = side == 0
        middle = jnp.where(early, decay, theirs) * state + jnp.where(early, total, their)

        @pl.when(level < levels - 1)
        def _():
            end = jnp.where(early, theirs, decay) * middle + jnp.where(early, their, total)
            f_out[r] = end.astype(jnp.bfloat16)
            chain(r).start()

        @pl.when(me != 1)
        def _():
            back[r] = jnp.where(early, middle, state).astype(jnp.bfloat16)
            give(r).start()

        near_entry[r] = jnp.where(early, state, middle).astype(jnp.bfloat16)
        return carry

    def links(j):
        with jax.named_scope("links"):
            lax.fori_loop(j * units, (j + 1) * units, relay, 0)

    def offer(j):
        for u in range(units):
            pair(j * units + u).start()

    ahead = parts // 2
    for j in range(parts):
        load(0, j).wait()
        if j == ahead:
            with jax.named_scope("barrier"):
                pl.semaphore_wait(barrier, n - 1)
            fade().start()
            for k in range(ahead):
                offer(k)
            for off in range(1, n):
                there = lax.rem(me + off, n)
                send(order_own, order_all.at[me], send3, recv3, there).start()
        with jax.named_scope("ends"):
            ends(2 * j + 1 - side, 0)
        if j >= ahead:
            offer(j)
        with jax.named_scope("ends"):
            ends(2 * j + side, 0)
    fade().wait_recv()
    tile = fade_in[0:1, :]
    for c in range(chunks):

        @pl.when(c % 2 == side)
        def _(c=c):
            lanes = spread(tile[:, c * CHUNK : (c + 1) * CHUNK])
            for u in range(units):
                fade_s[c // 2 * units + u] = jnp.broadcast_to(lanes[:, u * UNIT : (u + 1) * UNIT], (8, UNIT))

    @pl.when(low)
    def _():
        with jax.named_scope("linksall"):
            lax.fori_loop(0, parts * units, relay, 0)

    def by_distance(k):
        return jnp.where(low, levels - 1 - k, k)

    def gate_ready(j):
        for s in range(parts):

            @pl.when(j == s)
            def _():
                load(1, s).wait()

    def compute(j, i, entry):
        def put(g, value):
            for p in range(per):
                made[2 * p + i, j, g] = value[:, p * piece : (p + 1) * piece]

        with jax.named_scope("gated"):
            state = jnp.concatenate([entry[j * units + u].astype(jnp.float32) for u in range(units)], axis=1)
            gated_chunk(2 * j + i, state, put, x_ref, gate_ref, read_ref, starts_ref, *scratch)

    def outward(j, there, wanted):
        for s in range(parts):

            @pl.when(jnp.logical_and(j == s, jnp.logical_and(there != me, wanted)))
            def _():
                first(there, s).start()

    def near_column(j, carry):
        @pl.when(jnp.logical_not(low))
        def _():
            links(j)

        gate_ready(j)
        compute(j, side, near_entry)
        for k in range(per):
            there = 2 * k + side
            outward(j, there, jnp.logical_or(low, k < level))
        for s in range(parts):

            @pl.when(j == s)
            def _():
                for g in range(groups):
                    got[s][me * groups + g] = made[me, s, g]

        return carry

    def postponed(j, carry):
        for k in range(per):
            outward(j, 2 * k + side, jnp.logical_not(jnp.logical_or(low, k < level)))
        return carry

    def far_column(j, carry):
        @pl.when(me > 0)
        def _():
            with jax.named_scope("waitgive"):
                for u in range(units):
                    give(j * units + u).wait_recv()

        compute(j, 1 - side, far_entry)
        for k in range(per):
            outward(j, 2 * by_distance(k) + 1 - side, True)
        return carry

    lax.fori_loop(0, parts, near_column, 0)
    lax.fori_loop(0, parts, postponed, 0)
    lax.fori_loop(0, parts, far_column, 0)

    lower_inner = jnp.logical_and(level == levels // 2 - 1, level > 0)
    upper_inner = jnp.logical_and(level == levels // 2, level < levels - 1)
    inner = jnp.logical_or(lower_inner, upper_inner)

    @pl.when(inner)
    def _():
        with jax.named_scope("crossed"):
            left(made.at[pl.ds(0, half)], send1.at[1])
        pl.semaphore_signal(
            gate_sem,
            inc=1,
            device_id={"ctx": jnp.where(low, me - 2, lax.rem(me + 2, n))},
            device_id_type=pl.DeviceIdType.MESH,
        )

    landed(order_all.at[pl.ds(0, n - 1)], recv3)
    fetch = pltpu.make_async_copy(order_all, order_s, order_sem)
    fetch.start()
    fetch.wait()
    if levels > 2:

        @pl.when(jnp.logical_or(level == levels // 2 - 2, level == levels // 2 + 1))
        def _():
            with jax.named_scope("gate"):
                pl.semaphore_wait(gate_sem, 1)

    for j in range(parts):
        with jax.named_scope("waitfirst"):
            landed(got[j].at[pl.ds(0, (n - 1) * groups)], recv1.at[j])

        def pick(k, carry, j=j):
            there = 2 * lax.rem(k // 2 + jnp.where(low, levels // 2, 0), levels) + lax.rem(k + me, 2)

            @pl.when(there != me)
            def _():
                for g in range(groups):
                    stage[there, j, g] = got[j][order_s[there, 0, g]]
                second(there, j).start()

            @pl.when(there == me)
            def _():
                for g in range(groups):
                    final[me, j, g] = got[j][order_s[me, 0, g]]

            return carry

        with jax.named_scope("pick"):
            lax.fori_loop(0, n, pick, 0)
    tile = 32
    for j in range(parts):
        with jax.named_scope("waitsecond"):
            landed(final.at[pl.ds(0, n - 1), j], recv2.at[j])

        def add(r, carry, j=j):
            for g in range(groups):
                at = pl.ds(pl.multiple_of(r * tile, tile), tile)
                into = pl.ds(pl.multiple_of(g * GROUP + r * tile, tile), tile)
                total = jnp.zeros((tile, 128), jnp.float32) if j == 0 else squares[into, :]
                for s in range(n):
                    raw = final[s, j, g, at, :]
                    start = (2 * j + s % 2) * WIDE + s // 2 * piece
                    out_ref[into, start : start + piece] = raw
                    v = raw.astype(jnp.float32)
                    v = v * v
                    for q in range(0, piece, 128):
                        total = total + v[:, q : q + 128]
                squares[into, :] = total
            return carry

        with jax.named_scope("add"):
            lax.fori_loop(0, GROUP // tile, add, 0)

    with jax.named_scope("sent"):
        left(pair_out, link_send.at[0])
        left(fade_out, fade_send)

        @pl.when(level < levels - 1)
        def _():
            left(f_out, link_send.at[1])

        @pl.when(me != 1)
        def _():
            left(back, link_send.at[2])

        left(order_all.at[pl.ds(0, n - 1)], send3)
        left(made.at[pl.ds(0, half - 1)], send1.at[0])

        @pl.when(jnp.logical_not(inner))
        def _():
            left(made.at[pl.ds(0, half)], send1.at[1])

        left(stage.at[pl.ds(0, n - 1)], send2)


def scale_kernel(in_ref, squares_ref, weight_ref, out_hbm, ready, sem):
    rows, width = in_ref.shape
    tile = rows // sem.shape[0]

    def push(r):
        at = pl.ds(r * tile, tile)
        return pltpu.make_async_copy(ready.at[at, :], out_hbm.at[at, :], sem.at[r])

    for r in range(sem.shape[0]):
        at = slice(r * tile, (r + 1) * tile)
        total = jnp.sum(squares_ref[at, :], axis=1, keepdims=True)
        scale = lax.rsqrt(total * (1.0 / width) + 1e-05)
        for q in range(0, width, WIDE):
            cols = slice(q, q + WIDE)
            v = in_ref[at, cols].astype(jnp.float32)
            ready[at, cols] = (v * scale * weight_ref[:, cols]).astype(jnp.bfloat16)
        push(r).start()
    for r in range(sem.shape[0]):
        push(r).wait()


def norm_kernel(in_ref, weight_ref, out_ref):
    parts, rows, width = in_ref.shape
    tile = 32

    def one(r, carry):
        at = pl.ds(pl.multiple_of(r * tile, tile), tile)
        total = jnp.zeros((tile, 1), jnp.float32)
        for s in range(parts):
            v = in_ref[s, at, :].astype(jnp.float32)
            total = total + jnp.sum(v * v, axis=1, keepdims=True)
        scale = lax.rsqrt(total * (1.0 / (parts * width)) + 1e-05)
        for s in range(parts):
            v = in_ref[s, at, :].astype(jnp.float32)
            w = weight_ref[:, s * width : (s + 1) * width]
            out_ref[at, s * width : (s + 1) * width] = (v * scale * w).astype(jnp.bfloat16)
        return carry

    lax.fori_loop(0, rows // tile, one, 0)


def local(
    head_input,
    gate_input,
    write_vector,
    read_vector,
    increment_preactivation,
    step_bias,
    decay_log,
    skip_gain,
    norm_weight,
    doc_starts,
    block_order,
):
    devices = lax.axis_size("ctx")
    rows, features = head_input.shape
    heads = step_bias.shape[0]
    groups = rows // GROUP
    chunks = heads // CHUNK
    width = features // devices
    state_size = write_vector.shape[1]
    direct = width % WIDE == 0
    parts = devices if direct else 1
    limit = pltpu.CompilerParams(vmem_limit_bytes=48 * 1024 * 1024)
    common = [
        pltpu.VMEM((groups, chunks, GROUP, CHUNK), jnp.float32),
        pltpu.VMEM((groups, chunks, GROUP, CHUNK), jnp.float32),
        pltpu.VMEM((groups, state_size, GROUP), jnp.bfloat16),
    ]
    more = [
        pltpu.VMEM((groups, chunks, CHUNK, GROUP), jnp.float32),
        pltpu.VMEM((groups, chunks, CHUNK, GROUP), jnp.float32),
        pltpu.VMEM((chunks, 8, CHUNK), jnp.float32),
        pltpu.VMEM((groups, GROUP, GROUP), jnp.float32),
    ]
    bias, dlog, gain = (v.reshape(1, -1) for v in (step_bias, decay_log, skip_gain))

    def to_owners(v):
        if not direct:
            v = v.reshape(v.shape[1], devices, width).transpose(1, 0, 2)
        return lax.all_to_all(v, "ctx", split_axis=0, concat_axis=0, tiled=True)

    def joined(v):
        if not direct:
            v = v.transpose(1, 0, 2).reshape(1, v.shape[1], features)
        return v

    piece = width // PARTS
    per = max(WIDE // max(piece, 1), 1)
    if width == 512 and devices == 2 * per and chunks == 2 * PARTS:
        slab = (devices, PARTS, groups, GROUP, piece)
        links = features // UNIT // 2
        state = (links, state_size, UNIT)
        sems = pltpu.SemaphoreType.DMA
        packed, squares = pl.pallas_call(
            functools.partial(fused_kernel, devices, PARTS),
            out_shape=[
                pltpu.VMEM((rows, features), jnp.bfloat16),
                pltpu.VMEM((rows, 128), jnp.float32),
            ],
            in_specs=[ANY] * 2 + [VM] * 6 + [SM] * 2,
            out_specs=[VM] * 2,
            scratch_shapes=[
                pltpu.VMEM((rows, features), jnp.bfloat16),
                pltpu.VMEM((rows, features), jnp.bfloat16),
                pltpu.VMEM(state, jnp.bfloat16),
                pltpu.VMEM(state, jnp.bfloat16),
                pltpu.VMEM((8, 128), jnp.float32),
                pltpu.VMEM((8, 128), jnp.float32),
                pltpu.VMEM((links, 8, UNIT), jnp.float32),
                pltpu.VMEM(state, jnp.float32),
                pltpu.VMEM((links, 8, UNIT), jnp.float32),
            ]
            + [pltpu.VMEM(state, jnp.bfloat16)] * 5
            + [pltpu.VMEM(slab, jnp.bfloat16)] * 3
            + [
                pltpu.VMEM((8, 128), jnp.int32),
                pltpu.VMEM((devices, 8, 128), jnp.int32),
                pltpu.SMEM((devices, 8, 128), jnp.int32),
                sems((2, PARTS)),
                sems((3, links)),
                sems((3,)),
                sems,
                sems,
                sems((2,)),
                sems((PARTS,)),
                sems,
                sems((PARTS,)),
                sems,
                sems,
                sems,
                pltpu.SemaphoreType.REGULAR,
            ]
            + [pltpu.VMEM((devices * groups, GROUP, piece), jnp.bfloat16)] * PARTS
            + common
            + more,
            compiler_params=pltpu.CompilerParams(
                collective_id=0, has_side_effects=True, vmem_limit_bytes=LIMIT
            ),
            name="fused",
        )(
            head_input,
            gate_input,
            increment_preactivation.T,
            write_vector,
            read_vector,
            bias,
            dlog,
            gain,
            doc_starts,
            block_order,
        )
        return pl.pallas_call(
            scale_kernel,
            out_shape=jax.ShapeDtypeStruct((rows, features), jnp.bfloat16),
            in_specs=[VM] * 3,
            out_specs=ANY,
            scratch_shapes=[pltpu.VMEM((rows, features), jnp.bfloat16), sems((4,))],
            compiler_params=pltpu.CompilerParams(vmem_limit_bytes=8 * 1024 * 1024),
            name="scale",
        )(packed, squares, norm_weight.reshape(1, -1))

    ends = pl.pallas_call(
        state_kernel,
        out_shape=jax.ShapeDtypeStruct((parts, state_size + EXTRA, features // parts), jnp.bfloat16),
        in_specs=[VM] * 5 + [SM] * 2,
        out_specs=VM,
        scratch_shapes=common,
        compiler_params=limit,
        name="end_states",
    )(head_input, increment_preactivation.T, write_vector, bias, dlog, doc_starts, block_order)
    ends = to_owners(ends)
    all_order = ends[:, state_size + 2, :groups].astype(jnp.int32).reshape(-1)
    entry = pl.pallas_call(
        scan_kernel,
        out_shape=jax.ShapeDtypeStruct((devices, state_size, width), jnp.bfloat16),
        in_specs=[VM],
        out_specs=VM,
        compiler_params=limit,
        name="scan_states",
    )(ends)
    entry = joined(lax.all_to_all(entry, "ctx", split_axis=0, concat_axis=0, tiled=True))
    gated = pl.pallas_call(
        gated_kernel,
        out_shape=jax.ShapeDtypeStruct((parts, rows, features // parts), jnp.bfloat16),
        in_specs=[VM] * 9 + [SM],
        out_specs=VM,
        scratch_shapes=common
        + more,
        compiler_params=limit,
        name="gated",
    )(
        head_input,
        gate_input,
        increment_preactivation.T,
        write_vector,
        read_vector,
        entry,
        bias,
        dlog,
        gain,
        doc_starts,
    )
    gated = to_owners(gated)
    blocks = gated.reshape(devices * groups, GROUP, width)[all_order]
    packed = lax.all_to_all(
        blocks.reshape(devices, rows, width), "ctx", split_axis=0, concat_axis=0, tiled=True
    )
    return pl.pallas_call(
        norm_kernel,
        out_shape=jax.ShapeDtypeStruct((rows, features), jnp.bfloat16),
        in_specs=[VM] * 2,
        out_specs=VM,
        compiler_params=limit,
        name="norm",
    )(joined(packed), norm_weight.reshape(1, -1))


def solution(mesh):
    return jax.shard_map(
        local,
        mesh=mesh,
        in_specs=(
            P(("dp", "ctx"), None),
            P(("dp", "ctx"), None),
            P(("dp", "ctx"), None),
            P(("dp", "ctx"), None),
            P(("dp", "ctx"), None),
            P(),
            P(),
            P(),
            P(),
            P(("dp", "ctx")),
            P(("dp", "ctx")),
        ),
        out_specs=P(("dp", "ctx"), None),
        check_vma=False,
    )
```

```python
import functools

import jax
import jax.numpy as jnp
from jax import lax
from jax.experimental import pallas as pl
from jax.experimental.pallas import tpu as pltpu
from jax.sharding import PartitionSpec as P

HEAD_DIM = 64
GROUP = 128
CHUNK = 8
WIDE = CHUNK * HEAD_DIM
EXTRA = 16
PARTS = 4
LIMIT = 61 * 1024 * 1024
UNIT = 128

highest = lax.Precision.HIGHEST
VM = pl.BlockSpec(memory_space=pltpu.VMEM)
SM = pl.BlockSpec(memory_space=pltpu.SMEM)
ANY = pl.BlockSpec(memory_space=pltpu.HBM)


def transposed(v):
    rows, cols = v.shape
    if cols < 128:
        v = jnp.concatenate([v, jnp.zeros((rows, 128 - cols), v.dtype)], axis=1)
    return v.T[:cols]


def upright(v):
    rows, cols = v.shape
    if rows < 128:
        v = jnp.concatenate([v, jnp.zeros((128 - rows, cols), v.dtype)], axis=0)
    return v.T[:, :rows]


def lower_mask():
    row = lax.broadcasted_iota(jnp.int32, (GROUP, GROUP), 0)
    col = lax.broadcasted_iota(jnp.int32, (GROUP, GROUP), 1)
    return row >= col


def step_terms(logit_ref, bias_ref, dlog_ref):
    raw = logit_ref[...].astype(jnp.float32)
    raw = jnp.concatenate([upright(raw[:, k : k + GROUP]) for k in range(0, raw.shape[1], GROUP)], axis=0)
    v = raw + bias_ref[...]
    dt = jnp.maximum(v, 0.0) + jnp.log(1.0 + jnp.exp(-jnp.abs(v)))
    return dt, -dt * jnp.exp(dlog_ref[...])


def spread(v):
    rows = v.shape[0]
    first = lax.broadcasted_iota(jnp.int32, (rows, 128), 1) < HEAD_DIM
    return jnp.concatenate(
        [
            jnp.where(first, v[:, k : k + 1], v[:, k + 1 : k + 2])
            for k in range(0, CHUNK, 2)
        ],
        axis=1,
    )


def prepare(logit_ref, bias_ref, dlog_ref, write_ref, cum_s, dt_s, write_t):
    heads = bias_ref.shape[1]
    dt, fall = step_terms(logit_ref, bias_ref, dlog_ref)
    tri = lower_mask().astype(jnp.float32)
    cums = []
    for g in range(write_t.shape[0]):
        rows = slice(g * GROUP, (g + 1) * GROUP)
        cum = jnp.dot(tri, fall[rows], precision=highest, preferred_element_type=jnp.float32)
        cums.append(cum)
        for c in range(heads // CHUNK):
            cum_s[g, c] = cum[:, c * CHUNK : (c + 1) * CHUNK]
            dt_s[g, c] = dt[rows, c * CHUNK : (c + 1) * CHUNK]
        write_t[g] = write_ref[rows, :].astype(jnp.float32).T.astype(jnp.bfloat16)
    return dt, cums


def group_state(g, c, x, cum_s, dt_s, write_t):
    cum = cum_s[g, c]
    last = cum[GROUP - 1 : GROUP]
    tail = jnp.exp(last - cum) * dt_s[g, c]
    scaled = (x.astype(jnp.float32) * spread(tail)).astype(jnp.bfloat16)
    state = jnp.dot(write_t[g], scaled, preferred_element_type=jnp.float32)
    return state, spread(jnp.exp(last))


def state_kernel(
    x_ref, logit_ref, write_ref, bias_ref, dlog_ref, starts_ref, order_ref, out_ref, cum_s, dt_s, write_t
):
    groups = write_t.shape[0]
    prepare(logit_ref, bias_ref, dlog_ref, write_ref, cum_s, dt_s, write_t)
    parts, _, width = out_ref.shape
    chunks = cum_s.shape[1]
    per = width // WIDE

    def one(c, carry):
        cols = pl.ds(pl.multiple_of(c * WIDE, WIDE), WIDE)
        total, decay = None, None
        for g in range(groups):
            x = x_ref[g * GROUP : (g + 1) * GROUP, cols]
            state, last = group_state(g, c, x, cum_s, dt_s, write_t)
            keep = 1.0 - starts_ref[g].astype(jnp.float32)
            factor = keep * last
            total = state if total is None else factor * total + state
            decay = factor if decay is None else factor * decay
        coarse = decay.astype(jnp.bfloat16)
        fine = (decay - coarse.astype(jnp.float32)).astype(jnp.bfloat16)
        row = lax.broadcasted_iota(jnp.int32, (EXTRA, WIDE), 0)
        lane = lax.broadcasted_iota(jnp.int32, (EXTRA, WIDE), 1)
        order = jnp.zeros((EXTRA, WIDE), jnp.float32)
        for g in range(groups):
            order = jnp.where(lane == g, order_ref[g].astype(jnp.float32), order)
        extra = jnp.where(
            row == 0,
            coarse.astype(jnp.float32),
            jnp.where(row == 1, fine.astype(jnp.float32), order),
        )
        full = jnp.concatenate([total, extra], axis=0).astype(jnp.bfloat16)
        if parts == 1:
            out_ref[0, :, cols] = full
        else:
            into = pl.ds(pl.multiple_of((c % per) * WIDE, WIDE), WIDE)
            out_ref[c // per, :, into] = full
        return carry

    lax.fori_loop(0, chunks, one, 0)


def scan_kernel(in_ref, out_ref):
    parts, _, width = in_ref.shape
    state = jnp.zeros((GROUP, width), jnp.float32)
    for s in range(parts):
        out_ref[s] = state.astype(jnp.bfloat16)
        extra = in_ref[s, GROUP : GROUP + EXTRA, :].astype(jnp.float32)
        decay = extra[0:1] + extra[1:2]
        state = decay * state + in_ref[s, :GROUP, :].astype(jnp.float32)


def gated_setup(
    logit_ref, bias_ref, dlog_ref, write_ref, read_ref, gain_ref, cum_s, dt_s, write_t, cum_t, dt_t, gain_s, score_s
):
    dt, cums = prepare(logit_ref, bias_ref, dlog_ref, write_ref, cum_s, dt_s, write_t)
    score_setup(dt, cums, read_ref, gain_ref, cum_s, write_t, cum_t, dt_t, gain_s, score_s)


def score_setup(dt, cums, read_ref, gain_ref, cum_s, write_t, cum_t, dt_t, gain_s, score_s):
    groups, chunks = cum_s.shape[:2]
    mask = lower_mask()
    for g in range(groups):
        rows = slice(g * GROUP, (g + 1) * GROUP)
        ct = transposed(cums[g])
        dtt = transposed(dt[rows])
        for c in range(chunks):
            cum_t[g, c] = ct[c * CHUNK : (c + 1) * CHUNK]
            dt_t[g, c] = dtt[c * CHUNK : (c + 1) * CHUNK]
        score = jnp.dot(read_ref[rows, :], write_t[g], preferred_element_type=jnp.float32)
        score_s[g] = jnp.where(mask, score, 0.0)
    for c in range(chunks):
        gain_s[c] = jnp.broadcast_to(gain_ref[:, c * CHUNK : (c + 1) * CHUNK], (8, CHUNK))


def gated_chunk(
    c, state, put, x_ref, gate_ref, read_ref, starts_ref, cum_s, dt_s, write_t, cum_t, dt_t, gain_s, score_s
):
    groups = cum_s.shape[0]
    first = lax.broadcasted_iota(jnp.int32, (GROUP, 128), 1) < HEAD_DIM
    cols = pl.ds(pl.multiple_of(c * WIDE, WIDE), WIDE)
    gain = spread(gain_s[c][0:1])
    for g in range(groups):
        rows = slice(g * GROUP, (g + 1) * GROUP)
        x = x_ref[rows, cols]
        keep = 1.0 - starts_ref[g].astype(jnp.float32)
        entering = (keep * state).astype(jnp.bfloat16)
        cum = cum_s[g, c]
        carried = jnp.dot(read_ref[rows, :], entering, preferred_element_type=jnp.float32)
        mixed = carried * spread(jnp.exp(cum)) + gain * x.astype(jnp.float32)
        score = score_s[g]
        ct, dtt = cum_t[g, c], dt_t[g, c]
        pieces = []
        for k in range(0, CHUNK, 2):
            pair = x[:, k * HEAD_DIM : (k + 2) * HEAD_DIM]
            both = []
            for h in (k, k + 1):
                gap = cum[:, h : h + 1] - ct[h : h + 1]
                weight = score * jnp.exp(jnp.minimum(gap, 0.0)) * dtt[h : h + 1]
                both.append(
                    jnp.dot(weight.astype(jnp.bfloat16), pair, preferred_element_type=jnp.float32)
                )
            pieces.append(jnp.where(first, both[0], both[1]))
        mixed = mixed + jnp.concatenate(pieces, axis=1)
        gate = gate_ref[rows, cols].astype(jnp.float32)
        put(g, (mixed * (gate / (1.0 + jnp.exp(-gate)))).astype(jnp.bfloat16))
        if g + 1 < groups:
            own, last = group_state(g, c, x, cum_s, dt_s, write_t)
            state = keep * last * state + own


def gated_kernel(
    x_ref,
    gate_ref,
    logit_ref,
    write_ref,
    read_ref,
    entry_ref,
    bias_ref,
    dlog_ref,
    gain_ref,
    starts_ref,
    out_ref,
    *scratch,
):
    gated_setup(logit_ref, bias_ref, dlog_ref, write_ref, read_ref, gain_ref, *scratch)
    parts, _, width = out_ref.shape
    chunks = scratch[0].shape[1]
    per = width // WIDE

    def one(c, carry):
        cols = pl.ds(pl.multiple_of(c * WIDE, WIDE), WIDE)
        into = pl.ds(pl.multiple_of((c % per) * WIDE, WIDE), WIDE)
        if parts == 1:
            state = entry_ref[0, :, cols].astype(jnp.float32)
        else:
            state = entry_ref[c // per, :, into].astype(jnp.float32)

        def put(g, value):
            rows = slice(g * GROUP, (g + 1) * GROUP)
            if parts == 1:
                out_ref[0, rows, cols] = value
            else:
                out_ref[c // per, rows, into] = value

        gated_chunk(c, state, put, x_ref, gate_ref, read_ref, starts_ref, *scratch)
        return carry

    lax.fori_loop(0, chunks, one, 0)


def fused_kernel(
    n,
    parts,
    x_hbm,
    gate_hbm,
    logit_ref,
    write_ref,
    read_ref,
    bias_ref,
    dlog_ref,
    gain_ref,
    starts_ref,
    order_ref,
    out_ref,
    squares,
    x_ref,
    gate_ref,
    pair_out,
    pair_in,
    fade_out,
    fade_in,
    fade_s,
    total_s,
    decay_s,
    e_in,
    f_out,
    back,
    near_entry,
    far_entry,
    made,
    stage,
    final,
    order_own,
    order_all,
    order_s,
    load_sem,
    link_recv,
    give_recv,
    link_send,
    fade_send,
    fade_recv,
    send1,
    recv1,
    send2,
    recv2,
    send3,
    recv3,
    order_sem,
    gate_sem,
    ready_sem,
    side_sem,
    *rest,
):
    got, scratch = rest[:parts], rest[parts:]
    cum_s, dt_s, write_t = scratch[:3]
    groups, chunks = cum_s.shape[:2]
    piece = stage.shape[-1]
    per = WIDE // piece
    units = WIDE // UNIT
    span = 2 * WIDE
    me = lax.axis_index("ctx")
    side = me % 2
    level = me // 2
    levels = n // 2
    half = n // 2
    buddy = me + 1 - 2 * side
    low = level < levels // 2

    def send(source, target, sends, recvs, there):
        return pltpu.make_async_remote_copy(
            src_ref=source,
            dst_ref=target,
            send_sem=sends,
            recv_sem=recvs,
            device_id={"ctx": there},
            device_id_type=pl.DeviceIdType.MESH,
        )

    def landed(ref, sem):
        send(ref, ref, sem, sem, buddy).wait_recv()

    def left(ref, sem):
        send(ref, ref, sem, sem, buddy).wait_send()

    def load(which, j):
        cols = pl.ds(j * span, span)
        source, target = ((x_hbm, x_ref), (gate_hbm, gate_ref))[which]
        return pltpu.make_async_copy(source.at[:, cols], target.at[:, cols], load_sem.at[which, j])

    def pair(r):
        return send(pair_out.at[r], pair_in.at[r], link_send.at[0], link_recv.at[0, r], buddy)

    def chain(r):
        return send(f_out.at[r], e_in.at[r], link_send.at[1], link_recv.at[1, r], lax.rem(me + 2, n))

    def give(r):
        return send(back.at[r], far_entry.at[r], link_send.at[2], give_recv.at[r // units], buddy)

    def fade():
        return send(fade_out, fade_in, fade_send, fade_recv, buddy)

    def first(there, j):
        far = ((there < half) != low).astype(jnp.int32)
        return send(
            made.at[there, j], got[j].at[pl.ds(me * groups, groups)], send1.at[far], recv1.at[j], there
        )

    def second(there, j):
        return send(stage.at[there, j], final.at[me, j], send2, recv2.at[j], there)

    for j in range(parts):
        load(0, j).start()
    for j in range(parts):
        load(1, j).start()
    barrier = pltpu.get_barrier_semaphore()

    def tell(sem, there):
        pl.semaphore_signal(sem, inc=1, device_id={"ctx": there}, device_id_type=pl.DeviceIdType.MESH)

    above = level < levels - 1
    below = level > 0
    tell(barrier, buddy)

    @pl.when(above)
    def _():
        tell(barrier, lax.rem(me + 2, n))

    @pl.when(below)
    def _():
        tell(barrier, lax.rem(me + n - 2, n))

    def send_orders():
        for off in range(1, n):
            there = lax.rem(me + off, n)
            send(order_own, order_all.at[me], send3, recv3, there).start()

    with jax.named_scope("setup"):
        lane = lax.broadcasted_iota(jnp.int32, order_own.shape, 1)
        held = jnp.zeros(order_own.shape, jnp.int32)
        for g in range(groups):
            held = jnp.where(lane == g, order_ref[g], held)
        order_own[...] = held
        order_all[me] = held
        dt, cums = prepare(logit_ref, bias_ref, dlog_ref, write_ref, cum_s, dt_s, write_t)
        heads = bias_ref.shape[1]
        whole = None
        for g in range(groups):
            factor = (1.0 - starts_ref[g].astype(jnp.float32)) * jnp.exp(cums[g][GROUP - 1 : GROUP])
            whole = factor if whole is None else whole * factor
        whole = jnp.concatenate([whole, jnp.zeros((1, 128 - heads), jnp.float32)], axis=1)
        fade_out[...] = jnp.broadcast_to(whole, (8, 128))

    @pl.when(level == 0)
    def _():
        e_in[...] = jnp.zeros_like(e_in)

    @pl.when(me == 0)
    def _():
        far_entry[...] = jnp.zeros_like(far_entry)

    def ends(c, carry):
        cols = pl.ds(pl.multiple_of(c * WIDE, WIDE), WIDE)
        total, decay = None, None
        for g in range(groups):
            x = x_ref[g * GROUP : (g + 1) * GROUP, cols]
            state, last = group_state(g, c, x, cum_s, dt_s, write_t)
            factor = (1.0 - starts_ref[g].astype(jnp.float32)) * last
            total = state if total is None else factor * total + state
            decay = factor if decay is None else factor * decay
        base = c // 2 * units

        @pl.when(c % 2 == side)
        def _():
            for u in range(units):
                cut = slice(u * UNIT, (u + 1) * UNIT)
                total_s[base + u] = total[:, cut]
                decay_s[base + u] = jnp.broadcast_to(decay[:, cut], (8, UNIT))

        @pl.when(c % 2 != side)
        def _():
            for u in range(units):
                pair_out[base + u] = total[:, u * UNIT : (u + 1) * UNIT].astype(jnp.bfloat16)

        return carry

    def relay(r, carry):
        pair(r).wait_recv()

        @pl.when(level > 0)
        def _():
            chain(r).wait_recv()

        state = e_in[r].astype(jnp.float32)
        their = pair_in[r].astype(jnp.float32)
        theirs = fade_s[r][0:1]
        total, decay = total_s[r], decay_s[r][0:1]
        early = side == 0
        middle = jnp.where(early, decay, theirs) * state + jnp.where(early, total, their)

        @pl.when(level < levels - 1)
        def _():
            end = jnp.where(early, theirs, decay) * middle + jnp.where(early, their, total)
            f_out[r] = end.astype(jnp.bfloat16)
            chain(r).start()

        @pl.when(me != 1)
        def _():
            back[r] = jnp.where(early, middle, state).astype(jnp.bfloat16)
            give(r).start()

        near_entry[r] = jnp.where(early, state, middle).astype(jnp.bfloat16)
        return carry

    def links(j):
        with jax.named_scope("links"):
            lax.fori_loop(j * units, (j + 1) * units, relay, 0)

    def offer(j):
        for u in range(units):
            pair(j * units + u).start()

    def hear_above():
        with jax.named_scope("ready"):
            pl.semaphore_wait(ready_sem, 1)

    def swap_half(j):
        with jax.named_scope("ends"):
            ends(2 * j + 1 - side, 0)
        if j == 0:
            with jax.named_scope("barrier"):
                pl.semaphore_wait(barrier, 1 + above.astype(jnp.int32) + below.astype(jnp.int32))
            fade().start()
        offer(j)

    def keep_half(j):
        with jax.named_scope("ends"):
            ends(2 * j + side, 0)

    def by_distance(k):
        return jnp.where(low, levels - 1 - k, k)

    def gate_ready(j):
        for s in range(parts):

            @pl.when(j == s)
            def _():
                load(1, s).wait()

    def compute(j, i, entry):
        def put(g, value):
            for p in range(per):
                made[2 * p + i, j, g] = value[:, p * piece : (p + 1) * piece]

        with jax.named_scope("gated"):
            state = jnp.concatenate([entry[j * units + u].astype(jnp.float32) for u in range(units)], axis=1)
            gated_chunk(2 * j + i, state, put, x_ref, gate_ref, read_ref, starts_ref, *scratch)

    def outward(j, there, wanted):
        for s in range(parts):

            @pl.when(jnp.logical_and(j == s, jnp.logical_and(there != me, wanted)))
            def _():
                first(there, s).start()

    late = parts - 1
    for j in range(late):
        load(0, j).wait()
        swap_half(j)
        if j == 0:

            @pl.when(jnp.logical_and(below, level == levels - 2))
            def _():
                tell(ready_sem, me - 2)

            with jax.named_scope("scores"):
                score_setup(dt, cums, read_ref, gain_ref, cum_s, write_t, *scratch[3:])
        if j == 1:
            keep_half(0)
            keep_half(1)
    fade().wait_recv()
    tile = fade_in[0:1, :]
    for c in range(chunks):

        @pl.when(c % 2 == side)
        def _(c=c):
            lanes = spread(tile[:, c * CHUNK : (c + 1) * CHUNK])
            for u in range(units):
                fade_s[c // 2 * units + u] = jnp.broadcast_to(lanes[:, u * UNIT : (u + 1) * UNIT], (8, UNIT))

    @pl.when(jnp.logical_and(below, level < levels - 2))
    def _():
        hear_above()
        tell(ready_sem, me - 2)

    @pl.when(low)
    def _():
        links(0)

    bottom = jnp.logical_and(level == 0, levels > 2)

    @pl.when(bottom)
    def _():
        hear_above()
        load(1, 0).wait()
        compute(0, side, near_entry)
        for k in range(per):
            outward(0, 2 * k + side, k >= levels // 2)

    load(0, late).wait()
    swap_half(late)
    for j in range(2, parts):
        keep_half(j)

    @pl.when(low)
    def _():
        with jax.named_scope("linksall"):
            lax.fori_loop(units, parts * units, relay, 0)

        tell(side_sem, buddy)


    def near_column(j, carry):
        @pl.when(jnp.logical_not(low))
        def _():
            links(j)

        begun = jnp.logical_and(bottom, j == 0)

        @pl.when(jnp.logical_not(begun))
        def _():
            gate_ready(j)
            compute(j, side, near_entry)

        for k in range(per):
            there = 2 * by_distance(k) + side
            high = there // 2
            fresh = jnp.logical_not(jnp.logical_and(begun, high >= levels // 2))
            outward(j, there, jnp.logical_and(fresh, jnp.logical_or(low, high < level)))
        for s in range(parts):

            @pl.when(j == s)
            def _():
                for g in range(groups):
                    got[s][me * groups + g] = made[me, s, g]

        return carry

    def postponed(j, carry):
        for k in range(per):
            outward(j, 2 * k + side, jnp.logical_not(jnp.logical_or(low, k < level)))
        return carry

    def far_column(j, carry):
        @pl.when(me > 0)
        def _():
            with jax.named_scope("waitgive"):
                landed(far_entry.at[pl.ds(j * units, units)], give_recv.at[j])

        @pl.when(jnp.logical_and(j == 0, jnp.logical_not(low)))
        def _():
            send_orders()

        compute(j, 1 - side, far_entry)
        for k in range(per):
            outward(j, 2 * by_distance(k) + 1 - side, True)
        return carry

    lax.fori_loop(0, parts, near_column, 0)
    lax.fori_loop(0, parts, postponed, 0)

    @pl.when(low)
    def _():
        pl.semaphore_wait(side_sem, 1)
        send_orders()

    lax.fori_loop(0, parts, far_column, 0)

    lower_inner = jnp.logical_and(level == levels // 2 - 1, level > 0)
    upper_inner = jnp.logical_and(level == levels // 2, level < levels - 1)
    inner = jnp.logical_or(lower_inner, upper_inner)

    @pl.when(inner)
    def _():
        with jax.named_scope("crossed"):
            left(made.at[pl.ds(0, half)], send1.at[1])
        pl.semaphore_signal(
            gate_sem,
            inc=1,
            device_id={"ctx": jnp.where(low, me - 2, lax.rem(me + 2, n))},
            device_id_type=pl.DeviceIdType.MESH,
        )

    landed(order_all.at[pl.ds(0, n - 1)], recv3)
    fetch = pltpu.make_async_copy(order_all, order_s, order_sem)
    fetch.start()
    fetch.wait()
    if levels > 2:

        @pl.when(jnp.logical_or(level == levels // 2 - 2, level == levels // 2 + 1))
        def _():
            with jax.named_scope("gate"):
                pl.semaphore_wait(gate_sem, 1)

    for j in range(parts):
        with jax.named_scope("waitfirst"):
            landed(got[j].at[pl.ds(0, (n - 1) * groups)], recv1.at[j])

        def pick(k, carry, j=j):
            there = 2 * by_distance(k // 2) + lax.rem(k + 1 + me, 2)

            @pl.when(there != me)
            def _():
                for g in range(groups):
                    stage[there, j, g] = got[j][order_s[there, 0, g]]
                second(there, j).start()

            @pl.when(there == me)
            def _():
                for g in range(groups):
                    final[me, j, g] = got[j][order_s[me, 0, g]]

            return carry

        with jax.named_scope("pick"):
            lax.fori_loop(0, n, pick, 0)
    tile = 32
    for j in range(parts):
        with jax.named_scope("waitsecond"):
            landed(final.at[pl.ds(0, n - 1), j], recv2.at[j])

        def add(r, carry, j=j):
            for g in range(groups):
                at = pl.ds(pl.multiple_of(r * tile, tile), tile)
                into = pl.ds(pl.multiple_of(g * GROUP + r * tile, tile), tile)
                total = jnp.zeros((tile, 128), jnp.float32) if j == 0 else squares[into, :]
                for s in range(n):
                    raw = final[s, j, g, at, :]
                    start = (2 * j + s % 2) * WIDE + s // 2 * piece
                    out_ref[into, start : start + piece] = raw
                    v = raw.astype(jnp.float32)
                    v = v * v
                    for q in range(0, piece, 128):
                        total = total + v[:, q : q + 128]
                squares[into, :] = total
            return carry

        with jax.named_scope("add"):
            lax.fori_loop(0, GROUP // tile, add, 0)

    with jax.named_scope("sent"):
        left(pair_out, link_send.at[0])
        left(fade_out, fade_send)

        @pl.when(level < levels - 1)
        def _():
            left(f_out, link_send.at[1])

        @pl.when(me != 1)
        def _():
            left(back, link_send.at[2])

        left(order_all.at[pl.ds(0, n - 1)], send3)
        left(made.at[pl.ds(0, half - 1)], send1.at[0])

        @pl.when(jnp.logical_not(inner))
        def _():
            left(made.at[pl.ds(0, half)], send1.at[1])

        left(stage.at[pl.ds(0, n - 1)], send2)


def scale_kernel(in_ref, squares_ref, weight_ref, out_hbm, ready, sem):
    rows, width = in_ref.shape
    tile = rows // sem.shape[0]

    def push(r):
        at = pl.ds(r * tile, tile)
        return pltpu.make_async_copy(ready.at[at, :], out_hbm.at[at, :], sem.at[r])

    for r in range(sem.shape[0]):
        at = slice(r * tile, (r + 1) * tile)
        total = jnp.sum(squares_ref[at, :], axis=1, keepdims=True)
        scale = lax.rsqrt(total * (1.0 / width) + 1e-05)
        for q in range(0, width, WIDE):
            cols = slice(q, q + WIDE)
            v = in_ref[at, cols].astype(jnp.float32)
            ready[at, cols] = (v * scale * weight_ref[:, cols]).astype(jnp.bfloat16)
        push(r).start()
    for r in range(sem.shape[0]):
        push(r).wait()


def norm_kernel(in_ref, weight_ref, out_ref):
    parts, rows, width = in_ref.shape
    tile = 32

    def one(r, carry):
        at = pl.ds(pl.multiple_of(r * tile, tile), tile)
        total = jnp.zeros((tile, 1), jnp.float32)
        for s in range(parts):
            v = in_ref[s, at, :].astype(jnp.float32)
            total = total + jnp.sum(v * v, axis=1, keepdims=True)
        scale = lax.rsqrt(total * (1.0 / (parts * width)) + 1e-05)
        for s in range(parts):
            v = in_ref[s, at, :].astype(jnp.float32)
            w = weight_ref[:, s * width : (s + 1) * width]
            out_ref[at, s * width : (s + 1) * width] = (v * scale * w).astype(jnp.bfloat16)
        return carry

    lax.fori_loop(0, rows // tile, one, 0)


def local(
    head_input,
    gate_input,
    write_vector,
    read_vector,
    increment_preactivation,
    step_bias,
    decay_log,
    skip_gain,
    norm_weight,
    doc_starts,
    block_order,
):
    devices = lax.axis_size("ctx")
    rows, features = head_input.shape
    heads = step_bias.shape[0]
    groups = rows // GROUP
    chunks = heads // CHUNK
    width = features // devices
    state_size = write_vector.shape[1]
    direct = width % WIDE == 0
    parts = devices if direct else 1
    limit = pltpu.CompilerParams(vmem_limit_bytes=48 * 1024 * 1024)
    common = [
        pltpu.VMEM((groups, chunks, GROUP, CHUNK), jnp.float32),
        pltpu.VMEM((groups, chunks, GROUP, CHUNK), jnp.float32),
        pltpu.VMEM((groups, state_size, GROUP), jnp.bfloat16),
    ]
    more = [
        pltpu.VMEM((groups, chunks, CHUNK, GROUP), jnp.float32),
        pltpu.VMEM((groups, chunks, CHUNK, GROUP), jnp.float32),
        pltpu.VMEM((chunks, 8, CHUNK), jnp.float32),
        pltpu.VMEM((groups, GROUP, GROUP), jnp.float32),
    ]
    bias, dlog, gain = (v.reshape(1, -1) for v in (step_bias, decay_log, skip_gain))

    def to_owners(v):
        if not direct:
            v = v.reshape(v.shape[1], devices, width).transpose(1, 0, 2)
        return lax.all_to_all(v, "ctx", split_axis=0, concat_axis=0, tiled=True)

    def joined(v):
        if not direct:
            v = v.transpose(1, 0, 2).reshape(1, v.shape[1], features)
        return v

    piece = width // PARTS
    per = max(WIDE // max(piece, 1), 1)
    if width == 512 and devices == 2 * per and chunks == 2 * PARTS:
        slab = (devices, PARTS, groups, GROUP, piece)
        links = features // UNIT // 2
        state = (links, state_size, UNIT)
        sems = pltpu.SemaphoreType.DMA
        packed, squares = pl.pallas_call(
            functools.partial(fused_kernel, devices, PARTS),
            out_shape=[
                pltpu.VMEM((rows, features), jnp.bfloat16),
                pltpu.VMEM((rows, 128), jnp.float32),
            ],
            in_specs=[ANY] * 2 + [VM] * 6 + [SM] * 2,
            out_specs=[VM] * 2,
            scratch_shapes=[
                pltpu.VMEM((rows, features), jnp.bfloat16),
                pltpu.VMEM((rows, features), jnp.bfloat16),
                pltpu.VMEM(state, jnp.bfloat16),
                pltpu.VMEM(state, jnp.bfloat16),
                pltpu.VMEM((8, 128), jnp.float32),
                pltpu.VMEM((8, 128), jnp.float32),
                pltpu.VMEM((links, 8, UNIT), jnp.float32),
                pltpu.VMEM(state, jnp.float32),
                pltpu.VMEM((links, 8, UNIT), jnp.float32),
            ]
            + [pltpu.VMEM(state, jnp.bfloat16)] * 5
            + [pltpu.VMEM(slab, jnp.bfloat16)] * 3
            + [
                pltpu.VMEM((8, 128), jnp.int32),
                pltpu.VMEM((devices, 8, 128), jnp.int32),
                pltpu.SMEM((devices, 8, 128), jnp.int32),
                sems((2, PARTS)),
                sems((2, links)),
                sems((PARTS,)),
                sems((3,)),
                sems,
                sems,
                sems((2,)),
                sems((PARTS,)),
                sems,
                sems((PARTS,)),
                sems,
                sems,
                sems,
            ]
            + [pltpu.SemaphoreType.REGULAR] * 3
            + [pltpu.VMEM((devices * groups, GROUP, piece), jnp.bfloat16)] * PARTS
            + common
            + more,
            compiler_params=pltpu.CompilerParams(
                collective_id=0, has_side_effects=True, vmem_limit_bytes=LIMIT
            ),
            name="fused",
        )(
            head_input,
            gate_input,
            increment_preactivation.T,
            write_vector,
            read_vector,
            bias,
            dlog,
            gain,
            doc_starts,
            block_order,
        )
        return pl.pallas_call(
            scale_kernel,
            out_shape=jax.ShapeDtypeStruct((rows, features), jnp.bfloat16),
            in_specs=[VM] * 3,
            out_specs=ANY,
            scratch_shapes=[pltpu.VMEM((rows, features), jnp.bfloat16), sems((4,))],
            compiler_params=pltpu.CompilerParams(vmem_limit_bytes=8 * 1024 * 1024),
            name="scale",
        )(packed, squares, norm_weight.reshape(1, -1))

    ends = pl.pallas_call(
        state_kernel,
        out_shape=jax.ShapeDtypeStruct((parts, state_size + EXTRA, features // parts), jnp.bfloat16),
        in_specs=[VM] * 5 + [SM] * 2,
        out_specs=VM,
        scratch_shapes=common,
        compiler_params=limit,
        name="end_states",
    )(head_input, increment_preactivation.T, write_vector, bias, dlog, doc_starts, block_order)
    ends = to_owners(ends)
    all_order = ends[:, state_size + 2, :groups].astype(jnp.int32).reshape(-1)
    entry = pl.pallas_call(
        scan_kernel,
        out_shape=jax.ShapeDtypeStruct((devices, state_size, width), jnp.bfloat16),
        in_specs=[VM],
        out_specs=VM,
        compiler_params=limit,
        name="scan_states",
    )(ends)
    entry = joined(lax.all_to_all(entry, "ctx", split_axis=0, concat_axis=0, tiled=True))
    gated = pl.pallas_call(
        gated_kernel,
        out_shape=jax.ShapeDtypeStruct((parts, rows, features // parts), jnp.bfloat16),
        in_specs=[VM] * 9 + [SM],
        out_specs=VM,
        scratch_shapes=common
        + more,
        compiler_params=limit,
        name="gated",
    )(
        head_input,
        gate_input,
        increment_preactivation.T,
        write_vector,
        read_vector,
        entry,
        bias,
        dlog,
        gain,
        doc_starts,
    )
    gated = to_owners(gated)
    blocks = gated.reshape(devices * groups, GROUP, width)[all_order]
    packed = lax.all_to_all(
        blocks.reshape(devices, rows, width), "ctx", split_axis=0, concat_axis=0, tiled=True
    )
    return pl.pallas_call(
        norm_kernel,
        out_shape=jax.ShapeDtypeStruct((rows, features), jnp.bfloat16),
        in_specs=[VM] * 2,
        out_specs=VM,
        compiler_params=limit,
        name="norm",
    )(joined(packed), norm_weight.reshape(1, -1))


def solution(mesh):
    return jax.shard_map(
        local,
        mesh=mesh,
        in_specs=(
            P(("dp", "ctx"), None),
            P(("dp", "ctx"), None),
            P(("dp", "ctx"), None),
            P(("dp", "ctx"), None),
            P(("dp", "ctx"), None),
            P(),
            P(),
            P(),
            P(),
            P(("dp", "ctx")),
            P(("dp", "ctx")),
        ),
        out_specs=P(("dp", "ctx"), None),
        check_vma=False,
    )
```

```python
import functools

import jax
import jax.numpy as jnp
from jax import lax
from jax.experimental import pallas as pl
from jax.experimental.pallas import tpu as pltpu
from jax.sharding import PartitionSpec as P

HEAD_DIM = 64
GROUP = 128
CHUNK = 8
WIDE = CHUNK * HEAD_DIM
EXTRA = 16
PARTS = 4
LIMIT = 61 * 1024 * 1024
UNIT = 128

highest = lax.Precision.HIGHEST
VM = pl.BlockSpec(memory_space=pltpu.VMEM)
SM = pl.BlockSpec(memory_space=pltpu.SMEM)
ANY = pl.BlockSpec(memory_space=pltpu.HBM)


def transposed(v):
    rows, cols = v.shape
    if cols < 128:
        v = jnp.concatenate([v, jnp.zeros((rows, 128 - cols), v.dtype)], axis=1)
    return v.T[:cols]


def upright(v):
    rows, cols = v.shape
    if rows < 128:
        v = jnp.concatenate([v, jnp.zeros((128 - rows, cols), v.dtype)], axis=0)
    return v.T[:, :rows]


def lower_mask():
    row = lax.broadcasted_iota(jnp.int32, (GROUP, GROUP), 0)
    col = lax.broadcasted_iota(jnp.int32, (GROUP, GROUP), 1)
    return row >= col


def step_terms(logit_ref, bias_ref, dlog_ref):
    raw = logit_ref[...].astype(jnp.float32)
    raw = jnp.concatenate([upright(raw[:, k : k + GROUP]) for k in range(0, raw.shape[1], GROUP)], axis=0)
    v = raw + bias_ref[...]
    dt = jnp.maximum(v, 0.0) + jnp.log(1.0 + jnp.exp(-jnp.abs(v)))
    return dt, -dt * jnp.exp(dlog_ref[...])


def spread(v):
    rows = v.shape[0]
    first = lax.broadcasted_iota(jnp.int32, (rows, 128), 1) < HEAD_DIM
    return jnp.concatenate(
        [
            jnp.where(first, v[:, k : k + 1], v[:, k + 1 : k + 2])
            for k in range(0, CHUNK, 2)
        ],
        axis=1,
    )


def scatter(dt, cums, cum_s, dt_s, some):
    for g in range(len(cums)):
        rows = slice(g * GROUP, (g + 1) * GROUP)
        for c in some:
            cum_s[g, c] = cums[g][:, c * CHUNK : (c + 1) * CHUNK]
            dt_s[g, c] = dt[rows, c * CHUNK : (c + 1) * CHUNK]


def prepare(logit_ref, bias_ref, dlog_ref, write_ref, cum_s, dt_s, write_t, some=None):
    heads = bias_ref.shape[1]
    dt, fall = step_terms(logit_ref, bias_ref, dlog_ref)
    tri = lower_mask().astype(jnp.float32)
    cums = []
    for g in range(write_t.shape[0]):
        rows = slice(g * GROUP, (g + 1) * GROUP)
        cum = jnp.dot(tri, fall[rows], precision=highest, preferred_element_type=jnp.float32)
        cums.append(cum)
        write_t[g] = write_ref[rows, :].astype(jnp.float32).T.astype(jnp.bfloat16)
    scatter(dt, cums, cum_s, dt_s, range(heads // CHUNK) if some is None else some)
    return dt, cums


def group_state(g, c, x, cum_s, dt_s, write_t):
    cum = cum_s[g, c]
    last = cum[GROUP - 1 : GROUP]
    tail = jnp.exp(last - cum) * dt_s[g, c]
    scaled = (x.astype(jnp.float32) * spread(tail)).astype(jnp.bfloat16)
    state = jnp.dot(write_t[g], scaled, preferred_element_type=jnp.float32)
    return state, spread(jnp.exp(last))


def state_kernel(
    x_ref, logit_ref, write_ref, bias_ref, dlog_ref, starts_ref, order_ref, out_ref, cum_s, dt_s, write_t
):
    groups = write_t.shape[0]
    prepare(logit_ref, bias_ref, dlog_ref, write_ref, cum_s, dt_s, write_t)
    parts, _, width = out_ref.shape
    chunks = cum_s.shape[1]
    per = width // WIDE

    def one(c, carry):
        cols = pl.ds(pl.multiple_of(c * WIDE, WIDE), WIDE)
        total, decay = None, None
        for g in range(groups):
            x = x_ref[g * GROUP : (g + 1) * GROUP, cols]
            state, last = group_state(g, c, x, cum_s, dt_s, write_t)
            keep = 1.0 - starts_ref[g].astype(jnp.float32)
            factor = keep * last
            total = state if total is None else factor * total + state
            decay = factor if decay is None else factor * decay
        coarse = decay.astype(jnp.bfloat16)
        fine = (decay - coarse.astype(jnp.float32)).astype(jnp.bfloat16)
        row = lax.broadcasted_iota(jnp.int32, (EXTRA, WIDE), 0)
        lane = lax.broadcasted_iota(jnp.int32, (EXTRA, WIDE), 1)
        order = jnp.zeros((EXTRA, WIDE), jnp.float32)
        for g in range(groups):
            order = jnp.where(lane == g, order_ref[g].astype(jnp.float32), order)
        extra = jnp.where(
            row == 0,
            coarse.astype(jnp.float32),
            jnp.where(row == 1, fine.astype(jnp.float32), order),
        )
        full = jnp.concatenate([total, extra], axis=0).astype(jnp.bfloat16)
        if parts == 1:
            out_ref[0, :, cols] = full
        else:
            into = pl.ds(pl.multiple_of((c % per) * WIDE, WIDE), WIDE)
            out_ref[c // per, :, into] = full
        return carry

    lax.fori_loop(0, chunks, one, 0)


def scan_kernel(in_ref, out_ref):
    parts, _, width = in_ref.shape
    state = jnp.zeros((GROUP, width), jnp.float32)
    for s in range(parts):
        out_ref[s] = state.astype(jnp.bfloat16)
        extra = in_ref[s, GROUP : GROUP + EXTRA, :].astype(jnp.float32)
        decay = extra[0:1] + extra[1:2]
        state = decay * state + in_ref[s, :GROUP, :].astype(jnp.float32)


def gated_setup(
    logit_ref, bias_ref, dlog_ref, write_ref, read_ref, gain_ref, cum_s, dt_s, write_t, cum_t, dt_t, gain_s, score_s
):
    dt, cums = prepare(logit_ref, bias_ref, dlog_ref, write_ref, cum_s, dt_s, write_t)
    score_setup(dt, cums, read_ref, gain_ref, cum_s, write_t, cum_t, dt_t, gain_s, score_s)


def score_setup(dt, cums, read_ref, gain_ref, cum_s, write_t, cum_t, dt_t, gain_s, score_s):
    groups, chunks = cum_s.shape[:2]
    mask = lower_mask()
    for g in range(groups):
        rows = slice(g * GROUP, (g + 1) * GROUP)
        ct = transposed(cums[g])
        dtt = transposed(dt[rows])
        for c in range(chunks):
            cum_t[g, c] = ct[c * CHUNK : (c + 1) * CHUNK]
            dt_t[g, c] = dtt[c * CHUNK : (c + 1) * CHUNK]
        score = jnp.dot(read_ref[rows, :], write_t[g], preferred_element_type=jnp.float32)
        score_s[g] = jnp.where(mask, score, 0.0)
    for c in range(chunks):
        gain_s[c] = jnp.broadcast_to(gain_ref[:, c * CHUNK : (c + 1) * CHUNK], (8, CHUNK))


def gated_chunk(
    c, state, put, x_ref, gate_ref, read_ref, starts_ref, cum_s, dt_s, write_t, cum_t, dt_t, gain_s, score_s
):
    groups = cum_s.shape[0]
    first = lax.broadcasted_iota(jnp.int32, (GROUP, 128), 1) < HEAD_DIM
    cols = pl.ds(pl.multiple_of(c * WIDE, WIDE), WIDE)
    gain = spread(gain_s[c][0:1])
    for g in range(groups):
        rows = slice(g * GROUP, (g + 1) * GROUP)
        x = x_ref[rows, cols]
        keep = 1.0 - starts_ref[g].astype(jnp.float32)
        entering = (keep * state).astype(jnp.bfloat16)
        cum = cum_s[g, c]
        carried = jnp.dot(read_ref[rows, :], entering, preferred_element_type=jnp.float32)
        mixed = carried * spread(jnp.exp(cum)) + gain * x.astype(jnp.float32)
        score = score_s[g]
        ct, dtt = cum_t[g, c], dt_t[g, c]
        pieces = []
        for k in range(0, CHUNK, 2):
            pair = x[:, k * HEAD_DIM : (k + 2) * HEAD_DIM]
            both = []
            for h in (k, k + 1):
                gap = cum[:, h : h + 1] - ct[h : h + 1]
                weight = score * jnp.exp(jnp.minimum(gap, 0.0)) * dtt[h : h + 1]
                both.append(
                    jnp.dot(weight.astype(jnp.bfloat16), pair, preferred_element_type=jnp.float32)
                )
            pieces.append(jnp.where(first, both[0], both[1]))
        mixed = mixed + jnp.concatenate(pieces, axis=1)
        gate = gate_ref[rows, cols].astype(jnp.float32)
        put(g, (mixed * (gate / (1.0 + jnp.exp(-gate)))).astype(jnp.bfloat16))
        if g + 1 < groups:
            own, last = group_state(g, c, x, cum_s, dt_s, write_t)
            state = keep * last * state + own


def gated_kernel(
    x_ref,
    gate_ref,
    logit_ref,
    write_ref,
    read_ref,
    entry_ref,
    bias_ref,
    dlog_ref,
    gain_ref,
    starts_ref,
    out_ref,
    *scratch,
):
    gated_setup(logit_ref, bias_ref, dlog_ref, write_ref, read_ref, gain_ref, *scratch)
    parts, _, width = out_ref.shape
    chunks = scratch[0].shape[1]
    per = width // WIDE

    def one(c, carry):
        cols = pl.ds(pl.multiple_of(c * WIDE, WIDE), WIDE)
        into = pl.ds(pl.multiple_of((c % per) * WIDE, WIDE), WIDE)
        if parts == 1:
            state = entry_ref[0, :, cols].astype(jnp.float32)
        else:
            state = entry_ref[c // per, :, into].astype(jnp.float32)

        def put(g, value):
            rows = slice(g * GROUP, (g + 1) * GROUP)
            if parts == 1:
                out_ref[0, rows, cols] = value
            else:
                out_ref[c // per, rows, into] = value

        gated_chunk(c, state, put, x_ref, gate_ref, read_ref, starts_ref, *scratch)
        return carry

    lax.fori_loop(0, chunks, one, 0)


def fused_kernel(
    n,
    parts,
    x_hbm,
    gate_hbm,
    logit_hbm,
    write_hbm,
    read_hbm,
    bias_hbm,
    dlog_hbm,
    gain_hbm,
    starts_hbm,
    order_hbm,
    out_ref,
    squares,
    logit_ref,
    write_ref,
    read_ref,
    bias_ref,
    dlog_ref,
    gain_ref,
    starts_ref,
    order_ref,
    small_sem,
    x_ref,
    gate_ref,
    pair_out,
    pair_in,
    fade_out,
    fade_in,
    fade_s,
    total_s,
    decay_s,
    e_in,
    f_out,
    back,
    near_entry,
    far_entry,
    made,
    stage,
    final,
    order_own,
    order_all,
    order_s,
    load_sem,
    link_recv,
    give_recv,
    link_send,
    fade_send,
    fade_recv,
    send1,
    recv1,
    send2,
    recv2,
    send3,
    recv3,
    order_sem,
    gate_sem,
    ready_sem,
    side_sem,
    *rest,
):
    got, scratch = rest[:parts], rest[parts:]
    cum_s, dt_s, write_t = scratch[:3]
    groups, chunks = cum_s.shape[:2]
    piece = stage.shape[-1]
    per = WIDE // piece
    units = WIDE // UNIT
    span = 2 * WIDE
    me = lax.axis_index("ctx")
    side = me % 2
    level = me // 2
    levels = n // 2
    half = n // 2
    buddy = me + 1 - 2 * side
    low = level < levels // 2

    def send(source, target, sends, recvs, there):
        return pltpu.make_async_remote_copy(
            src_ref=source,
            dst_ref=target,
            send_sem=sends,
            recv_sem=recvs,
            device_id={"ctx": there},
            device_id_type=pl.DeviceIdType.MESH,
        )

    def landed(ref, sem):
        send(ref, ref, sem, sem, buddy).wait_recv()

    def left(ref, sem):
        send(ref, ref, sem, sem, buddy).wait_send()

    def load(which, j):
        cols = pl.ds(j * span, span)
        source, target = ((x_hbm, x_ref), (gate_hbm, gate_ref))[which]
        return pltpu.make_async_copy(source.at[:, cols], target.at[:, cols], load_sem.at[which, j])

    def pair(r):
        return send(pair_out.at[r], pair_in.at[r], link_send.at[0], link_recv.at[0, r], buddy)

    def chain(r):
        return send(f_out.at[r], e_in.at[r], link_send.at[1], link_recv.at[1, r], lax.rem(me + 2, n))

    def give(r):
        return send(back.at[r], far_entry.at[r], link_send.at[2], give_recv.at[r // units], buddy)

    def fade():
        return send(fade_out, fade_in, fade_send, fade_recv, buddy)

    def first(there, j):
        far = ((there < half) != low).astype(jnp.int32)
        return send(
            made.at[there, j], got[j].at[pl.ds(me * groups, groups)], send1.at[far], recv1.at[j], there
        )

    def second(there, j):
        return send(stage.at[there, j], final.at[me, j], send2, recv2.at[j], there)

    barrier = pltpu.get_barrier_semaphore()

    def tell(sem, there):
        pl.semaphore_signal(sem, inc=1, device_id={"ctx": there}, device_id_type=pl.DeviceIdType.MESH)

    above = level < levels - 1
    below = level > 0
    tell(barrier, buddy)

    @pl.when(above)
    def _():
        tell(barrier, lax.rem(me + 2, n))

    @pl.when(below)
    def _():
        tell(barrier, lax.rem(me + n - 2, n))

    small = [
        pltpu.make_async_copy(source, target, small_sem.at[k])
        for k, (source, target) in enumerate(
            (
                (logit_hbm, logit_ref),
                (bias_hbm, bias_ref),
                (dlog_hbm, dlog_ref),
                (write_hbm, write_ref),
                (starts_hbm, starts_ref),
                (read_hbm, read_ref),
                (gain_hbm, gain_ref),
                (order_hbm, order_ref),
            )
        )
    ]
    for copy in small[:5]:
        copy.start()
    load(0, 0).start()
    for copy in small[5:]:
        copy.start()
    for copy in small[:4]:
        copy.wait()
    for j in range(1, parts):
        load(0, j).start()
    for j in range(parts):
        load(1, j).start()

    def send_orders():
        for off in range(1, n):
            there = lax.rem(me + off, n)
            send(order_own, order_all.at[me], send3, recv3, there).start()

    with jax.named_scope("setup"):
        dt, cums = prepare(logit_ref, bias_ref, dlog_ref, write_ref, cum_s, dt_s, write_t, range(2))
        heads = bias_ref.shape[1]
        small[4].wait()
        whole = None
        for g in range(groups):
            factor = (1.0 - starts_ref[g].astype(jnp.float32)) * jnp.exp(cums[g][GROUP - 1 : GROUP])
            whole = factor if whole is None else whole * factor
        whole = jnp.concatenate([whole, jnp.zeros((1, 128 - heads), jnp.float32)], axis=1)
        fade_out[...] = jnp.broadcast_to(whole, (8, 128))

    @pl.when(level == 0)
    def _():
        e_in[...] = jnp.zeros_like(e_in)

    @pl.when(me == 0)
    def _():
        far_entry[...] = jnp.zeros_like(far_entry)

    def ends(c, carry):
        cols = pl.ds(pl.multiple_of(c * WIDE, WIDE), WIDE)
        total, decay = None, None
        for g in range(groups):
            x = x_ref[g * GROUP : (g + 1) * GROUP, cols]
            state, last = group_state(g, c, x, cum_s, dt_s, write_t)
            factor = (1.0 - starts_ref[g].astype(jnp.float32)) * last
            total = state if total is None else factor * total + state
            decay = factor if decay is None else factor * decay
        base = c // 2 * units

        @pl.when(c % 2 == side)
        def _():
            for u in range(units):
                cut = slice(u * UNIT, (u + 1) * UNIT)
                total_s[base + u] = total[:, cut]
                decay_s[base + u] = jnp.broadcast_to(decay[:, cut], (8, UNIT))

        @pl.when(c % 2 != side)
        def _():
            for u in range(units):
                pair_out[base + u] = total[:, u * UNIT : (u + 1) * UNIT].astype(jnp.bfloat16)

        return carry

    def relay(r, carry):
        pair(r).wait_recv()

        @pl.when(level > 0)
        def _():
            chain(r).wait_recv()

        state = e_in[r].astype(jnp.float32)
        their = pair_in[r].astype(jnp.float32)
        theirs = fade_s[r][0:1]
        total, decay = total_s[r], decay_s[r][0:1]
        early = side == 0
        middle = jnp.where(early, decay, theirs) * state + jnp.where(early, total, their)

        @pl.when(level < levels - 1)
        def _():
            end = jnp.where(early, theirs, decay) * middle + jnp.where(early, their, total)
            f_out[r] = end.astype(jnp.bfloat16)
            chain(r).start()

        @pl.when(me != 1)
        def _():
            back[r] = jnp.where(early, middle, state).astype(jnp.bfloat16)
            give(r).start()

        near_entry[r] = jnp.where(early, state, middle).astype(jnp.bfloat16)
        return carry

    def links(j):
        with jax.named_scope("links"):
            lax.fori_loop(j * units, (j + 1) * units, relay, 0)

    def offer(j):
        for u in range(units):
            pair(j * units + u).start()

    def hear_above():
        with jax.named_scope("ready"):
            pl.semaphore_wait(ready_sem, 1)

    def swap_half(j):
        with jax.named_scope("ends"):
            ends(2 * j + 1 - side, 0)
        if j == 0:
            with jax.named_scope("barrier"):
                pl.semaphore_wait(barrier, 1 + above.astype(jnp.int32) + below.astype(jnp.int32))
            fade().start()
        offer(j)

    def keep_half(j):
        with jax.named_scope("ends"):
            ends(2 * j + side, 0)

    def by_distance(k):
        return jnp.where(low, levels - 1 - k, k)

    def gate_ready(j):
        for s in range(parts):

            @pl.when(j == s)
            def _():
                load(1, s).wait()

    def compute(j, i, entry):
        def put(g, value):
            for p in range(per):
                made[2 * p + i, j, g] = value[:, p * piece : (p + 1) * piece]

        with jax.named_scope("gated"):
            state = jnp.concatenate([entry[j * units + u].astype(jnp.float32) for u in range(units)], axis=1)
            gated_chunk(2 * j + i, state, put, x_ref, gate_ref, read_ref, starts_ref, *scratch)

    def outward(j, there, wanted):
        for s in range(parts):

            @pl.when(jnp.logical_and(j == s, jnp.logical_and(there != me, wanted)))
            def _():
                first(there, s).start()

    late = parts - 1
    for j in range(late):
        load(0, j).wait()
        swap_half(j)
        if j == 0:

            @pl.when(jnp.logical_and(below, level == levels - 2))
            def _():
                tell(ready_sem, me - 2)

            with jax.named_scope("scores"):
                for copy in small[5:]:
                    copy.wait()
                lane = lax.broadcasted_iota(jnp.int32, order_own.shape, 1)
                held = jnp.zeros(order_own.shape, jnp.int32)
                for g in range(groups):
                    held = jnp.where(lane == g, order_ref[g], held)
                order_own[...] = held
                order_all[me] = held
                scatter(dt, cums, cum_s, dt_s, range(2, chunks))
                score_setup(dt, cums, read_ref, gain_ref, cum_s, write_t, *scratch[3:])
        if j == 1:
            keep_half(0)
            keep_half(1)
    fade().wait_recv()
    tile = fade_in[0:1, :]
    for c in range(chunks):

        @pl.when(c % 2 == side)
        def _(c=c):
            lanes = spread(tile[:, c * CHUNK : (c + 1) * CHUNK])
            for u in range(units):
                fade_s[c // 2 * units + u] = jnp.broadcast_to(lanes[:, u * UNIT : (u + 1) * UNIT], (8, UNIT))

    @pl.when(jnp.logical_and(below, level < levels - 2))
    def _():
        hear_above()
        tell(ready_sem, me - 2)

    @pl.when(low)
    def _():
        links(0)

    bottom = jnp.logical_and(level == 0, levels > 2)

    @pl.when(bottom)
    def _():
        hear_above()
        load(1, 0).wait()
        compute(0, side, near_entry)
        for k in range(per):
            outward(0, 2 * k + side, k >= levels // 2)

    load(0, late).wait()
    swap_half(late)
    for j in range(2, parts):
        keep_half(j)

    @pl.when(low)
    def _():
        with jax.named_scope("linksall"):
            lax.fori_loop(units, parts * units, relay, 0)

        tell(side_sem, buddy)


    def near_column(j, carry):
        @pl.when(jnp.logical_not(low))
        def _():
            links(j)

        begun = jnp.logical_and(bottom, j == 0)

        @pl.when(jnp.logical_not(begun))
        def _():
            gate_ready(j)
            compute(j, side, near_entry)

        for k in range(per):
            there = 2 * by_distance(k) + side
            high = there // 2
            fresh = jnp.logical_not(jnp.logical_and(begun, high >= levels // 2))
            outward(j, there, jnp.logical_and(fresh, jnp.logical_or(low, high < level)))
        for s in range(parts):

            @pl.when(j == s)
            def _():
                for g in range(groups):
                    got[s][me * groups + g] = made[me, s, g]

        return carry

    def postponed(j, carry):
        for k in range(per):
            outward(j, 2 * k + side, jnp.logical_not(jnp.logical_or(low, k < level)))
        return carry

    def far_column(j, carry):
        @pl.when(me > 0)
        def _():
            with jax.named_scope("waitgive"):
                landed(far_entry.at[pl.ds(j * units, units)], give_recv.at[j])

        @pl.when(jnp.logical_and(j == 0, jnp.logical_not(low)))
        def _():
            send_orders()

        compute(j, 1 - side, far_entry)
        for k in range(per):
            outward(j, 2 * by_distance(k) + 1 - side, True)
        return carry

    lax.fori_loop(0, parts, near_column, 0)
    lax.fori_loop(0, parts, postponed, 0)

    @pl.when(low)
    def _():
        pl.semaphore_wait(side_sem, 1)
        send_orders()

    lax.fori_loop(0, parts, far_column, 0)

    lower_inner = jnp.logical_and(level == levels // 2 - 1, level > 0)
    upper_inner = jnp.logical_and(level == levels // 2, level < levels - 1)
    inner = jnp.logical_or(lower_inner, upper_inner)

    def crossed():
        with jax.named_scope("crossed"):
            left(made.at[pl.ds(0, half)], send1.at[1])
        tell(gate_sem, jnp.where(low, me - 2, lax.rem(me + 2, n)))

    landed(order_all.at[pl.ds(0, n - 1)], recv3)
    fetch = pltpu.make_async_copy(order_all, order_s, order_sem)
    fetch.start()
    fetch.wait()

    @pl.when(upper_inner)
    def _():
        crossed()

    if levels > 2:

        @pl.when(jnp.logical_or(level == levels // 2 - 2, level == levels // 2 + 1))
        def _():
            with jax.named_scope("gate"):
                pl.semaphore_wait(gate_sem, 1)

    for j in range(parts):
        with jax.named_scope("waitfirst"):
            landed(got[j].at[pl.ds(0, (n - 1) * groups)], recv1.at[j])

        def pick(k, carry, j=j):
            there = 2 * by_distance(k // 2) + lax.rem(k + 1 + me, 2)

            @pl.when(there != me)
            def _():
                for g in range(groups):
                    stage[there, j, g] = got[j][order_s[there, 0, g]]
                second(there, j).start()

            @pl.when(there == me)
            def _():
                for g in range(groups):
                    final[me, j, g] = got[j][order_s[me, 0, g]]

            return carry

        with jax.named_scope("pick"):
            lax.fori_loop(0, n, pick, 0)
        if j == parts - 2:

            @pl.when(lower_inner)
            def _():
                crossed()

    tile = 32
    for j in range(parts):
        with jax.named_scope("waitsecond"):
            landed(final.at[pl.ds(0, n - 1), j], recv2.at[j])

        def add(r, carry, j=j):
            for g in range(groups):
                at = pl.ds(pl.multiple_of(r * tile, tile), tile)
                into = pl.ds(pl.multiple_of(g * GROUP + r * tile, tile), tile)
                total = jnp.zeros((tile, 128), jnp.float32) if j == 0 else squares[into, :]
                for s in range(n):
                    raw = final[s, j, g, at, :]
                    start = (2 * j + s % 2) * WIDE + s // 2 * piece
                    out_ref[into, start : start + piece] = raw
                    v = raw.astype(jnp.float32)
                    v = v * v
                    for q in range(0, piece, 128):
                        total = total + v[:, q : q + 128]
                squares[into, :] = total
            return carry

        with jax.named_scope("add"):
            lax.fori_loop(0, GROUP // tile, add, 0)

    with jax.named_scope("sent"):
        left(pair_out, link_send.at[0])
        left(fade_out, fade_send)

        @pl.when(level < levels - 1)
        def _():
            left(f_out, link_send.at[1])

        @pl.when(me != 1)
        def _():
            left(back, link_send.at[2])

        left(order_all.at[pl.ds(0, n - 1)], send3)
        left(made.at[pl.ds(0, half - 1)], send1.at[0])

        @pl.when(jnp.logical_not(inner))
        def _():
            left(made.at[pl.ds(0, half)], send1.at[1])

        left(stage.at[pl.ds(0, n - 1)], send2)


def scale_kernel(in_ref, squares_ref, weight_ref, out_hbm, ready, sem):
    rows, width = in_ref.shape
    tile = rows // sem.shape[0]

    def push(r):
        at = pl.ds(r * tile, tile)
        return pltpu.make_async_copy(ready.at[at, :], out_hbm.at[at, :], sem.at[r])

    for r in range(sem.shape[0]):
        at = slice(r * tile, (r + 1) * tile)
        total = jnp.sum(squares_ref[at, :], axis=1, keepdims=True)
        scale = lax.rsqrt(total * (1.0 / width) + 1e-05)
        for q in range(0, width, WIDE):
            cols = slice(q, q + WIDE)
            v = in_ref[at, cols].astype(jnp.float32)
            ready[at, cols] = (v * scale * weight_ref[:, cols]).astype(jnp.bfloat16)
        push(r).start()
    for r in range(sem.shape[0]):
        push(r).wait()


def norm_kernel(in_ref, weight_ref, out_ref):
    parts, rows, width = in_ref.shape
    tile = 32

    def one(r, carry):
        at = pl.ds(pl.multiple_of(r * tile, tile), tile)
        total = jnp.zeros((tile, 1), jnp.float32)
        for s in range(parts):
            v = in_ref[s, at, :].astype(jnp.float32)
            total = total + jnp.sum(v * v, axis=1, keepdims=True)
        scale = lax.rsqrt(total * (1.0 / (parts * width)) + 1e-05)
        for s in range(parts):
            v = in_ref[s, at, :].astype(jnp.float32)
            w = weight_ref[:, s * width : (s + 1) * width]
            out_ref[at, s * width : (s + 1) * width] = (v * scale * w).astype(jnp.bfloat16)
        return carry

    lax.fori_loop(0, rows // tile, one, 0)


def local(
    head_input,
    gate_input,
    write_vector,
    read_vector,
    increment_preactivation,
    step_bias,
    decay_log,
    skip_gain,
    norm_weight,
    doc_starts,
    block_order,
):
    devices = lax.axis_size("ctx")
    rows, features = head_input.shape
    heads = step_bias.shape[0]
    groups = rows // GROUP
    chunks = heads // CHUNK
    width = features // devices
    state_size = write_vector.shape[1]
    direct = width % WIDE == 0
    parts = devices if direct else 1
    limit = pltpu.CompilerParams(vmem_limit_bytes=48 * 1024 * 1024)
    common = [
        pltpu.VMEM((groups, chunks, GROUP, CHUNK), jnp.float32),
        pltpu.VMEM((groups, chunks, GROUP, CHUNK), jnp.float32),
        pltpu.VMEM((groups, state_size, GROUP), jnp.bfloat16),
    ]
    more = [
        pltpu.VMEM((groups, chunks, CHUNK, GROUP), jnp.float32),
        pltpu.VMEM((groups, chunks, CHUNK, GROUP), jnp.float32),
        pltpu.VMEM((chunks, 8, CHUNK), jnp.float32),
        pltpu.VMEM((groups, GROUP, GROUP), jnp.float32),
    ]
    bias, dlog, gain = (v.reshape(1, -1) for v in (step_bias, decay_log, skip_gain))

    def to_owners(v):
        if not direct:
            v = v.reshape(v.shape[1], devices, width).transpose(1, 0, 2)
        return lax.all_to_all(v, "ctx", split_axis=0, concat_axis=0, tiled=True)

    def joined(v):
        if not direct:
            v = v.transpose(1, 0, 2).reshape(1, v.shape[1], features)
        return v

    piece = width // PARTS
    per = max(WIDE // max(piece, 1), 1)
    if width == 512 and devices == 2 * per and chunks == 2 * PARTS:
        slab = (devices, PARTS, groups, GROUP, piece)
        links = features // UNIT // 2
        state = (links, state_size, UNIT)
        sems = pltpu.SemaphoreType.DMA
        packed, squares = pl.pallas_call(
            functools.partial(fused_kernel, devices, PARTS),
            out_shape=[
                pltpu.VMEM((rows, features), jnp.bfloat16),
                pltpu.VMEM((rows, 128), jnp.float32),
            ],
            in_specs=[ANY] * 10,
            out_specs=[VM] * 2,
            scratch_shapes=[
                pltpu.VMEM((heads, rows), jnp.bfloat16),
                pltpu.VMEM((rows, state_size), jnp.bfloat16),
                pltpu.VMEM((rows, state_size), jnp.bfloat16),
                pltpu.VMEM((1, heads), jnp.float32),
                pltpu.VMEM((1, heads), jnp.float32),
                pltpu.VMEM((1, heads), jnp.float32),
                pltpu.SMEM((groups,), jnp.int32),
                pltpu.SMEM((groups,), jnp.int32),
                sems((8,)),
                pltpu.VMEM((rows, features), jnp.bfloat16),
                pltpu.VMEM((rows, features), jnp.bfloat16),
                pltpu.VMEM(state, jnp.bfloat16),
                pltpu.VMEM(state, jnp.bfloat16),
                pltpu.VMEM((8, 128), jnp.float32),
                pltpu.VMEM((8, 128), jnp.float32),
                pltpu.VMEM((links, 8, UNIT), jnp.float32),
                pltpu.VMEM(state, jnp.float32),
                pltpu.VMEM((links, 8, UNIT), jnp.float32),
            ]
            + [pltpu.VMEM(state, jnp.bfloat16)] * 5
            + [pltpu.VMEM(slab, jnp.bfloat16)] * 3
            + [
                pltpu.VMEM((8, 128), jnp.int32),
                pltpu.VMEM((devices, 8, 128), jnp.int32),
                pltpu.SMEM((devices, 8, 128), jnp.int32),
                sems((2, PARTS)),
                sems((2, links)),
                sems((PARTS,)),
                sems((3,)),
                sems,
                sems,
                sems((2,)),
                sems((PARTS,)),
                sems,
                sems((PARTS,)),
                sems,
                sems,
                sems,
            ]
            + [pltpu.SemaphoreType.REGULAR] * 3
            + [pltpu.VMEM((devices * groups, GROUP, piece), jnp.bfloat16)] * PARTS
            + common
            + more,
            compiler_params=pltpu.CompilerParams(
                collective_id=0, has_side_effects=True, vmem_limit_bytes=LIMIT
            ),
            name="fused",
        )(
            head_input,
            gate_input,
            increment_preactivation.T,
            write_vector,
            read_vector,
            bias,
            dlog,
            gain,
            doc_starts,
            block_order,
        )
        return pl.pallas_call(
            scale_kernel,
            out_shape=jax.ShapeDtypeStruct((rows, features), jnp.bfloat16),
            in_specs=[VM] * 3,
            out_specs=ANY,
            scratch_shapes=[pltpu.VMEM((rows, features), jnp.bfloat16), sems((4,))],
            compiler_params=pltpu.CompilerParams(vmem_limit_bytes=8 * 1024 * 1024),
            name="scale",
        )(packed, squares, norm_weight.reshape(1, -1))

    ends = pl.pallas_call(
        state_kernel,
        out_shape=jax.ShapeDtypeStruct((parts, state_size + EXTRA, features // parts), jnp.bfloat16),
        in_specs=[VM] * 5 + [SM] * 2,
        out_specs=VM,
        scratch_shapes=common,
        compiler_params=limit,
        name="end_states",
    )(head_input, increment_preactivation.T, write_vector, bias, dlog, doc_starts, block_order)
    ends = to_owners(ends)
    all_order = ends[:, state_size + 2, :groups].astype(jnp.int32).reshape(-1)
    entry = pl.pallas_call(
        scan_kernel,
        out_shape=jax.ShapeDtypeStruct((devices, state_size, width), jnp.bfloat16),
        in_specs=[VM],
        out_specs=VM,
        compiler_params=limit,
        name="scan_states",
    )(ends)
    entry = joined(lax.all_to_all(entry, "ctx", split_axis=0, concat_axis=0, tiled=True))
    gated = pl.pallas_call(
        gated_kernel,
        out_shape=jax.ShapeDtypeStruct((parts, rows, features // parts), jnp.bfloat16),
        in_specs=[VM] * 9 + [SM],
        out_specs=VM,
        scratch_shapes=common
        + more,
        compiler_params=limit,
        name="gated",
    )(
        head_input,
        gate_input,
        increment_preactivation.T,
        write_vector,
        read_vector,
        entry,
        bias,
        dlog,
        gain,
        doc_starts,
    )
    gated = to_owners(gated)
    blocks = gated.reshape(devices * groups, GROUP, width)[all_order]
    packed = lax.all_to_all(
        blocks.reshape(devices, rows, width), "ctx", split_axis=0, concat_axis=0, tiled=True
    )
    return pl.pallas_call(
        norm_kernel,
        out_shape=jax.ShapeDtypeStruct((rows, features), jnp.bfloat16),
        in_specs=[VM] * 2,
        out_specs=VM,
        compiler_params=limit,
        name="norm",
    )(joined(packed), norm_weight.reshape(1, -1))


def solution(mesh):
    return jax.shard_map(
        local,
        mesh=mesh,
        in_specs=(
            P(("dp", "ctx"), None),
            P(("dp", "ctx"), None),
            P(("dp", "ctx"), None),
            P(("dp", "ctx"), None),
            P(("dp", "ctx"), None),
            P(),
            P(),
            P(),
            P(),
            P(("dp", "ctx")),
            P(("dp", "ctx")),
        ),
        out_specs=P(("dp", "ctx"), None),
        check_vma=False,
    )
```

```python
import functools

import jax
import jax.numpy as jnp
from jax import lax
from jax.experimental import pallas as pl
from jax.experimental.pallas import tpu as pltpu
from jax.sharding import PartitionSpec as P

HEAD_DIM = 64
GROUP = 128
CHUNK = 8
WIDE = CHUNK * HEAD_DIM
EXTRA = 16
PARTS = 4
LIMIT = 61 * 1024 * 1024
UNIT = 128

highest = lax.Precision.HIGHEST
VM = pl.BlockSpec(memory_space=pltpu.VMEM)
SM = pl.BlockSpec(memory_space=pltpu.SMEM)
ANY = pl.BlockSpec(memory_space=pltpu.HBM)


def transposed(v):
    rows, cols = v.shape
    if cols < 128:
        v = jnp.concatenate([v, jnp.zeros((rows, 128 - cols), v.dtype)], axis=1)
    return v.T[:cols]


def upright(v):
    rows, cols = v.shape
    if rows < 128:
        v = jnp.concatenate([v, jnp.zeros((128 - rows, cols), v.dtype)], axis=0)
    return v.T[:, :rows]


def lower_mask():
    row = lax.broadcasted_iota(jnp.int32, (GROUP, GROUP), 0)
    col = lax.broadcasted_iota(jnp.int32, (GROUP, GROUP), 1)
    return row >= col


def step_terms(logit_ref, bias_ref, dlog_ref):
    raw = logit_ref[...].astype(jnp.float32)
    raw = jnp.concatenate([upright(raw[:, k : k + GROUP]) for k in range(0, raw.shape[1], GROUP)], axis=0)
    v = raw + bias_ref[...]
    dt = jnp.maximum(v, 0.0) + jnp.log(1.0 + jnp.exp(-jnp.abs(v)))
    return dt, -dt * jnp.exp(dlog_ref[...])


def spread(v):
    rows = v.shape[0]
    first = lax.broadcasted_iota(jnp.int32, (rows, 128), 1) < HEAD_DIM
    return jnp.concatenate(
        [
            jnp.where(first, v[:, k : k + 1], v[:, k + 1 : k + 2])
            for k in range(0, CHUNK, 2)
        ],
        axis=1,
    )


def scatter(dt, cums, cum_s, dt_s, some):
    for g in range(len(cums)):
        rows = slice(g * GROUP, (g + 1) * GROUP)
        for c in some:
            cum_s[g, c] = cums[g][:, c * CHUNK : (c + 1) * CHUNK]
            dt_s[g, c] = dt[rows, c * CHUNK : (c + 1) * CHUNK]


def prepare(logit_ref, bias_ref, dlog_ref, write_ref, cum_s, dt_s, write_t, some=None):
    heads = bias_ref.shape[1]
    dt, fall = step_terms(logit_ref, bias_ref, dlog_ref)
    tri = lower_mask().astype(jnp.float32)
    cums = []
    for g in range(write_t.shape[0]):
        rows = slice(g * GROUP, (g + 1) * GROUP)
        cum = jnp.dot(tri, fall[rows], precision=highest, preferred_element_type=jnp.float32)
        cums.append(cum)
        write_t[g] = write_ref[rows, :].astype(jnp.float32).T.astype(jnp.bfloat16)
    scatter(dt, cums, cum_s, dt_s, range(heads // CHUNK) if some is None else some)
    return dt, cums


def group_state(g, c, x, cum_s, dt_s, write_t):
    cum = cum_s[g, c]
    last = cum[GROUP - 1 : GROUP]
    tail = jnp.exp(last - cum) * dt_s[g, c]
    scaled = (x.astype(jnp.float32) * spread(tail)).astype(jnp.bfloat16)
    state = jnp.dot(write_t[g], scaled, preferred_element_type=jnp.float32)
    return state, spread(jnp.exp(last))


def state_kernel(
    x_ref, logit_ref, write_ref, bias_ref, dlog_ref, starts_ref, order_ref, out_ref, cum_s, dt_s, write_t
):
    groups = write_t.shape[0]
    prepare(logit_ref, bias_ref, dlog_ref, write_ref, cum_s, dt_s, write_t)
    parts, _, width = out_ref.shape
    chunks = cum_s.shape[1]
    per = width // WIDE

    def one(c, carry):
        cols = pl.ds(pl.multiple_of(c * WIDE, WIDE), WIDE)
        total, decay = None, None
        for g in range(groups):
            x = x_ref[g * GROUP : (g + 1) * GROUP, cols]
            state, last = group_state(g, c, x, cum_s, dt_s, write_t)
            keep = 1.0 - starts_ref[g].astype(jnp.float32)
            factor = keep * last
            total = state if total is None else factor * total + state
            decay = factor if decay is None else factor * decay
        coarse = decay.astype(jnp.bfloat16)
        fine = (decay - coarse.astype(jnp.float32)).astype(jnp.bfloat16)
        row = lax.broadcasted_iota(jnp.int32, (EXTRA, WIDE), 0)
        lane = lax.broadcasted_iota(jnp.int32, (EXTRA, WIDE), 1)
        order = jnp.zeros((EXTRA, WIDE), jnp.float32)
        for g in range(groups):
            order = jnp.where(lane == g, order_ref[g].astype(jnp.float32), order)
        extra = jnp.where(
            row == 0,
            coarse.astype(jnp.float32),
            jnp.where(row == 1, fine.astype(jnp.float32), order),
        )
        full = jnp.concatenate([total, extra], axis=0).astype(jnp.bfloat16)
        if parts == 1:
            out_ref[0, :, cols] = full
        else:
            into = pl.ds(pl.multiple_of((c % per) * WIDE, WIDE), WIDE)
            out_ref[c // per, :, into] = full
        return carry

    lax.fori_loop(0, chunks, one, 0)


def scan_kernel(in_ref, out_ref):
    parts, _, width = in_ref.shape
    state = jnp.zeros((GROUP, width), jnp.float32)
    for s in range(parts):
        out_ref[s] = state.astype(jnp.bfloat16)
        extra = in_ref[s, GROUP : GROUP + EXTRA, :].astype(jnp.float32)
        decay = extra[0:1] + extra[1:2]
        state = decay * state + in_ref[s, :GROUP, :].astype(jnp.float32)


def gated_setup(
    logit_ref, bias_ref, dlog_ref, write_ref, read_ref, gain_ref, cum_s, dt_s, write_t, cum_t, dt_t, gain_s, score_s
):
    dt, cums = prepare(logit_ref, bias_ref, dlog_ref, write_ref, cum_s, dt_s, write_t)
    score_setup(dt, cums, read_ref, gain_ref, cum_s, write_t, cum_t, dt_t, gain_s, score_s)


def score_setup(dt, cums, read_ref, gain_ref, cum_s, write_t, cum_t, dt_t, gain_s, score_s):
    groups, chunks = cum_s.shape[:2]
    mask = lower_mask()
    for g in range(groups):
        rows = slice(g * GROUP, (g + 1) * GROUP)
        ct = transposed(cums[g])
        dtt = transposed(dt[rows])
        for c in range(chunks):
            cum_t[g, c] = ct[c * CHUNK : (c + 1) * CHUNK]
            dt_t[g, c] = dtt[c * CHUNK : (c + 1) * CHUNK]
        score = jnp.dot(read_ref[rows, :], write_t[g], preferred_element_type=jnp.float32)
        score_s[g] = jnp.where(mask, score, 0.0)
    for c in range(chunks):
        gain_s[c] = jnp.broadcast_to(gain_ref[:, c * CHUNK : (c + 1) * CHUNK], (8, CHUNK))


def gated_chunk(
    c, state, put, x_ref, gate_ref, read_ref, starts_ref, cum_s, dt_s, write_t, cum_t, dt_t, gain_s, score_s
):
    groups = cum_s.shape[0]
    first = lax.broadcasted_iota(jnp.int32, (GROUP, 128), 1) < HEAD_DIM
    cols = pl.ds(pl.multiple_of(c * WIDE, WIDE), WIDE)
    gain = spread(gain_s[c][0:1])
    for g in range(groups):
        rows = slice(g * GROUP, (g + 1) * GROUP)
        x = x_ref[rows, cols]
        keep = 1.0 - starts_ref[g].astype(jnp.float32)
        entering = (keep * state).astype(jnp.bfloat16)
        cum = cum_s[g, c]
        carried = jnp.dot(read_ref[rows, :], entering, preferred_element_type=jnp.float32)
        mixed = carried * spread(jnp.exp(cum)) + gain * x.astype(jnp.float32)
        score = score_s[g]
        ct, dtt = cum_t[g, c], dt_t[g, c]
        pieces = []
        for k in range(0, CHUNK, 2):
            pair = x[:, k * HEAD_DIM : (k + 2) * HEAD_DIM]
            both = []
            for h in (k, k + 1):
                gap = cum[:, h : h + 1] - ct[h : h + 1]
                weight = score * jnp.exp(jnp.minimum(gap, 0.0)) * dtt[h : h + 1]
                both.append(
                    jnp.dot(weight.astype(jnp.bfloat16), pair, preferred_element_type=jnp.float32)
                )
            pieces.append(jnp.where(first, both[0], both[1]))
        mixed = mixed + jnp.concatenate(pieces, axis=1)
        gate = gate_ref[rows, cols].astype(jnp.float32)
        put(g, (mixed * (gate / (1.0 + jnp.exp(-gate)))).astype(jnp.bfloat16))
        if g + 1 < groups:
            own, last = group_state(g, c, x, cum_s, dt_s, write_t)
            state = keep * last * state + own


def gated_kernel(
    x_ref,
    gate_ref,
    logit_ref,
    write_ref,
    read_ref,
    entry_ref,
    bias_ref,
    dlog_ref,
    gain_ref,
    starts_ref,
    out_ref,
    *scratch,
):
    gated_setup(logit_ref, bias_ref, dlog_ref, write_ref, read_ref, gain_ref, *scratch)
    parts, _, width = out_ref.shape
    chunks = scratch[0].shape[1]
    per = width // WIDE

    def one(c, carry):
        cols = pl.ds(pl.multiple_of(c * WIDE, WIDE), WIDE)
        into = pl.ds(pl.multiple_of((c % per) * WIDE, WIDE), WIDE)
        if parts == 1:
            state = entry_ref[0, :, cols].astype(jnp.float32)
        else:
            state = entry_ref[c // per, :, into].astype(jnp.float32)

        def put(g, value):
            rows = slice(g * GROUP, (g + 1) * GROUP)
            if parts == 1:
                out_ref[0, rows, cols] = value
            else:
                out_ref[c // per, rows, into] = value

        gated_chunk(c, state, put, x_ref, gate_ref, read_ref, starts_ref, *scratch)
        return carry

    lax.fori_loop(0, chunks, one, 0)


def fused_kernel(
    n,
    parts,
    x_hbm,
    gate_hbm,
    logit_hbm,
    write_hbm,
    read_hbm,
    bias_hbm,
    dlog_hbm,
    gain_hbm,
    starts_hbm,
    order_hbm,
    out_ref,
    squares,
    logit_ref,
    write_ref,
    read_ref,
    bias_ref,
    dlog_ref,
    gain_ref,
    starts_ref,
    order_ref,
    small_sem,
    x_ref,
    gate_ref,
    pair_out,
    pair_in,
    fade_out,
    fade_in,
    fade_s,
    total_s,
    decay_s,
    e_in,
    f_out,
    back,
    near_entry,
    far_entry,
    made,
    stage,
    final,
    order_own,
    order_all,
    order_s,
    load_sem,
    link_recv,
    give_recv,
    link_send,
    fade_send,
    fade_recv,
    send1,
    recv1,
    send2,
    recv2,
    send3,
    recv3,
    order_sem,
    gate_sem,
    ready_sem,
    side_sem,
    *rest,
):
    got, scratch = rest[:parts], rest[parts:]
    cum_s, dt_s, write_t = scratch[:3]
    groups, chunks = cum_s.shape[:2]
    piece = stage.shape[-1]
    per = WIDE // piece
    units = WIDE // UNIT
    span = 2 * WIDE
    me = lax.axis_index("ctx")
    side = me % 2
    level = me // 2
    levels = n // 2
    half = n // 2
    buddy = me + 1 - 2 * side
    low = level < levels // 2

    def send(source, target, sends, recvs, there):
        return pltpu.make_async_remote_copy(
            src_ref=source,
            dst_ref=target,
            send_sem=sends,
            recv_sem=recvs,
            device_id={"ctx": there},
            device_id_type=pl.DeviceIdType.MESH,
        )

    def landed(ref, sem):
        send(ref, ref, sem, sem, buddy).wait_recv()

    def left(ref, sem):
        send(ref, ref, sem, sem, buddy).wait_send()

    def load(which, j):
        cols = pl.ds(j * span, span)
        source, target = ((x_hbm, x_ref), (gate_hbm, gate_ref))[which]
        return pltpu.make_async_copy(source.at[:, cols], target.at[:, cols], load_sem.at[which, j])

    def pair(r):
        return send(pair_out.at[r], pair_in.at[r], link_send.at[0], link_recv.at[0, r], buddy)

    def chain(r):
        return send(f_out.at[r], e_in.at[r], link_send.at[1], link_recv.at[1, r], lax.rem(me + 2, n))

    def give(r):
        return send(back.at[r], far_entry.at[r], link_send.at[2], give_recv.at[r // units], buddy)

    def fade():
        return send(fade_out, fade_in, fade_send, fade_recv, buddy)

    def first(there, j):
        far = ((there < half) != low).astype(jnp.int32)
        return send(
            made.at[there, j], got[j].at[pl.ds(me * groups, groups)], send1.at[far], recv1.at[j], there
        )

    def second(there, j):
        return send(stage.at[there, j], final.at[me, j], send2, recv2.at[j], there)

    barrier = pltpu.get_barrier_semaphore()

    def tell(sem, there):
        pl.semaphore_signal(sem, inc=1, device_id={"ctx": there}, device_id_type=pl.DeviceIdType.MESH)

    above = level < levels - 1
    below = level > 0
    tell(barrier, buddy)

    @pl.when(above)
    def _():
        tell(barrier, lax.rem(me + 2, n))

    @pl.when(below)
    def _():
        tell(barrier, lax.rem(me + n - 2, n))

    small = [
        pltpu.make_async_copy(source, target, small_sem.at[k])
        for k, (source, target) in enumerate(
            (
                (logit_hbm, logit_ref),
                (bias_hbm, bias_ref),
                (dlog_hbm, dlog_ref),
                (write_hbm, write_ref),
                (starts_hbm, starts_ref),
                (read_hbm, read_ref),
                (gain_hbm, gain_ref),
                (order_hbm, order_ref),
            )
        )
    ]
    for copy in small[:5]:
        copy.start()
    load(0, 0).start()
    for copy in small[5:]:
        copy.start()
    for copy in small[:4]:
        copy.wait()
    for j in range(1, parts):
        load(0, j).start()
    for j in range(parts):
        load(1, j).start()

    def send_orders():
        for off in range(1, n):
            there = lax.rem(me + off, n)
            send(order_own, order_all.at[me], send3, recv3, there).start()

    with jax.named_scope("setup"):
        dt, cums = prepare(logit_ref, bias_ref, dlog_ref, write_ref, cum_s, dt_s, write_t, range(2))
        heads = bias_ref.shape[1]
        small[4].wait()
        whole = None
        for g in range(groups):
            factor = (1.0 - starts_ref[g].astype(jnp.float32)) * jnp.exp(cums[g][GROUP - 1 : GROUP])
            whole = factor if whole is None else whole * factor
        whole = jnp.concatenate([whole, jnp.zeros((1, 128 - heads), jnp.float32)], axis=1)
        fade_out[...] = whole

    @pl.when(level == 0)
    def _():
        e_in[...] = jnp.zeros_like(e_in)

    @pl.when(me == 0)
    def _():
        far_entry[...] = jnp.zeros_like(far_entry)

    def ends(c, carry):
        cols = pl.ds(pl.multiple_of(c * WIDE, WIDE), WIDE)
        total, decay = None, None
        for g in range(groups):
            x = x_ref[g * GROUP : (g + 1) * GROUP, cols]
            state, last = group_state(g, c, x, cum_s, dt_s, write_t)
            factor = (1.0 - starts_ref[g].astype(jnp.float32)) * last
            total = state if total is None else factor * total + state
            decay = factor if decay is None else factor * decay
        base = c // 2 * units

        @pl.when(c % 2 == side)
        def _():
            for u in range(units):
                cut = slice(u * UNIT, (u + 1) * UNIT)
                total_s[base + u] = total[:, cut]
                decay_s[base + u] = jnp.broadcast_to(decay[:, cut], (8, UNIT))

        @pl.when(c % 2 != side)
        def _():
            for u in range(units):
                pair_out[base + u] = total[:, u * UNIT : (u + 1) * UNIT].astype(jnp.bfloat16)

        return carry

    def relay(r, carry):
        pair(r).wait_recv()

        @pl.when(level > 0)
        def _():
            chain(r).wait_recv()

        state = e_in[r].astype(jnp.float32)
        their = pair_in[r].astype(jnp.float32)
        theirs = fade_s[r][0:1]
        total, decay = total_s[r], decay_s[r][0:1]
        early = side == 0
        middle = jnp.where(early, decay, theirs) * state + jnp.where(early, total, their)

        @pl.when(level < levels - 1)
        def _():
            end = jnp.where(early, theirs, decay) * middle + jnp.where(early, their, total)
            f_out[r] = end.astype(jnp.bfloat16)
            chain(r).start()

        @pl.when(me != 1)
        def _():
            back[r] = jnp.where(early, middle, state).astype(jnp.bfloat16)
            give(r).start()

        near_entry[r] = jnp.where(early, state, middle).astype(jnp.bfloat16)
        return carry

    def links(j):
        with jax.named_scope("links"):
            lax.fori_loop(j * units, (j + 1) * units, relay, 0)

    def offer(j):
        for u in range(units):
            pair(j * units + u).start()

    def hear_above():
        with jax.named_scope("ready"):
            pl.semaphore_wait(ready_sem, 1)

    def swap_half(j):
        with jax.named_scope("ends"):
            ends(2 * j + 1 - side, 0)
        if j == 0:
            with jax.named_scope("barrier"):
                pl.semaphore_wait(barrier, 1 + above.astype(jnp.int32) + below.astype(jnp.int32))
            fade().start()
        offer(j)

    def keep_half(j):
        with jax.named_scope("ends"):
            ends(2 * j + side, 0)

    def by_distance(k):
        return jnp.where(low, levels - 1 - k, k)

    def gate_ready(j):
        for s in range(parts):

            @pl.when(j == s)
            def _():
                load(1, s).wait()

    def compute(j, i, entry):
        def put(g, value):
            for p in range(per):
                made[2 * p + i, j, g] = value[:, p * piece : (p + 1) * piece]

        with jax.named_scope("gated"):
            state = jnp.concatenate([entry[j * units + u].astype(jnp.float32) for u in range(units)], axis=1)
            gated_chunk(2 * j + i, state, put, x_ref, gate_ref, read_ref, starts_ref, *scratch)

    def outward(j, there, wanted):
        for s in range(parts):

            @pl.when(jnp.logical_and(j == s, jnp.logical_and(there != me, wanted)))
            def _():
                first(there, s).start()

    late = parts - 1
    for j in range(late):
        load(0, j).wait()
        swap_half(j)
        if j == 0:

            @pl.when(jnp.logical_and(below, level == levels - 2))
            def _():
                tell(ready_sem, me - 2)

            with jax.named_scope("scores"):
                for copy in small[5:]:
                    copy.wait()
                lane = lax.broadcasted_iota(jnp.int32, order_own.shape, 1)
                held = jnp.zeros(order_own.shape, jnp.int32)
                for g in range(groups):
                    held = jnp.where(lane == g, order_ref[g], held)
                order_own[...] = held
                order_all[me] = held
                scatter(dt, cums, cum_s, dt_s, range(2, chunks))
                score_setup(dt, cums, read_ref, gain_ref, cum_s, write_t, *scratch[3:])
        if j == 1:
            keep_half(0)
            keep_half(1)
    fade().wait_recv()
    tile = fade_in[0:1, :]
    for c in range(chunks):

        @pl.when(c % 2 == side)
        def _(c=c):
            lanes = spread(tile[:, c * CHUNK : (c + 1) * CHUNK])
            for u in range(units):
                fade_s[c // 2 * units + u] = jnp.broadcast_to(lanes[:, u * UNIT : (u + 1) * UNIT], (8, UNIT))

    @pl.when(jnp.logical_and(below, level < levels - 2))
    def _():
        hear_above()
        tell(ready_sem, me - 2)

    @pl.when(low)
    def _():
        links(0)

    bottom = jnp.logical_and(level == 0, levels > 2)

    @pl.when(bottom)
    def _():
        hear_above()
        load(1, 0).wait()
        compute(0, side, near_entry)
        for k in range(per):
            outward(0, 2 * k + side, k >= levels // 2)

    load(0, late).wait()
    swap_half(late)
    for j in range(2, parts):
        keep_half(j)

    @pl.when(low)
    def _():
        with jax.named_scope("linksall"):
            lax.fori_loop(units, parts * units, relay, 0)

        tell(side_sem, buddy)


    def near_column(j, carry):
        @pl.when(jnp.logical_not(low))
        def _():
            links(j)

        begun = jnp.logical_and(bottom, j == 0)

        @pl.when(jnp.logical_not(begun))
        def _():
            gate_ready(j)
            compute(j, side, near_entry)

        for k in range(per):
            there = 2 * by_distance(k) + side
            high = there // 2
            fresh = jnp.logical_not(jnp.logical_and(begun, high >= levels // 2))
            outward(j, there, jnp.logical_and(fresh, jnp.logical_or(low, high < level)))
        for s in range(parts):

            @pl.when(j == s)
            def _():
                for g in range(groups):
                    got[s][me * groups + g] = made[me, s, g]

        return carry

    def postponed(j, carry):
        for k in range(per):
            outward(j, 2 * k + side, jnp.logical_not(jnp.logical_or(low, k < level)))
        return carry

    def far_column(j, carry):
        @pl.when(me > 0)
        def _():
            with jax.named_scope("waitgive"):
                landed(far_entry.at[pl.ds(j * units, units)], give_recv.at[j])

        @pl.when(jnp.logical_and(j == 0, jnp.logical_not(low)))
        def _():
            send_orders()

        compute(j, 1 - side, far_entry)
        for k in range(per):
            outward(j, 2 * by_distance(k) + 1 - side, True)
        return carry

    lax.fori_loop(0, parts, near_column, 0)
    lax.fori_loop(0, parts, postponed, 0)

    @pl.when(low)
    def _():
        pl.semaphore_wait(side_sem, 1)
        send_orders()

    lax.fori_loop(0, parts, far_column, 0)

    lower_inner = jnp.logical_and(level == levels // 2 - 1, level > 0)
    upper_inner = jnp.logical_and(level == levels // 2, level < levels - 1)
    inner = jnp.logical_or(lower_inner, upper_inner)

    def crossed():
        with jax.named_scope("crossed"):
            left(made.at[pl.ds(0, half)], send1.at[1])
        tell(gate_sem, jnp.where(low, me - 2, lax.rem(me + 2, n)))

    landed(order_all.at[pl.ds(0, n - 1)], recv3)
    fetch = pltpu.make_async_copy(order_all, order_s, order_sem)
    fetch.start()
    fetch.wait()

    @pl.when(upper_inner)
    def _():
        crossed()

    if levels > 2:

        @pl.when(jnp.logical_or(level == levels // 2 - 2, level == levels // 2 + 1))
        def _():
            with jax.named_scope("gate"):
                pl.semaphore_wait(gate_sem, 1)

    for j in range(parts):
        with jax.named_scope("waitfirst"):
            landed(got[j].at[pl.ds(0, (n - 1) * groups)], recv1.at[j])

        def pick(k, carry, j=j):
            there = 2 * by_distance(k // 2) + lax.rem(k + 1 + me, 2)

            @pl.when(there != me)
            def _():
                for g in range(groups):
                    stage[there, j, g] = got[j][order_s[there, 0, g]]
                second(there, j).start()

            @pl.when(there == me)
            def _():
                for g in range(groups):
                    final[me, j, g] = got[j][order_s[me, 0, g]]

            return carry

        with jax.named_scope("pick"):
            lax.fori_loop(0, n, pick, 0)
        if j == parts - 2:

            @pl.when(lower_inner)
            def _():
                crossed()

    tile = 32
    for j in range(parts):
        with jax.named_scope("waitsecond"):
            landed(final.at[pl.ds(0, n - 1), j], recv2.at[j])

        def add(r, carry, j=j):
            for g in range(groups):
                at = pl.ds(pl.multiple_of(r * tile, tile), tile)
                into = pl.ds(pl.multiple_of(g * GROUP + r * tile, tile), tile)
                total = jnp.zeros((tile, 128), jnp.float32) if j == 0 else squares[into, :]
                for s in range(n):
                    raw = final[s, j, g, at, :]
                    start = (2 * j + s % 2) * WIDE + s // 2 * piece
                    out_ref[into, start : start + piece] = raw
                    v = raw.astype(jnp.float32)
                    v = v * v
                    for q in range(0, piece, 128):
                        total = total + v[:, q : q + 128]
                squares[into, :] = total
            return carry

        with jax.named_scope("add"):
            lax.fori_loop(0, GROUP // tile, add, 0)

    with jax.named_scope("sent"):
        left(pair_out, link_send.at[0])
        left(fade_out, fade_send)

        @pl.when(level < levels - 1)
        def _():
            left(f_out, link_send.at[1])

        @pl.when(me != 1)
        def _():
            left(back, link_send.at[2])

        left(order_all.at[pl.ds(0, n - 1)], send3)
        left(made.at[pl.ds(0, half - 1)], send1.at[0])

        @pl.when(jnp.logical_not(inner))
        def _():
            left(made.at[pl.ds(0, half)], send1.at[1])

        left(stage.at[pl.ds(0, n - 1)], send2)


def scale_kernel(in_ref, squares_ref, weight_ref, out_hbm, ready, sem):
    rows, width = in_ref.shape
    tile = rows // sem.shape[0]

    def push(r):
        at = pl.ds(r * tile, tile)
        return pltpu.make_async_copy(ready.at[at, :], out_hbm.at[at, :], sem.at[r])

    for r in range(sem.shape[0]):
        at = slice(r * tile, (r + 1) * tile)
        total = jnp.sum(squares_ref[at, :], axis=1, keepdims=True)
        scale = lax.rsqrt(total * (1.0 / width) + 1e-05)
        for q in range(0, width, WIDE):
            cols = slice(q, q + WIDE)
            v = in_ref[at, cols].astype(jnp.float32)
            ready[at, cols] = (v * scale * weight_ref[:, cols]).astype(jnp.bfloat16)
        push(r).start()
    for r in range(sem.shape[0]):
        push(r).wait()


def norm_kernel(in_ref, weight_ref, out_ref):
    parts, rows, width = in_ref.shape
    tile = 32

    def one(r, carry):
        at = pl.ds(pl.multiple_of(r * tile, tile), tile)
        total = jnp.zeros((tile, 1), jnp.float32)
        for s in range(parts):
            v = in_ref[s, at, :].astype(jnp.float32)
            total = total + jnp.sum(v * v, axis=1, keepdims=True)
        scale = lax.rsqrt(total * (1.0 / (parts * width)) + 1e-05)
        for s in range(parts):
            v = in_ref[s, at, :].astype(jnp.float32)
            w = weight_ref[:, s * width : (s + 1) * width]
            out_ref[at, s * width : (s + 1) * width] = (v * scale * w).astype(jnp.bfloat16)
        return carry

    lax.fori_loop(0, rows // tile, one, 0)


def local(
    head_input,
    gate_input,
    write_vector,
    read_vector,
    increment_preactivation,
    step_bias,
    decay_log,
    skip_gain,
    norm_weight,
    doc_starts,
    block_order,
):
    devices = lax.axis_size("ctx")
    rows, features = head_input.shape
    heads = step_bias.shape[0]
    groups = rows // GROUP
    chunks = heads // CHUNK
    width = features // devices
    state_size = write_vector.shape[1]
    direct = width % WIDE == 0
    parts = devices if direct else 1
    limit = pltpu.CompilerParams(vmem_limit_bytes=48 * 1024 * 1024)
    common = [
        pltpu.VMEM((groups, chunks, GROUP, CHUNK), jnp.float32),
        pltpu.VMEM((groups, chunks, GROUP, CHUNK), jnp.float32),
        pltpu.VMEM((groups, state_size, GROUP), jnp.bfloat16),
    ]
    more = [
        pltpu.VMEM((groups, chunks, CHUNK, GROUP), jnp.float32),
        pltpu.VMEM((groups, chunks, CHUNK, GROUP), jnp.float32),
        pltpu.VMEM((chunks, 8, CHUNK), jnp.float32),
        pltpu.VMEM((groups, GROUP, GROUP), jnp.float32),
    ]
    bias, dlog, gain = (v.reshape(1, -1) for v in (step_bias, decay_log, skip_gain))

    def to_owners(v):
        if not direct:
            v = v.reshape(v.shape[1], devices, width).transpose(1, 0, 2)
        return lax.all_to_all(v, "ctx", split_axis=0, concat_axis=0, tiled=True)

    def joined(v):
        if not direct:
            v = v.transpose(1, 0, 2).reshape(1, v.shape[1], features)
        return v

    piece = width // PARTS
    per = max(WIDE // max(piece, 1), 1)
    if width == 512 and devices == 2 * per and chunks == 2 * PARTS:
        slab = (devices, PARTS, groups, GROUP, piece)
        links = features // UNIT // 2
        state = (links, state_size, UNIT)
        sems = pltpu.SemaphoreType.DMA
        packed, squares = pl.pallas_call(
            functools.partial(fused_kernel, devices, PARTS),
            out_shape=[
                pltpu.VMEM((rows, features), jnp.bfloat16),
                pltpu.VMEM((rows, 128), jnp.float32),
            ],
            in_specs=[ANY] * 10,
            out_specs=[VM] * 2,
            scratch_shapes=[
                pltpu.VMEM((heads, rows), jnp.bfloat16),
                pltpu.VMEM((rows, state_size), jnp.bfloat16),
                pltpu.VMEM((rows, state_size), jnp.bfloat16),
                pltpu.VMEM((1, heads), jnp.float32),
                pltpu.VMEM((1, heads), jnp.float32),
                pltpu.VMEM((1, heads), jnp.float32),
                pltpu.SMEM((groups,), jnp.int32),
                pltpu.SMEM((groups,), jnp.int32),
                sems((8,)),
                pltpu.VMEM((rows, features), jnp.bfloat16),
                pltpu.VMEM((rows, features), jnp.bfloat16),
                pltpu.VMEM(state, jnp.bfloat16),
                pltpu.VMEM(state, jnp.bfloat16),
                pltpu.VMEM((1, 128), jnp.float32),
                pltpu.VMEM((1, 128), jnp.float32),
                pltpu.VMEM((links, 8, UNIT), jnp.float32),
                pltpu.VMEM(state, jnp.float32),
                pltpu.VMEM((links, 8, UNIT), jnp.float32),
            ]
            + [pltpu.VMEM(state, jnp.bfloat16)] * 5
            + [pltpu.VMEM(slab, jnp.bfloat16)] * 3
            + [
                pltpu.VMEM((1, 128), jnp.int32),
                pltpu.VMEM((devices, 1, 128), jnp.int32),
                pltpu.SMEM((devices, 1, 128), jnp.int32),
                sems((2, PARTS)),
                sems((2, links)),
                sems((PARTS,)),
                sems((3,)),
                sems,
                sems,
                sems((2,)),
                sems((PARTS,)),
                sems,
                sems((PARTS,)),
                sems,
                sems,
                sems,
            ]
            + [pltpu.SemaphoreType.REGULAR] * 3
            + [pltpu.VMEM((devices * groups, GROUP, piece), jnp.bfloat16)] * PARTS
            + common
            + more,
            compiler_params=pltpu.CompilerParams(
                collective_id=0, has_side_effects=True, vmem_limit_bytes=LIMIT
            ),
            name="fused",
        )(
            head_input,
            gate_input,
            increment_preactivation.T,
            write_vector,
            read_vector,
            bias,
            dlog,
            gain,
            doc_starts,
            block_order,
        )
        return pl.pallas_call(
            scale_kernel,
            out_shape=jax.ShapeDtypeStruct((rows, features), jnp.bfloat16),
            in_specs=[VM] * 3,
            out_specs=ANY,
            scratch_shapes=[pltpu.VMEM((rows, features), jnp.bfloat16), sems((4,))],
            compiler_params=pltpu.CompilerParams(vmem_limit_bytes=8 * 1024 * 1024),
            name="scale",
        )(packed, squares, norm_weight.reshape(1, -1))

    ends = pl.pallas_call(
        state_kernel,
        out_shape=jax.ShapeDtypeStruct((parts, state_size + EXTRA, features // parts), jnp.bfloat16),
        in_specs=[VM] * 5 + [SM] * 2,
        out_specs=VM,
        scratch_shapes=common,
        compiler_params=limit,
        name="end_states",
    )(head_input, increment_preactivation.T, write_vector, bias, dlog, doc_starts, block_order)
    ends = to_owners(ends)
    all_order = ends[:, state_size + 2, :groups].astype(jnp.int32).reshape(-1)
    entry = pl.pallas_call(
        scan_kernel,
        out_shape=jax.ShapeDtypeStruct((devices, state_size, width), jnp.bfloat16),
        in_specs=[VM],
        out_specs=VM,
        compiler_params=limit,
        name="scan_states",
    )(ends)
    entry = joined(lax.all_to_all(entry, "ctx", split_axis=0, concat_axis=0, tiled=True))
    gated = pl.pallas_call(
        gated_kernel,
        out_shape=jax.ShapeDtypeStruct((parts, rows, features // parts), jnp.bfloat16),
        in_specs=[VM] * 9 + [SM],
        out_specs=VM,
        scratch_shapes=common
        + more,
        compiler_params=limit,
        name="gated",
    )(
        head_input,
        gate_input,
        increment_preactivation.T,
        write_vector,
        read_vector,
        entry,
        bias,
        dlog,
        gain,
        doc_starts,
    )
    gated = to_owners(gated)
    blocks = gated.reshape(devices * groups, GROUP, width)[all_order]
    packed = lax.all_to_all(
        blocks.reshape(devices, rows, width), "ctx", split_axis=0, concat_axis=0, tiled=True
    )
    return pl.pallas_call(
        norm_kernel,
        out_shape=jax.ShapeDtypeStruct((rows, features), jnp.bfloat16),
        in_specs=[VM] * 2,
        out_specs=VM,
        compiler_params=limit,
        name="norm",
    )(joined(packed), norm_weight.reshape(1, -1))


def solution(mesh):
    return jax.shard_map(
        local,
        mesh=mesh,
        in_specs=(
            P(("dp", "ctx"), None),
            P(("dp", "ctx"), None),
            P(("dp", "ctx"), None),
            P(("dp", "ctx"), None),
            P(("dp", "ctx"), None),
            P(),
            P(),
            P(),
            P(),
            P(("dp", "ctx")),
            P(("dp", "ctx")),
        ),
        out_specs=P(("dp", "ctx"), None),
        check_vma=False,
    )
```

```python
import functools

import jax
import jax.numpy as jnp
from jax import lax
from jax.experimental import pallas as pl
from jax.experimental.pallas import tpu as pltpu
from jax.sharding import PartitionSpec as P

HEAD_DIM = 64
GROUP = 128
CHUNK = 8
WIDE = CHUNK * HEAD_DIM
EXTRA = 16
PARTS = 4
LIMIT = 61 * 1024 * 1024
UNIT = 128

highest = lax.Precision.HIGHEST
VM = pl.BlockSpec(memory_space=pltpu.VMEM)
SM = pl.BlockSpec(memory_space=pltpu.SMEM)
ANY = pl.BlockSpec(memory_space=pltpu.HBM)


def transposed(v):
    rows, cols = v.shape
    if cols < 128:
        v = jnp.concatenate([v, jnp.zeros((rows, 128 - cols), v.dtype)], axis=1)
    return v.T[:cols]


def upright(v):
    rows, cols = v.shape
    if rows < 128:
        v = jnp.concatenate([v, jnp.zeros((128 - rows, cols), v.dtype)], axis=0)
    return v.T[:, :rows]


def lower_mask():
    row = lax.broadcasted_iota(jnp.int32, (GROUP, GROUP), 0)
    col = lax.broadcasted_iota(jnp.int32, (GROUP, GROUP), 1)
    return row >= col


def step_terms(logit_ref, bias_ref, dlog_ref):
    raw = logit_ref[...].astype(jnp.float32)
    raw = jnp.concatenate([upright(raw[:, k : k + GROUP]) for k in range(0, raw.shape[1], GROUP)], axis=0)
    v = raw + bias_ref[...]
    dt = jnp.maximum(v, 0.0) + jnp.log(1.0 + jnp.exp(-jnp.abs(v)))
    return dt, -dt * jnp.exp(dlog_ref[...])


def spread(v):
    rows = v.shape[0]
    first = lax.broadcasted_iota(jnp.int32, (rows, 128), 1) < HEAD_DIM
    return jnp.concatenate(
        [
            jnp.where(first, v[:, k : k + 1], v[:, k + 1 : k + 2])
            for k in range(0, CHUNK, 2)
        ],
        axis=1,
    )


def scatter(dt, cums, cum_s, dt_s, some):
    for g in range(len(cums)):
        rows = slice(g * GROUP, (g + 1) * GROUP)
        for c in some:
            cum_s[g, c] = cums[g][:, c * CHUNK : (c + 1) * CHUNK]
            dt_s[g, c] = dt[rows, c * CHUNK : (c + 1) * CHUNK]


def prepare(logit_ref, bias_ref, dlog_ref, write_ref, cum_s, dt_s, write_t, some=None):
    heads = bias_ref.shape[1]
    dt, fall = step_terms(logit_ref, bias_ref, dlog_ref)
    tri = lower_mask().astype(jnp.float32)
    cums = []
    for g in range(write_t.shape[0]):
        rows = slice(g * GROUP, (g + 1) * GROUP)
        cum = jnp.dot(tri, fall[rows], precision=highest, preferred_element_type=jnp.float32)
        cums.append(cum)
        write_t[g] = write_ref[rows, :].astype(jnp.float32).T.astype(jnp.bfloat16)
    scatter(dt, cums, cum_s, dt_s, range(heads // CHUNK) if some is None else some)
    return dt, cums


def group_state(g, c, x, cum_s, dt_s, write_t):
    cum = cum_s[g, c]
    last = cum[GROUP - 1 : GROUP]
    tail = jnp.exp(last - cum) * dt_s[g, c]
    scaled = (x.astype(jnp.float32) * spread(tail)).astype(jnp.bfloat16)
    state = jnp.dot(write_t[g], scaled, preferred_element_type=jnp.float32)
    return state, spread(jnp.exp(last))


def state_kernel(
    x_ref, logit_ref, write_ref, bias_ref, dlog_ref, starts_ref, order_ref, out_ref, cum_s, dt_s, write_t
):
    groups = write_t.shape[0]
    prepare(logit_ref, bias_ref, dlog_ref, write_ref, cum_s, dt_s, write_t)
    parts, _, width = out_ref.shape
    chunks = cum_s.shape[1]
    per = width // WIDE

    def one(c, carry):
        cols = pl.ds(pl.multiple_of(c * WIDE, WIDE), WIDE)
        total, decay = None, None
        for g in range(groups):
            x = x_ref[g * GROUP : (g + 1) * GROUP, cols]
            state, last = group_state(g, c, x, cum_s, dt_s, write_t)
            keep = 1.0 - starts_ref[g].astype(jnp.float32)
            factor = keep * last
            total = state if total is None else factor * total + state
            decay = factor if decay is None else factor * decay
        coarse = decay.astype(jnp.bfloat16)
        fine = (decay - coarse.astype(jnp.float32)).astype(jnp.bfloat16)
        row = lax.broadcasted_iota(jnp.int32, (EXTRA, WIDE), 0)
        lane = lax.broadcasted_iota(jnp.int32, (EXTRA, WIDE), 1)
        order = jnp.zeros((EXTRA, WIDE), jnp.float32)
        for g in range(groups):
            order = jnp.where(lane == g, order_ref[g].astype(jnp.float32), order)
        extra = jnp.where(
            row == 0,
            coarse.astype(jnp.float32),
            jnp.where(row == 1, fine.astype(jnp.float32), order),
        )
        full = jnp.concatenate([total, extra], axis=0).astype(jnp.bfloat16)
        if parts == 1:
            out_ref[0, :, cols] = full
        else:
            into = pl.ds(pl.multiple_of((c % per) * WIDE, WIDE), WIDE)
            out_ref[c // per, :, into] = full
        return carry

    lax.fori_loop(0, chunks, one, 0)


def scan_kernel(in_ref, out_ref):
    parts, _, width = in_ref.shape
    state = jnp.zeros((GROUP, width), jnp.float32)
    for s in range(parts):
        out_ref[s] = state.astype(jnp.bfloat16)
        extra = in_ref[s, GROUP : GROUP + EXTRA, :].astype(jnp.float32)
        decay = extra[0:1] + extra[1:2]
        state = decay * state + in_ref[s, :GROUP, :].astype(jnp.float32)


def gated_setup(
    logit_ref, bias_ref, dlog_ref, write_ref, read_ref, gain_ref, cum_s, dt_s, write_t, cum_t, dt_t, gain_s, score_s
):
    dt, cums = prepare(logit_ref, bias_ref, dlog_ref, write_ref, cum_s, dt_s, write_t)
    score_setup(dt, cums, read_ref, gain_ref, cum_s, write_t, cum_t, dt_t, gain_s, score_s)


def score_setup(dt, cums, read_ref, gain_ref, cum_s, write_t, cum_t, dt_t, gain_s, score_s):
    groups, chunks = cum_s.shape[:2]
    mask = lower_mask()
    for g in range(groups):
        rows = slice(g * GROUP, (g + 1) * GROUP)
        ct = transposed(cums[g])
        dtt = transposed(dt[rows])
        for c in range(chunks):
            cum_t[g, c] = ct[c * CHUNK : (c + 1) * CHUNK]
            dt_t[g, c] = dtt[c * CHUNK : (c + 1) * CHUNK]
        score = jnp.dot(read_ref[rows, :], write_t[g], preferred_element_type=jnp.float32)
        score_s[g] = jnp.where(mask, score, 0.0)
    for c in range(chunks):
        gain_s[c] = jnp.broadcast_to(gain_ref[:, c * CHUNK : (c + 1) * CHUNK], (8, CHUNK))


def gated_chunk(
    c, state, put, x_ref, gate_ref, read_ref, starts_ref, cum_s, dt_s, write_t, cum_t, dt_t, gain_s, score_s
):
    groups = cum_s.shape[0]
    first = lax.broadcasted_iota(jnp.int32, (GROUP, 128), 1) < HEAD_DIM
    cols = pl.ds(pl.multiple_of(c * WIDE, WIDE), WIDE)
    gain = spread(gain_s[c][0:1])
    for g in range(groups):
        rows = slice(g * GROUP, (g + 1) * GROUP)
        x = x_ref[rows, cols]
        keep = 1.0 - starts_ref[g].astype(jnp.float32)
        entering = (keep * state).astype(jnp.bfloat16)
        cum = cum_s[g, c]
        carried = jnp.dot(read_ref[rows, :], entering, preferred_element_type=jnp.float32)
        mixed = carried * spread(jnp.exp(cum)) + gain * x.astype(jnp.float32)
        score = score_s[g]
        ct, dtt = cum_t[g, c], dt_t[g, c]
        pieces = []
        for k in range(0, CHUNK, 2):
            pair = x[:, k * HEAD_DIM : (k + 2) * HEAD_DIM]
            both = []
            for h in (k, k + 1):
                gap = cum[:, h : h + 1] - ct[h : h + 1]
                weight = score * jnp.exp(jnp.minimum(gap, 0.0)) * dtt[h : h + 1]
                both.append(
                    jnp.dot(weight.astype(jnp.bfloat16), pair, preferred_element_type=jnp.float32)
                )
            pieces.append(jnp.where(first, both[0], both[1]))
        mixed = mixed + jnp.concatenate(pieces, axis=1)
        gate = gate_ref[rows, cols].astype(jnp.float32)
        put(g, (mixed * (gate / (1.0 + jnp.exp(-gate)))).astype(jnp.bfloat16))
        if g + 1 < groups:
            own, last = group_state(g, c, x, cum_s, dt_s, write_t)
            state = keep * last * state + own


def gated_kernel(
    x_ref,
    gate_ref,
    logit_ref,
    write_ref,
    read_ref,
    entry_ref,
    bias_ref,
    dlog_ref,
    gain_ref,
    starts_ref,
    out_ref,
    *scratch,
):
    gated_setup(logit_ref, bias_ref, dlog_ref, write_ref, read_ref, gain_ref, *scratch)
    parts, _, width = out_ref.shape
    chunks = scratch[0].shape[1]
    per = width // WIDE

    def one(c, carry):
        cols = pl.ds(pl.multiple_of(c * WIDE, WIDE), WIDE)
        into = pl.ds(pl.multiple_of((c % per) * WIDE, WIDE), WIDE)
        if parts == 1:
            state = entry_ref[0, :, cols].astype(jnp.float32)
        else:
            state = entry_ref[c // per, :, into].astype(jnp.float32)

        def put(g, value):
            rows = slice(g * GROUP, (g + 1) * GROUP)
            if parts == 1:
                out_ref[0, rows, cols] = value
            else:
                out_ref[c // per, rows, into] = value

        gated_chunk(c, state, put, x_ref, gate_ref, read_ref, starts_ref, *scratch)
        return carry

    lax.fori_loop(0, chunks, one, 0)


def fused_kernel(
    n,
    parts,
    x_hbm,
    gate_hbm,
    logit_hbm,
    write_hbm,
    read_hbm,
    bias_hbm,
    dlog_hbm,
    gain_hbm,
    starts_hbm,
    order_hbm,
    out_ref,
    squares,
    logit_ref,
    write_ref,
    read_ref,
    bias_ref,
    dlog_ref,
    gain_ref,
    starts_ref,
    order_ref,
    small_sem,
    x_ref,
    gate_ref,
    pair_out,
    pair_in,
    fade_out,
    fade_in,
    fade_s,
    total_s,
    decay_s,
    e_in,
    f_out,
    back,
    near_entry,
    far_entry,
    made,
    stage,
    final,
    order_own,
    order_all,
    order_s,
    load_sem,
    link_recv,
    give_recv,
    link_send,
    fade_send,
    fade_recv,
    send1,
    recv1,
    send2,
    recv2,
    send3,
    recv3,
    order_sem,
    gate_sem,
    ready_sem,
    side_sem,
    *rest,
):
    got, scratch = rest[:parts], rest[parts:]
    cum_s, dt_s, write_t = scratch[:3]
    groups, chunks = cum_s.shape[:2]
    piece = stage.shape[-1]
    per = WIDE // piece
    units = WIDE // UNIT
    span = 2 * WIDE
    me = lax.axis_index("ctx")
    side = me % 2
    level = me // 2
    levels = n // 2
    half = n // 2
    buddy = me + 1 - 2 * side
    low = level < levels // 2

    def send(source, target, sends, recvs, there):
        return pltpu.make_async_remote_copy(
            src_ref=source,
            dst_ref=target,
            send_sem=sends,
            recv_sem=recvs,
            device_id={"ctx": there},
            device_id_type=pl.DeviceIdType.MESH,
        )

    def landed(ref, sem):
        send(ref, ref, sem, sem, buddy).wait_recv()

    def left(ref, sem):
        send(ref, ref, sem, sem, buddy).wait_send()

    def load(which, j):
        cols = pl.ds(j * span, span)
        source, target = ((x_hbm, x_ref), (gate_hbm, gate_ref))[which]
        return pltpu.make_async_copy(source.at[:, cols], target.at[:, cols], load_sem.at[which, j])

    def pair(r):
        return send(pair_out.at[r], pair_in.at[r], link_send.at[0], link_recv.at[0, r], buddy)

    def chain(r):
        return send(f_out.at[r], e_in.at[r], link_send.at[1], link_recv.at[1, r], lax.rem(me + 2, n))

    def give(r):
        return send(back.at[r], far_entry.at[r], link_send.at[2], give_recv.at[r // units], buddy)

    def fade():
        return send(fade_out, fade_in, fade_send, fade_recv, buddy)

    def first(there, j):
        far = ((there < half) != low).astype(jnp.int32)
        return send(
            made.at[there, j], got[j].at[pl.ds(me * groups, groups)], send1.at[far], recv1.at[j], there
        )

    def second(there, j):
        return send(stage.at[there, j], final.at[me, j], send2, recv2.at[j], there)

    barrier = pltpu.get_barrier_semaphore()

    def tell(sem, there):
        pl.semaphore_signal(sem, inc=1, device_id={"ctx": there}, device_id_type=pl.DeviceIdType.MESH)

    above = level < levels - 1
    below = level > 0
    tell(barrier, buddy)

    @pl.when(above)
    def _():
        tell(barrier, lax.rem(me + 2, n))

    @pl.when(below)
    def _():
        tell(barrier, lax.rem(me + n - 2, n))

    small = [
        pltpu.make_async_copy(source, target, small_sem.at[k])
        for k, (source, target) in enumerate(
            (
                (logit_hbm, logit_ref),
                (bias_hbm, bias_ref),
                (dlog_hbm, dlog_ref),
                (write_hbm, write_ref),
                (starts_hbm, starts_ref),
                (read_hbm, read_ref),
                (gain_hbm, gain_ref),
                (order_hbm, order_ref),
            )
        )
    ]
    for copy in small[:5]:
        copy.start()
    load(0, 0).start()
    for copy in small[5:]:
        copy.start()
    for copy in small[:4]:
        copy.wait()
    for j in range(1, parts):
        load(0, j).start()
    for j in range(parts):
        load(1, j).start()

    def send_orders():
        for off in range(1, n):
            there = lax.rem(me + off, n)
            send(order_own, order_all.at[me], send3, recv3, there).start()

    with jax.named_scope("setup"):
        dt, cums = prepare(logit_ref, bias_ref, dlog_ref, write_ref, cum_s, dt_s, write_t, range(2))
        heads = bias_ref.shape[1]
        small[4].wait()
        whole = None
        for g in range(groups):
            factor = (1.0 - starts_ref[g].astype(jnp.float32)) * jnp.exp(cums[g][GROUP - 1 : GROUP])
            whole = factor if whole is None else whole * factor
        whole = jnp.concatenate([whole, jnp.zeros((1, 128 - heads), jnp.float32)], axis=1)
        fade_out[...] = whole

    @pl.when(level == 0)
    def _():
        e_in[...] = jnp.zeros_like(e_in)

    @pl.when(me == 0)
    def _():
        near_entry[...] = jnp.zeros_like(near_entry)
        far_entry[...] = jnp.zeros_like(far_entry)

    def ends(c, carry):
        cols = pl.ds(pl.multiple_of(c * WIDE, WIDE), WIDE)
        total, decay = None, None
        for g in range(groups):
            x = x_ref[g * GROUP : (g + 1) * GROUP, cols]
            state, last = group_state(g, c, x, cum_s, dt_s, write_t)
            factor = (1.0 - starts_ref[g].astype(jnp.float32)) * last
            total = state if total is None else factor * total + state
            decay = factor if decay is None else factor * decay
        base = c // 2 * units

        @pl.when(c % 2 == side)
        def _():
            for u in range(units):
                cut = slice(u * UNIT, (u + 1) * UNIT)
                total_s[base + u] = total[:, cut]
                decay_s[base + u] = jnp.broadcast_to(decay[:, cut], (8, UNIT))

        @pl.when(c % 2 != side)
        def _():
            for u in range(units):
                pair_out[base + u] = total[:, u * UNIT : (u + 1) * UNIT].astype(jnp.bfloat16)

        return carry

    def relay(r, carry):
        pair(r).wait_recv()

        @pl.when(level > 0)
        def _():
            chain(r).wait_recv()

        state = e_in[r].astype(jnp.float32)
        their = pair_in[r].astype(jnp.float32)
        theirs = fade_s[r][0:1]
        total, decay = total_s[r], decay_s[r][0:1]
        early = side == 0
        middle = jnp.where(early, decay, theirs) * state + jnp.where(early, total, their)

        @pl.when(level < levels - 1)
        def _():
            end = jnp.where(early, theirs, decay) * middle + jnp.where(early, their, total)
            f_out[r] = end.astype(jnp.bfloat16)
            chain(r).start()

        @pl.when(me != 1)
        def _():
            back[r] = jnp.where(early, middle, state).astype(jnp.bfloat16)
            give(r).start()

        near_entry[r] = jnp.where(early, state, middle).astype(jnp.bfloat16)
        return carry

    def links(j):
        with jax.named_scope("links"):
            lax.fori_loop(j * units, (j + 1) * units, relay, 0)

    def offer(j):
        for u in range(units):
            pair(j * units + u).start()

    def hear_above():
        with jax.named_scope("ready"):
            pl.semaphore_wait(ready_sem, 1)

    def swap_half(j):
        with jax.named_scope("ends"):
            ends(2 * j + 1 - side, 0)
        if j == 0:
            with jax.named_scope("barrier"):
                pl.semaphore_wait(barrier, 1 + above.astype(jnp.int32) + below.astype(jnp.int32))
            fade().start()
        offer(j)

    def keep_half(j):
        with jax.named_scope("ends"):
            ends(2 * j + side, 0)

    def by_distance(k):
        return jnp.where(low, levels - 1 - k, k)

    def gate_ready(j):
        for s in range(parts):

            @pl.when(j == s)
            def _():
                load(1, s).wait()

    def compute(j, i, entry):
        def put(g, value):
            for p in range(per):
                made[2 * p + i, j, g] = value[:, p * piece : (p + 1) * piece]

        with jax.named_scope("gated"):
            state = jnp.concatenate([entry[j * units + u].astype(jnp.float32) for u in range(units)], axis=1)
            gated_chunk(2 * j + i, state, put, x_ref, gate_ref, read_ref, starts_ref, *scratch)

    def outward(j, there, wanted):
        for s in range(parts):

            @pl.when(jnp.logical_and(j == s, jnp.logical_and(there != me, wanted)))
            def _():
                first(there, s).start()

    bottom = jnp.logical_and(level == 0, levels > 2)

    def open_early():
        load(1, 0).wait()
        compute(0, side, near_entry)
        hear_above()
        for k in range(per):
            outward(0, 2 * k + side, k >= levels // 2)

    late = parts - 1
    for j in range(late):
        load(0, j).wait()
        swap_half(j)
        if j == 0:

            @pl.when(jnp.logical_and(below, level == levels - 2))
            def _():
                tell(ready_sem, me - 2)

            with jax.named_scope("scores"):
                for copy in small[5:]:
                    copy.wait()
                lane = lax.broadcasted_iota(jnp.int32, order_own.shape, 1)
                held = jnp.zeros(order_own.shape, jnp.int32)
                for g in range(groups):
                    held = jnp.where(lane == g, order_ref[g], held)
                order_own[...] = held
                order_all[me] = held
                scatter(dt, cums, cum_s, dt_s, range(2, chunks))
                score_setup(dt, cums, read_ref, gain_ref, cum_s, write_t, *scratch[3:])

            @pl.when(jnp.logical_and(below, level < levels - 2))
            def _():
                hear_above()
                tell(ready_sem, me - 2)

            @pl.when(jnp.logical_and(bottom, me == 0))
            def _():
                open_early()

        if j == 1:
            keep_half(0)
            keep_half(1)
    fade().wait_recv()
    tile = fade_in[0:1, :]
    for c in range(chunks):

        @pl.when(c % 2 == side)
        def _(c=c):
            lanes = spread(tile[:, c * CHUNK : (c + 1) * CHUNK])
            for u in range(units):
                fade_s[c // 2 * units + u] = jnp.broadcast_to(lanes[:, u * UNIT : (u + 1) * UNIT], (8, UNIT))

    @pl.when(low)
    def _():
        links(0)

    @pl.when(jnp.logical_and(bottom, me > 0))
    def _():
        open_early()

    load(0, late).wait()
    swap_half(late)
    for j in range(2, parts):
        keep_half(j)

    @pl.when(low)
    def _():
        with jax.named_scope("linksall"):
            lax.fori_loop(units, parts * units, relay, 0)

        tell(side_sem, buddy)


    def near_column(j, carry):
        @pl.when(jnp.logical_not(low))
        def _():
            links(j)

        begun = jnp.logical_and(bottom, j == 0)

        @pl.when(jnp.logical_not(begun))
        def _():
            gate_ready(j)
            compute(j, side, near_entry)

        for k in range(per):
            there = 2 * by_distance(k) + side
            high = there // 2
            fresh = jnp.logical_not(jnp.logical_and(begun, high >= levels // 2))
            outward(j, there, jnp.logical_and(fresh, jnp.logical_or(low, high < level)))
        for s in range(parts):

            @pl.when(j == s)
            def _():
                for g in range(groups):
                    got[s][me * groups + g] = made[me, s, g]

        return carry

    def postponed(j, carry):
        for k in range(per):
            outward(j, 2 * k + side, jnp.logical_not(jnp.logical_or(low, k < level)))
        return carry

    def far_column(j, carry):
        @pl.when(me > 0)
        def _():
            with jax.named_scope("waitgive"):
                landed(far_entry.at[pl.ds(j * units, units)], give_recv.at[j])

        @pl.when(jnp.logical_and(j == 0, jnp.logical_not(low)))
        def _():
            send_orders()

        compute(j, 1 - side, far_entry)
        for k in range(per):
            outward(j, 2 * by_distance(k) + 1 - side, True)
        return carry

    lax.fori_loop(0, parts, near_column, 0)
    lax.fori_loop(0, parts, postponed, 0)

    @pl.when(low)
    def _():
        pl.semaphore_wait(side_sem, 1)
        send_orders()

    lax.fori_loop(0, parts, far_column, 0)

    lower_inner = jnp.logical_and(level == levels // 2 - 1, level > 0)
    upper_inner = jnp.logical_and(level == levels // 2, level < levels - 1)
    inner = jnp.logical_or(lower_inner, upper_inner)

    def crossed():
        with jax.named_scope("crossed"):
            left(made.at[pl.ds(0, half)], send1.at[1])
        tell(gate_sem, jnp.where(low, me - 2, lax.rem(me + 2, n)))

    landed(order_all.at[pl.ds(0, n - 1)], recv3)
    fetch = pltpu.make_async_copy(order_all, order_s, order_sem)
    fetch.start()
    fetch.wait()

    @pl.when(upper_inner)
    def _():
        crossed()

    if levels > 2:

        @pl.when(jnp.logical_or(level == levels // 2 - 2, level == levels // 2 + 1))
        def _():
            with jax.named_scope("gate"):
                pl.semaphore_wait(gate_sem, 1)

    for j in range(parts):
        with jax.named_scope("waitfirst"):
            landed(got[j].at[pl.ds(0, (n - 1) * groups)], recv1.at[j])

        def pick(k, carry, j=j):
            there = 2 * by_distance(k // 2) + lax.rem(k + 1 + me, 2)

            @pl.when(there != me)
            def _():
                for g in range(groups):
                    stage[there, j, g] = got[j][order_s[there, 0, g]]
                second(there, j).start()

            @pl.when(there == me)
            def _():
                for g in range(groups):
                    final[me, j, g] = got[j][order_s[me, 0, g]]

            return carry

        with jax.named_scope("pick"):
            lax.fori_loop(0, n, pick, 0)
        if j == parts - 2:

            @pl.when(lower_inner)
            def _():
                crossed()

    tile = 32
    for j in range(parts):
        with jax.named_scope("waitsecond"):
            landed(final.at[pl.ds(0, n - 1), j], recv2.at[j])

        def add(r, carry, j=j):
            for g in range(groups):
                at = pl.ds(pl.multiple_of(r * tile, tile), tile)
                into = pl.ds(pl.multiple_of(g * GROUP + r * tile, tile), tile)
                total = jnp.zeros((tile, 128), jnp.float32) if j == 0 else squares[into, :]
                for s in range(n):
                    raw = final[s, j, g, at, :]
                    start = (2 * j + s % 2) * WIDE + s // 2 * piece
                    out_ref[into, start : start + piece] = raw
                    v = raw.astype(jnp.float32)
                    v = v * v
                    for q in range(0, piece, 128):
                        total = total + v[:, q : q + 128]
                squares[into, :] = total
            return carry

        with jax.named_scope("add"):
            lax.fori_loop(0, GROUP // tile, add, 0)

    with jax.named_scope("sent"):
        left(pair_out, link_send.at[0])
        left(fade_out, fade_send)

        @pl.when(level < levels - 1)
        def _():
            left(f_out, link_send.at[1])

        @pl.when(me != 1)
        def _():
            left(back, link_send.at[2])

        left(order_all.at[pl.ds(0, n - 1)], send3)
        left(made.at[pl.ds(0, half - 1)], send1.at[0])

        @pl.when(jnp.logical_not(inner))
        def _():
            left(made.at[pl.ds(0, half)], send1.at[1])

        left(stage.at[pl.ds(0, n - 1)], send2)


def scale_kernel(in_ref, squares_ref, weight_ref, out_hbm, ready, sem):
    rows, width = in_ref.shape
    tile = rows // sem.shape[0]

    def push(r):
        at = pl.ds(r * tile, tile)
        return pltpu.make_async_copy(ready.at[at, :], out_hbm.at[at, :], sem.at[r])

    for r in range(sem.shape[0]):
        at = slice(r * tile, (r + 1) * tile)
        total = jnp.sum(squares_ref[at, :], axis=1, keepdims=True)
        scale = lax.rsqrt(total * (1.0 / width) + 1e-05)
        for q in range(0, width, WIDE):
            cols = slice(q, q + WIDE)
            v = in_ref[at, cols].astype(jnp.float32)
            ready[at, cols] = (v * scale * weight_ref[:, cols]).astype(jnp.bfloat16)
        push(r).start()
    for r in range(sem.shape[0]):
        push(r).wait()


def norm_kernel(in_ref, weight_ref, out_ref):
    parts, rows, width = in_ref.shape
    tile = 32

    def one(r, carry):
        at = pl.ds(pl.multiple_of(r * tile, tile), tile)
        total = jnp.zeros((tile, 1), jnp.float32)
        for s in range(parts):
            v = in_ref[s, at, :].astype(jnp.float32)
            total = total + jnp.sum(v * v, axis=1, keepdims=True)
        scale = lax.rsqrt(total * (1.0 / (parts * width)) + 1e-05)
        for s in range(parts):
            v = in_ref[s, at, :].astype(jnp.float32)
            w = weight_ref[:, s * width : (s + 1) * width]
            out_ref[at, s * width : (s + 1) * width] = (v * scale * w).astype(jnp.bfloat16)
        return carry

    lax.fori_loop(0, rows // tile, one, 0)


def local(
    head_input,
    gate_input,
    write_vector,
    read_vector,
    increment_preactivation,
    step_bias,
    decay_log,
    skip_gain,
    norm_weight,
    doc_starts,
    block_order,
):
    devices = lax.axis_size("ctx")
    rows, features = head_input.shape
    heads = step_bias.shape[0]
    groups = rows // GROUP
    chunks = heads // CHUNK
    width = features // devices
    state_size = write_vector.shape[1]
    direct = width % WIDE == 0
    parts = devices if direct else 1
    limit = pltpu.CompilerParams(vmem_limit_bytes=48 * 1024 * 1024)
    common = [
        pltpu.VMEM((groups, chunks, GROUP, CHUNK), jnp.float32),
        pltpu.VMEM((groups, chunks, GROUP, CHUNK), jnp.float32),
        pltpu.VMEM((groups, state_size, GROUP), jnp.bfloat16),
    ]
    more = [
        pltpu.VMEM((groups, chunks, CHUNK, GROUP), jnp.float32),
        pltpu.VMEM((groups, chunks, CHUNK, GROUP), jnp.float32),
        pltpu.VMEM((chunks, 8, CHUNK), jnp.float32),
        pltpu.VMEM((groups, GROUP, GROUP), jnp.float32),
    ]
    bias, dlog, gain = (v.reshape(1, -1) for v in (step_bias, decay_log, skip_gain))

    def to_owners(v):
        if not direct:
            v = v.reshape(v.shape[1], devices, width).transpose(1, 0, 2)
        return lax.all_to_all(v, "ctx", split_axis=0, concat_axis=0, tiled=True)

    def joined(v):
        if not direct:
            v = v.transpose(1, 0, 2).reshape(1, v.shape[1], features)
        return v

    piece = width // PARTS
    per = max(WIDE // max(piece, 1), 1)
    if width == 512 and devices == 2 * per and chunks == 2 * PARTS:
        slab = (devices, PARTS, groups, GROUP, piece)
        links = features // UNIT // 2
        state = (links, state_size, UNIT)
        sems = pltpu.SemaphoreType.DMA
        packed, squares = pl.pallas_call(
            functools.partial(fused_kernel, devices, PARTS),
            out_shape=[
                pltpu.VMEM((rows, features), jnp.bfloat16),
                pltpu.VMEM((rows, 128), jnp.float32),
            ],
            in_specs=[ANY] * 10,
            out_specs=[VM] * 2,
            scratch_shapes=[
                pltpu.VMEM((heads, rows), jnp.bfloat16),
                pltpu.VMEM((rows, state_size), jnp.bfloat16),
                pltpu.VMEM((rows, state_size), jnp.bfloat16),
                pltpu.VMEM((1, heads), jnp.float32),
                pltpu.VMEM((1, heads), jnp.float32),
                pltpu.VMEM((1, heads), jnp.float32),
                pltpu.SMEM((groups,), jnp.int32),
                pltpu.SMEM((groups,), jnp.int32),
                sems((8,)),
                pltpu.VMEM((rows, features), jnp.bfloat16),
                pltpu.VMEM((rows, features), jnp.bfloat16),
                pltpu.VMEM(state, jnp.bfloat16),
                pltpu.VMEM(state, jnp.bfloat16),
                pltpu.VMEM((1, 128), jnp.float32),
                pltpu.VMEM((1, 128), jnp.float32),
                pltpu.VMEM((links, 8, UNIT), jnp.float32),
                pltpu.VMEM(state, jnp.float32),
                pltpu.VMEM((links, 8, UNIT), jnp.float32),
            ]
            + [pltpu.VMEM(state, jnp.bfloat16)] * 5
            + [pltpu.VMEM(slab, jnp.bfloat16)] * 3
            + [
                pltpu.VMEM((1, 128), jnp.int32),
                pltpu.VMEM((devices, 1, 128), jnp.int32),
                pltpu.SMEM((devices, 1, 128), jnp.int32),
                sems((2, PARTS)),
                sems((2, links)),
                sems((PARTS,)),
                sems((3,)),
                sems,
                sems,
                sems((2,)),
                sems((PARTS,)),
                sems,
                sems((PARTS,)),
                sems,
                sems,
                sems,
            ]
            + [pltpu.SemaphoreType.REGULAR] * 3
            + [pltpu.VMEM((devices * groups, GROUP, piece), jnp.bfloat16)] * PARTS
            + common
            + more,
            compiler_params=pltpu.CompilerParams(
                collective_id=0, has_side_effects=True, vmem_limit_bytes=LIMIT
            ),
            name="fused",
        )(
            head_input,
            gate_input,
            increment_preactivation.T,
            write_vector,
            read_vector,
            bias,
            dlog,
            gain,
            doc_starts,
            block_order,
        )
        return pl.pallas_call(
            scale_kernel,
            out_shape=jax.ShapeDtypeStruct((rows, features), jnp.bfloat16),
            in_specs=[VM] * 3,
            out_specs=ANY,
            scratch_shapes=[pltpu.VMEM((rows, features), jnp.bfloat16), sems((4,))],
            compiler_params=pltpu.CompilerParams(vmem_limit_bytes=8 * 1024 * 1024),
            name="scale",
        )(packed, squares, norm_weight.reshape(1, -1))

    ends = pl.pallas_call(
        state_kernel,
        out_shape=jax.ShapeDtypeStruct((parts, state_size + EXTRA, features // parts), jnp.bfloat16),
        in_specs=[VM] * 5 + [SM] * 2,
        out_specs=VM,
        scratch_shapes=common,
        compiler_params=limit,
        name="end_states",
    )(head_input, increment_preactivation.T, write_vector, bias, dlog, doc_starts, block_order)
    ends = to_owners(ends)
    all_order = ends[:, state_size + 2, :groups].astype(jnp.int32).reshape(-1)
    entry = pl.pallas_call(
        scan_kernel,
        out_shape=jax.ShapeDtypeStruct((devices, state_size, width), jnp.bfloat16),
        in_specs=[VM],
        out_specs=VM,
        compiler_params=limit,
        name="scan_states",
    )(ends)
    entry = joined(lax.all_to_all(entry, "ctx", split_axis=0, concat_axis=0, tiled=True))
    gated = pl.pallas_call(
        gated_kernel,
        out_shape=jax.ShapeDtypeStruct((parts, rows, features // parts), jnp.bfloat16),
        in_specs=[VM] * 9 + [SM],
        out_specs=VM,
        scratch_shapes=common
        + more,
        compiler_params=limit,
        name="gated",
    )(
        head_input,
        gate_input,
        increment_preactivation.T,
        write_vector,
        read_vector,
        entry,
        bias,
        dlog,
        gain,
        doc_starts,
    )
    gated = to_owners(gated)
    blocks = gated.reshape(devices * groups, GROUP, width)[all_order]
    packed = lax.all_to_all(
        blocks.reshape(devices, rows, width), "ctx", split_axis=0, concat_axis=0, tiled=True
    )
    return pl.pallas_call(
        norm_kernel,
        out_shape=jax.ShapeDtypeStruct((rows, features), jnp.bfloat16),
        in_specs=[VM] * 2,
        out_specs=VM,
        compiler_params=limit,
        name="norm",
    )(joined(packed), norm_weight.reshape(1, -1))


def solution(mesh):
    return jax.shard_map(
        local,
        mesh=mesh,
        in_specs=(
            P(("dp", "ctx"), None),
            P(("dp", "ctx"), None),
            P(("dp", "ctx"), None),
            P(("dp", "ctx"), None),
            P(("dp", "ctx"), None),
            P(),
            P(),
            P(),
            P(),
            P(("dp", "ctx")),
            P(("dp", "ctx")),
        ),
        out_specs=P(("dp", "ctx"), None),
        check_vma=False,
    )
```

```python
import functools

import jax
import jax.numpy as jnp
from jax import lax
from jax.experimental import pallas as pl
from jax.experimental.pallas import tpu as pltpu
from jax.sharding import PartitionSpec as P

HEAD_DIM = 64
GROUP = 128
CHUNK = 8
WIDE = CHUNK * HEAD_DIM
EXTRA = 16
PARTS = 4
LIMIT = 61 * 1024 * 1024
UNIT = 128

highest = lax.Precision.HIGHEST
VM = pl.BlockSpec(memory_space=pltpu.VMEM)
SM = pl.BlockSpec(memory_space=pltpu.SMEM)
ANY = pl.BlockSpec(memory_space=pltpu.HBM)


def transposed(v):
    rows, cols = v.shape
    if cols < 128:
        v = jnp.concatenate([v, jnp.zeros((rows, 128 - cols), v.dtype)], axis=1)
    return v.T[:cols]


def upright(v):
    rows, cols = v.shape
    if rows < 128:
        v = jnp.concatenate([v, jnp.zeros((128 - rows, cols), v.dtype)], axis=0)
    return v.T[:, :rows]


def lower_mask():
    row = lax.broadcasted_iota(jnp.int32, (GROUP, GROUP), 0)
    col = lax.broadcasted_iota(jnp.int32, (GROUP, GROUP), 1)
    return row >= col


def step_terms(logit_ref, bias_ref, dlog_ref):
    raw = logit_ref[...].astype(jnp.float32)
    raw = jnp.concatenate([upright(raw[:, k : k + GROUP]) for k in range(0, raw.shape[1], GROUP)], axis=0)
    v = raw + bias_ref[...]
    dt = jnp.maximum(v, 0.0) + jnp.log(1.0 + jnp.exp(-jnp.abs(v)))
    return dt, -dt * jnp.exp(dlog_ref[...])


def spread(v):
    rows = v.shape[0]
    first = lax.broadcasted_iota(jnp.int32, (rows, 128), 1) < HEAD_DIM
    return jnp.concatenate(
        [
            jnp.where(first, v[:, k : k + 1], v[:, k + 1 : k + 2])
            for k in range(0, CHUNK, 2)
        ],
        axis=1,
    )


def scatter(dt, cums, cum_s, dt_s, some):
    for g in range(len(cums)):
        rows = slice(g * GROUP, (g + 1) * GROUP)
        for c in some:
            cum_s[g, c] = cums[g][:, c * CHUNK : (c + 1) * CHUNK]
            dt_s[g, c] = dt[rows, c * CHUNK : (c + 1) * CHUNK]


def prepare(logit_ref, bias_ref, dlog_ref, write_ref, cum_s, dt_s, write_t, some=None):
    heads = bias_ref.shape[1]
    dt, fall = step_terms(logit_ref, bias_ref, dlog_ref)
    tri = lower_mask().astype(jnp.float32)
    cums = []
    for g in range(write_t.shape[0]):
        rows = slice(g * GROUP, (g + 1) * GROUP)
        cum = jnp.dot(tri, fall[rows], precision=highest, preferred_element_type=jnp.float32)
        cums.append(cum)
        write_t[g] = write_ref[rows, :].astype(jnp.float32).T.astype(jnp.bfloat16)
    scatter(dt, cums, cum_s, dt_s, range(heads // CHUNK) if some is None else some)
    return dt, cums


def group_state(g, c, x, cum_s, dt_s, write_t):
    cum = cum_s[g, c]
    last = cum[GROUP - 1 : GROUP]
    tail = jnp.exp(last - cum) * dt_s[g, c]
    scaled = (x.astype(jnp.float32) * spread(tail)).astype(jnp.bfloat16)
    state = jnp.dot(write_t[g], scaled, preferred_element_type=jnp.float32)
    return state, spread(jnp.exp(last))


def state_kernel(
    x_ref, logit_ref, write_ref, bias_ref, dlog_ref, starts_ref, order_ref, out_ref, cum_s, dt_s, write_t
):
    groups = write_t.shape[0]
    prepare(logit_ref, bias_ref, dlog_ref, write_ref, cum_s, dt_s, write_t)
    parts, _, width = out_ref.shape
    chunks = cum_s.shape[1]
    per = width // WIDE

    def one(c, carry):
        cols = pl.ds(pl.multiple_of(c * WIDE, WIDE), WIDE)
        total, decay = None, None
        for g in range(groups):
            x = x_ref[g * GROUP : (g + 1) * GROUP, cols]
            state, last = group_state(g, c, x, cum_s, dt_s, write_t)
            keep = 1.0 - starts_ref[g].astype(jnp.float32)
            factor = keep * last
            total = state if total is None else factor * total + state
            decay = factor if decay is None else factor * decay
        coarse = decay.astype(jnp.bfloat16)
        fine = (decay - coarse.astype(jnp.float32)).astype(jnp.bfloat16)
        row = lax.broadcasted_iota(jnp.int32, (EXTRA, WIDE), 0)
        lane = lax.broadcasted_iota(jnp.int32, (EXTRA, WIDE), 1)
        order = jnp.zeros((EXTRA, WIDE), jnp.float32)
        for g in range(groups):
            order = jnp.where(lane == g, order_ref[g].astype(jnp.float32), order)
        extra = jnp.where(
            row == 0,
            coarse.astype(jnp.float32),
            jnp.where(row == 1, fine.astype(jnp.float32), order),
        )
        full = jnp.concatenate([total, extra], axis=0).astype(jnp.bfloat16)
        if parts == 1:
            out_ref[0, :, cols] = full
        else:
            into = pl.ds(pl.multiple_of((c % per) * WIDE, WIDE), WIDE)
            out_ref[c // per, :, into] = full
        return carry

    lax.fori_loop(0, chunks, one, 0)


def scan_kernel(in_ref, out_ref):
    parts, _, width = in_ref.shape
    state = jnp.zeros((GROUP, width), jnp.float32)
    for s in range(parts):
        out_ref[s] = state.astype(jnp.bfloat16)
        extra = in_ref[s, GROUP : GROUP + EXTRA, :].astype(jnp.float32)
        decay = extra[0:1] + extra[1:2]
        state = decay * state + in_ref[s, :GROUP, :].astype(jnp.float32)


def gated_setup(
    logit_ref, bias_ref, dlog_ref, write_ref, read_ref, gain_ref, cum_s, dt_s, write_t, cum_t, dt_t, gain_s, score_s
):
    dt, cums = prepare(logit_ref, bias_ref, dlog_ref, write_ref, cum_s, dt_s, write_t)
    score_setup(dt, cums, read_ref, gain_ref, cum_s, write_t, cum_t, dt_t, gain_s, score_s)


def score_setup(dt, cums, read_ref, gain_ref, cum_s, write_t, cum_t, dt_t, gain_s, score_s):
    groups, chunks = cum_s.shape[:2]
    mask = lower_mask()
    for g in range(groups):
        rows = slice(g * GROUP, (g + 1) * GROUP)
        ct = transposed(cums[g])
        dtt = transposed(dt[rows])
        for c in range(chunks):
            cum_t[g, c] = ct[c * CHUNK : (c + 1) * CHUNK]
            dt_t[g, c] = dtt[c * CHUNK : (c + 1) * CHUNK]
        score = jnp.dot(read_ref[rows, :], write_t[g], preferred_element_type=jnp.float32)
        score_s[g] = jnp.where(mask, score, 0.0)
    for c in range(chunks):
        gain_s[c] = jnp.broadcast_to(gain_ref[:, c * CHUNK : (c + 1) * CHUNK], (8, CHUNK))


def gated_chunk(
    c, state, put, x_ref, gate_ref, read_ref, starts_ref, cum_s, dt_s, write_t, cum_t, dt_t, gain_s, score_s
):
    groups = cum_s.shape[0]
    first = lax.broadcasted_iota(jnp.int32, (GROUP, 128), 1) < HEAD_DIM
    cols = pl.ds(pl.multiple_of(c * WIDE, WIDE), WIDE)
    gain = spread(gain_s[c][0:1])
    for g in range(groups):
        rows = slice(g * GROUP, (g + 1) * GROUP)
        x = x_ref[rows, cols]
        keep = 1.0 - starts_ref[g].astype(jnp.float32)
        entering = (keep * state).astype(jnp.bfloat16)
        cum = cum_s[g, c]
        carried = jnp.dot(read_ref[rows, :], entering, preferred_element_type=jnp.float32)
        mixed = carried * spread(jnp.exp(cum)) + gain * x.astype(jnp.float32)
        score = score_s[g]
        ct, dtt = cum_t[g, c], dt_t[g, c]
        pieces = []
        for k in range(0, CHUNK, 2):
            pair = x[:, k * HEAD_DIM : (k + 2) * HEAD_DIM]
            both = []
            for h in (k, k + 1):
                gap = cum[:, h : h + 1] - ct[h : h + 1]
                weight = score * jnp.exp(jnp.minimum(gap, 0.0)) * dtt[h : h + 1]
                both.append(
                    jnp.dot(weight.astype(jnp.bfloat16), pair, preferred_element_type=jnp.float32)
                )
            pieces.append(jnp.where(first, both[0], both[1]))
        mixed = mixed + jnp.concatenate(pieces, axis=1)
        gate = gate_ref[rows, cols].astype(jnp.float32)
        put(g, (mixed * (gate / (1.0 + jnp.exp(-gate)))).astype(jnp.bfloat16))
        if g + 1 < groups:
            own, last = group_state(g, c, x, cum_s, dt_s, write_t)
            state = keep * last * state + own


def gated_kernel(
    x_ref,
    gate_ref,
    logit_ref,
    write_ref,
    read_ref,
    entry_ref,
    bias_ref,
    dlog_ref,
    gain_ref,
    starts_ref,
    out_ref,
    *scratch,
):
    gated_setup(logit_ref, bias_ref, dlog_ref, write_ref, read_ref, gain_ref, *scratch)
    parts, _, width = out_ref.shape
    chunks = scratch[0].shape[1]
    per = width // WIDE

    def one(c, carry):
        cols = pl.ds(pl.multiple_of(c * WIDE, WIDE), WIDE)
        into = pl.ds(pl.multiple_of((c % per) * WIDE, WIDE), WIDE)
        if parts == 1:
            state = entry_ref[0, :, cols].astype(jnp.float32)
        else:
            state = entry_ref[c // per, :, into].astype(jnp.float32)

        def put(g, value):
            rows = slice(g * GROUP, (g + 1) * GROUP)
            if parts == 1:
                out_ref[0, rows, cols] = value
            else:
                out_ref[c // per, rows, into] = value

        gated_chunk(c, state, put, x_ref, gate_ref, read_ref, starts_ref, *scratch)
        return carry

    lax.fori_loop(0, chunks, one, 0)


def fused_kernel(
    n,
    parts,
    x_hbm,
    gate_hbm,
    logit_hbm,
    write_hbm,
    read_hbm,
    bias_hbm,
    dlog_hbm,
    gain_hbm,
    starts_hbm,
    order_hbm,
    out_ref,
    squares,
    logit_ref,
    write_ref,
    read_ref,
    bias_ref,
    dlog_ref,
    gain_ref,
    starts_ref,
    order_ref,
    small_sem,
    x_ref,
    gate_ref,
    pair_out,
    pair_in,
    fade_out,
    fade_in,
    fade_s,
    total_s,
    decay_s,
    e_in,
    f_out,
    back,
    near_entry,
    far_entry,
    made,
    stage,
    final,
    order_own,
    order_all,
    order_s,
    load_sem,
    link_recv,
    give_recv,
    link_send,
    fade_send,
    fade_recv,
    send1,
    recv1,
    send2,
    recv2,
    send3,
    recv3,
    order_sem,
    gate_sem,
    ready_sem,
    side_sem,
    *rest,
):
    got, scratch = rest[:parts], rest[parts:]
    cum_s, dt_s, write_t = scratch[:3]
    groups, chunks = cum_s.shape[:2]
    piece = stage.shape[-1]
    per = WIDE // piece
    units = WIDE // UNIT
    span = 2 * WIDE
    me = lax.axis_index("ctx")
    side = me % 2
    level = me // 2
    levels = n // 2
    half = n // 2
    buddy = me + 1 - 2 * side
    low = level < levels // 2

    def send(source, target, sends, recvs, there):
        return pltpu.make_async_remote_copy(
            src_ref=source,
            dst_ref=target,
            send_sem=sends,
            recv_sem=recvs,
            device_id={"ctx": there},
            device_id_type=pl.DeviceIdType.MESH,
        )

    def landed(ref, sem):
        send(ref, ref, sem, sem, buddy).wait_recv()

    def left(ref, sem):
        send(ref, ref, sem, sem, buddy).wait_send()

    def load(j):
        cols = pl.ds(j * span, span)
        return pltpu.make_async_copy(x_hbm.at[:, cols], x_ref.at[:, cols], load_sem.at[j])

    def pair(r):
        return send(pair_out.at[r], pair_in.at[r], link_send.at[0], link_recv.at[0, r], buddy)

    def chain(r):
        return send(f_out.at[r], e_in.at[r], link_send.at[1], link_recv.at[1, r], lax.rem(me + 2, n))

    def give(r):
        return send(back.at[r], far_entry.at[r], link_send.at[2], give_recv.at[r // units], buddy)

    def fade():
        return send(fade_out, fade_in, fade_send, fade_recv, buddy)

    def first(there, j):
        far = ((there < half) != low).astype(jnp.int32)
        return send(
            made.at[there, j], got[j].at[pl.ds(me * groups, groups)], send1.at[far], recv1.at[j], there
        )

    def second(there, j):
        return send(stage.at[there, j], final.at[me, j], send2, recv2.at[j], there)

    barrier = pltpu.get_barrier_semaphore()

    def tell(sem, there):
        pl.semaphore_signal(sem, inc=1, device_id={"ctx": there}, device_id_type=pl.DeviceIdType.MESH)

    above = level < levels - 1
    below = level > 0
    tell(barrier, buddy)

    @pl.when(above)
    def _():
        tell(barrier, lax.rem(me + 2, n))

    @pl.when(below)
    def _():
        tell(barrier, lax.rem(me + n - 2, n))

    small = [
        pltpu.make_async_copy(source, target, small_sem.at[k])
        for k, (source, target) in enumerate(
            (
                (logit_hbm, logit_ref),
                (bias_hbm, bias_ref),
                (dlog_hbm, dlog_ref),
                (write_hbm, write_ref),
                (starts_hbm, starts_ref),
                (read_hbm, read_ref),
                (gain_hbm, gain_ref),
                (order_hbm, order_ref),
            )
        )
    ]
    for copy in small[:5]:
        copy.start()
    load(0).start()
    for copy in small[5:]:
        copy.start()
    for copy in small[:4]:
        copy.wait()
    for j in range(1, parts):
        load(j).start()
    gate_load = pltpu.make_async_copy(gate_hbm, gate_ref, load_sem.at[parts])
    gate_load.start()

    def send_orders():
        for off in range(1, n):
            there = lax.rem(me + off, n)
            send(order_own, order_all.at[me], send3, recv3, there).start()

    with jax.named_scope("setup"):
        dt, cums = prepare(logit_ref, bias_ref, dlog_ref, write_ref, cum_s, dt_s, write_t, range(2))
        heads = bias_ref.shape[1]
        small[4].wait()
        whole = None
        for g in range(groups):
            factor = (1.0 - starts_ref[g].astype(jnp.float32)) * jnp.exp(cums[g][GROUP - 1 : GROUP])
            whole = factor if whole is None else whole * factor
        whole = jnp.concatenate([whole, jnp.zeros((1, 128 - heads), jnp.float32)], axis=1)
        fade_out[...] = whole

    @pl.when(level == 0)
    def _():
        e_in[...] = jnp.zeros_like(e_in)

    @pl.when(me == 0)
    def _():
        near_entry[...] = jnp.zeros_like(near_entry)
        far_entry[...] = jnp.zeros_like(far_entry)

    def ends(c, carry):
        cols = pl.ds(pl.multiple_of(c * WIDE, WIDE), WIDE)
        total, decay = None, None
        for g in range(groups):
            x = x_ref[g * GROUP : (g + 1) * GROUP, cols]
            state, last = group_state(g, c, x, cum_s, dt_s, write_t)
            factor = (1.0 - starts_ref[g].astype(jnp.float32)) * last
            total = state if total is None else factor * total + state
            decay = factor if decay is None else factor * decay
        base = c // 2 * units

        @pl.when(c % 2 == side)
        def _():
            for u in range(units):
                cut = slice(u * UNIT, (u + 1) * UNIT)
                total_s[base + u] = total[:, cut]
                decay_s[base + u] = jnp.broadcast_to(decay[:, cut], (8, UNIT))

        @pl.when(c % 2 != side)
        def _():
            for u in range(units):
                pair_out[base + u] = total[:, u * UNIT : (u + 1) * UNIT].astype(jnp.bfloat16)

        return carry

    def relay(r, carry):
        pair(r).wait_recv()

        @pl.when(level > 0)
        def _():
            chain(r).wait_recv()

        state = e_in[r].astype(jnp.float32)
        their = pair_in[r].astype(jnp.float32)
        theirs = fade_s[r][0:1]
        total, decay = total_s[r], decay_s[r][0:1]
        early = side == 0
        middle = jnp.where(early, decay, theirs) * state + jnp.where(early, total, their)

        @pl.when(level < levels - 1)
        def _():
            end = jnp.where(early, theirs, decay) * middle + jnp.where(early, their, total)
            f_out[r] = end.astype(jnp.bfloat16)
            chain(r).start()

        @pl.when(me != 1)
        def _():
            back[r] = jnp.where(early, middle, state).astype(jnp.bfloat16)
            give(r).start()

        near_entry[r] = jnp.where(early, state, middle).astype(jnp.bfloat16)
        return carry

    def links(j):
        with jax.named_scope("links"):
            lax.fori_loop(j * units, (j + 1) * units, relay, 0)

    def offer(j):
        for u in range(units):
            pair(j * units + u).start()

    def hear_above():
        with jax.named_scope("ready"):
            pl.semaphore_wait(ready_sem, 1)

    def swap_half(j):
        with jax.named_scope("ends"):
            ends(2 * j + 1 - side, 0)
        if j == 0:
            with jax.named_scope("barrier"):
                pl.semaphore_wait(barrier, 1 + above.astype(jnp.int32) + below.astype(jnp.int32))
            fade().start()
        offer(j)

    def keep_half(j):
        with jax.named_scope("ends"):
            ends(2 * j + side, 0)

    def by_distance(k):
        return jnp.where(low, levels - 1 - k, k)

    def compute(j, i, entry):
        def put(g, value):
            for p in range(per):
                made[2 * p + i, j, g] = value[:, p * piece : (p + 1) * piece]

        with jax.named_scope("gated"):
            state = jnp.concatenate([entry[j * units + u].astype(jnp.float32) for u in range(units)], axis=1)
            gated_chunk(2 * j + i, state, put, x_ref, gate_ref, read_ref, starts_ref, *scratch)

    def outward(j, there, wanted):
        for s in range(parts):

            @pl.when(jnp.logical_and(j == s, jnp.logical_and(there != me, wanted)))
            def _():
                first(there, s).start()

    bottom = jnp.logical_and(level == 0, levels > 2)

    def open_early():
        gate_load.wait()
        compute(0, side, near_entry)
        hear_above()
        for k in range(per):
            outward(0, 2 * k + side, k >= levels // 2)

    late = parts - 1
    for j in range(late):
        load(j).wait()
        swap_half(j)
        if j == 0:

            @pl.when(jnp.logical_and(below, level == levels - 2))
            def _():
                tell(ready_sem, me - 2)

            with jax.named_scope("scores"):
                for copy in small[5:]:
                    copy.wait()
                lane = lax.broadcasted_iota(jnp.int32, order_own.shape, 1)
                held = jnp.zeros(order_own.shape, jnp.int32)
                for g in range(groups):
                    held = jnp.where(lane == g, order_ref[g], held)
                order_own[...] = held
                order_all[me] = held
                scatter(dt, cums, cum_s, dt_s, range(2, chunks))
                score_setup(dt, cums, read_ref, gain_ref, cum_s, write_t, *scratch[3:])

            @pl.when(jnp.logical_and(below, level < levels - 2))
            def _():
                hear_above()
                tell(ready_sem, me - 2)

            @pl.when(jnp.logical_and(bottom, me == 0))
            def _():
                open_early()

        if j == 1:
            keep_half(0)
            keep_half(1)
    fade().wait_recv()
    tile = fade_in[0:1, :]
    for c in range(chunks):

        @pl.when(c % 2 == side)
        def _(c=c):
            lanes = spread(tile[:, c * CHUNK : (c + 1) * CHUNK])
            for u in range(units):
                fade_s[c // 2 * units + u] = jnp.broadcast_to(lanes[:, u * UNIT : (u + 1) * UNIT], (8, UNIT))

    @pl.when(low)
    def _():
        links(0)

    @pl.when(jnp.logical_and(bottom, me > 0))
    def _():
        open_early()

    load(late).wait()
    swap_half(late)
    for j in range(2, parts):
        keep_half(j)

    @pl.when(low)
    def _():
        with jax.named_scope("linksall"):
            lax.fori_loop(units, parts * units, relay, 0)

        tell(side_sem, buddy)


    def near_column(j, carry):
        @pl.when(jnp.logical_not(low))
        def _():
            links(j)

        begun = jnp.logical_and(bottom, j == 0)

        @pl.when(jnp.logical_not(begun))
        def _():
            @pl.when(j == 0)
            def _():
                gate_load.wait()

            compute(j, side, near_entry)

        for k in range(per):
            there = 2 * by_distance(k) + side
            high = there // 2
            fresh = jnp.logical_not(jnp.logical_and(begun, high >= levels // 2))
            outward(j, there, jnp.logical_and(fresh, jnp.logical_or(low, high < level)))
        for s in range(parts):

            @pl.when(j == s)
            def _():
                for g in range(groups):
                    got[s][me * groups + g] = made[me, s, g]

        return carry

    def postponed(j, carry):
        for k in range(per):
            outward(j, 2 * k + side, jnp.logical_not(jnp.logical_or(low, k < level)))
        return carry

    def far_column(j, carry):
        @pl.when(me > 0)
        def _():
            with jax.named_scope("waitgive"):
                landed(far_entry.at[pl.ds(j * units, units)], give_recv.at[j])

        @pl.when(jnp.logical_and(j == 0, jnp.logical_not(low)))
        def _():
            send_orders()

        compute(j, 1 - side, far_entry)
        for k in range(per):
            outward(j, 2 * by_distance(k) + 1 - side, True)
        return carry

    lax.fori_loop(0, parts, near_column, 0)
    lax.fori_loop(0, parts, postponed, 0)

    @pl.when(low)
    def _():
        pl.semaphore_wait(side_sem, 1)
        send_orders()

    lax.fori_loop(0, parts, far_column, 0)

    lower_inner = jnp.logical_and(level == levels // 2 - 1, level > 0)
    upper_inner = jnp.logical_and(level == levels // 2, level < levels - 1)
    inner = jnp.logical_or(lower_inner, upper_inner)

    def crossed():
        with jax.named_scope("crossed"):
            left(made.at[pl.ds(0, half)], send1.at[1])
        tell(gate_sem, jnp.where(low, me - 2, lax.rem(me + 2, n)))

    landed(order_all.at[pl.ds(0, n - 1)], recv3)
    fetch = pltpu.make_async_copy(order_all, order_s, order_sem)
    fetch.start()
    fetch.wait()

    @pl.when(upper_inner)
    def _():
        crossed()

    if levels > 2:

        @pl.when(jnp.logical_or(level == levels // 2 - 2, level == levels // 2 + 1))
        def _():
            with jax.named_scope("gate"):
                pl.semaphore_wait(gate_sem, 1)

    for j in range(parts):
        with jax.named_scope("waitfirst"):
            landed(got[j].at[pl.ds(0, (n - 1) * groups)], recv1.at[j])

        def pick(k, carry, j=j):
            there = 2 * by_distance(k // 2) + lax.rem(k + 1 + me, 2)

            @pl.when(there != me)
            def _():
                for g in range(groups):
                    stage[there, j, g] = got[j][order_s[there, 0, g]]
                second(there, j).start()

            @pl.when(there == me)
            def _():
                for g in range(groups):
                    final[me, j, g] = got[j][order_s[me, 0, g]]

            return carry

        with jax.named_scope("pick"):
            lax.fori_loop(0, n, pick, 0)
        if j == parts - 2:

            @pl.when(lower_inner)
            def _():
                crossed()

    tile = 32
    for j in range(parts):
        with jax.named_scope("waitsecond"):
            landed(final.at[pl.ds(0, n - 1), j], recv2.at[j])

        def add(r, carry, j=j):
            for g in range(groups):
                at = pl.ds(pl.multiple_of(r * tile, tile), tile)
                into = pl.ds(pl.multiple_of(g * GROUP + r * tile, tile), tile)
                total = jnp.zeros((tile, 128), jnp.float32) if j == 0 else squares[into, :]
                for s in range(n):
                    raw = final[s, j, g, at, :]
                    start = (2 * j + s % 2) * WIDE + s // 2 * piece
                    out_ref[into, start : start + piece] = raw
                    v = raw.astype(jnp.float32)
                    v = v * v
                    for q in range(0, piece, 128):
                        total = total + v[:, q : q + 128]
                squares[into, :] = total
            return carry

        with jax.named_scope("add"):
            lax.fori_loop(0, GROUP // tile, add, 0)

    with jax.named_scope("sent"):
        left(pair_out, link_send.at[0])
        left(fade_out, fade_send)

        @pl.when(level < levels - 1)
        def _():
            left(f_out, link_send.at[1])

        @pl.when(me != 1)
        def _():
            left(back, link_send.at[2])

        left(order_all.at[pl.ds(0, n - 1)], send3)
        left(made.at[pl.ds(0, half - 1)], send1.at[0])

        @pl.when(jnp.logical_not(inner))
        def _():
            left(made.at[pl.ds(0, half)], send1.at[1])

        left(stage.at[pl.ds(0, n - 1)], send2)


def scale_kernel(in_ref, squares_ref, weight_ref, out_hbm, ready, sem):
    rows, width = in_ref.shape
    tile = rows // sem.shape[0]

    def push(r):
        at = pl.ds(r * tile, tile)
        return pltpu.make_async_copy(ready.at[at, :], out_hbm.at[at, :], sem.at[r])

    for r in range(sem.shape[0]):
        at = slice(r * tile, (r + 1) * tile)
        total = jnp.sum(squares_ref[at, :], axis=1, keepdims=True)
        scale = lax.rsqrt(total * (1.0 / width) + 1e-05)
        for q in range(0, width, WIDE):
            cols = slice(q, q + WIDE)
            v = in_ref[at, cols].astype(jnp.float32)
            ready[at, cols] = (v * scale * weight_ref[:, cols]).astype(jnp.bfloat16)
        push(r).start()
    for r in range(sem.shape[0]):
        push(r).wait()


def norm_kernel(in_ref, weight_ref, out_ref):
    parts, rows, width = in_ref.shape
    tile = 32

    def one(r, carry):
        at = pl.ds(pl.multiple_of(r * tile, tile), tile)
        total = jnp.zeros((tile, 1), jnp.float32)
        for s in range(parts):
            v = in_ref[s, at, :].astype(jnp.float32)
            total = total + jnp.sum(v * v, axis=1, keepdims=True)
        scale = lax.rsqrt(total * (1.0 / (parts * width)) + 1e-05)
        for s in range(parts):
            v = in_ref[s, at, :].astype(jnp.float32)
            w = weight_ref[:, s * width : (s + 1) * width]
            out_ref[at, s * width : (s + 1) * width] = (v * scale * w).astype(jnp.bfloat16)
        return carry

    lax.fori_loop(0, rows // tile, one, 0)


def local(
    head_input,
    gate_input,
    write_vector,
    read_vector,
    increment_preactivation,
    step_bias,
    decay_log,
    skip_gain,
    norm_weight,
    doc_starts,
    block_order,
):
    devices = lax.axis_size("ctx")
    rows, features = head_input.shape
    heads = step_bias.shape[0]
    groups = rows // GROUP
    chunks = heads // CHUNK
    width = features // devices
    state_size = write_vector.shape[1]
    direct = width % WIDE == 0
    parts = devices if direct else 1
    limit = pltpu.CompilerParams(vmem_limit_bytes=48 * 1024 * 1024)
    common = [
        pltpu.VMEM((groups, chunks, GROUP, CHUNK), jnp.float32),
        pltpu.VMEM((groups, chunks, GROUP, CHUNK), jnp.float32),
        pltpu.VMEM((groups, state_size, GROUP), jnp.bfloat16),
    ]
    more = [
        pltpu.VMEM((groups, chunks, CHUNK, GROUP), jnp.float32),
        pltpu.VMEM((groups, chunks, CHUNK, GROUP), jnp.float32),
        pltpu.VMEM((chunks, 8, CHUNK), jnp.float32),
        pltpu.VMEM((groups, GROUP, GROUP), jnp.float32),
    ]
    bias, dlog, gain = (v.reshape(1, -1) for v in (step_bias, decay_log, skip_gain))

    def to_owners(v):
        if not direct:
            v = v.reshape(v.shape[1], devices, width).transpose(1, 0, 2)
        return lax.all_to_all(v, "ctx", split_axis=0, concat_axis=0, tiled=True)

    def joined(v):
        if not direct:
            v = v.transpose(1, 0, 2).reshape(1, v.shape[1], features)
        return v

    piece = width // PARTS
    per = max(WIDE // max(piece, 1), 1)
    if width == 512 and devices == 2 * per and chunks == 2 * PARTS:
        slab = (devices, PARTS, groups, GROUP, piece)
        links = features // UNIT // 2
        state = (links, state_size, UNIT)
        sems = pltpu.SemaphoreType.DMA
        packed, squares = pl.pallas_call(
            functools.partial(fused_kernel, devices, PARTS),
            out_shape=[
                pltpu.VMEM((rows, features), jnp.bfloat16),
                pltpu.VMEM((rows, 128), jnp.float32),
            ],
            in_specs=[ANY] * 10,
            out_specs=[VM] * 2,
            scratch_shapes=[
                pltpu.VMEM((heads, rows), jnp.bfloat16),
                pltpu.VMEM((rows, state_size), jnp.bfloat16),
                pltpu.VMEM((rows, state_size), jnp.bfloat16),
                pltpu.VMEM((1, heads), jnp.float32),
                pltpu.VMEM((1, heads), jnp.float32),
                pltpu.VMEM((1, heads), jnp.float32),
                pltpu.SMEM((groups,), jnp.int32),
                pltpu.SMEM((groups,), jnp.int32),
                sems((8,)),
                pltpu.VMEM((rows, features), jnp.bfloat16),
                pltpu.VMEM((rows, features), jnp.bfloat16),
                pltpu.VMEM(state, jnp.bfloat16),
                pltpu.VMEM(state, jnp.bfloat16),
                pltpu.VMEM((1, 128), jnp.float32),
                pltpu.VMEM((1, 128), jnp.float32),
                pltpu.VMEM((links, 8, UNIT), jnp.float32),
                pltpu.VMEM(state, jnp.float32),
                pltpu.VMEM((links, 8, UNIT), jnp.float32),
            ]
            + [pltpu.VMEM(state, jnp.bfloat16)] * 5
            + [pltpu.VMEM(slab, jnp.bfloat16)] * 3
            + [
                pltpu.VMEM((1, 128), jnp.int32),
                pltpu.VMEM((devices, 1, 128), jnp.int32),
                pltpu.SMEM((devices, 1, 128), jnp.int32),
                sems((PARTS + 1,)),
                sems((2, links)),
                sems((PARTS,)),
                sems((3,)),
                sems,
                sems,
                sems((2,)),
                sems((PARTS,)),
                sems,
                sems((PARTS,)),
                sems,
                sems,
                sems,
            ]
            + [pltpu.SemaphoreType.REGULAR] * 3
            + [pltpu.VMEM((devices * groups, GROUP, piece), jnp.bfloat16)] * PARTS
            + common
            + more,
            compiler_params=pltpu.CompilerParams(
                collective_id=0, has_side_effects=True, vmem_limit_bytes=LIMIT
            ),
            name="fused",
        )(
            head_input,
            gate_input,
            increment_preactivation.T,
            write_vector,
            read_vector,
            bias,
            dlog,
            gain,
            doc_starts,
            block_order,
        )
        return pl.pallas_call(
            scale_kernel,
            out_shape=jax.ShapeDtypeStruct((rows, features), jnp.bfloat16),
            in_specs=[VM] * 3,
            out_specs=ANY,
            scratch_shapes=[pltpu.VMEM((rows, features), jnp.bfloat16), sems((4,))],
            compiler_params=pltpu.CompilerParams(vmem_limit_bytes=8 * 1024 * 1024),
            name="scale",
        )(packed, squares, norm_weight.reshape(1, -1))

    ends = pl.pallas_call(
        state_kernel,
        out_shape=jax.ShapeDtypeStruct((parts, state_size + EXTRA, features // parts), jnp.bfloat16),
        in_specs=[VM] * 5 + [SM] * 2,
        out_specs=VM,
        scratch_shapes=common,
        compiler_params=limit,
        name="end_states",
    )(head_input, increment_preactivation.T, write_vector, bias, dlog, doc_starts, block_order)
    ends = to_owners(ends)
    all_order = ends[:, state_size + 2, :groups].astype(jnp.int32).reshape(-1)
    entry = pl.pallas_call(
        scan_kernel,
        out_shape=jax.ShapeDtypeStruct((devices, state_size, width), jnp.bfloat16),
        in_specs=[VM],
        out_specs=VM,
        compiler_params=limit,
        name="scan_states",
    )(ends)
    entry = joined(lax.all_to_all(entry, "ctx", split_axis=0, concat_axis=0, tiled=True))
    gated = pl.pallas_call(
        gated_kernel,
        out_shape=jax.ShapeDtypeStruct((parts, rows, features // parts), jnp.bfloat16),
        in_specs=[VM] * 9 + [SM],
        out_specs=VM,
        scratch_shapes=common
        + more,
        compiler_params=limit,
        name="gated",
    )(
        head_input,
        gate_input,
        increment_preactivation.T,
        write_vector,
        read_vector,
        entry,
        bias,
        dlog,
        gain,
        doc_starts,
    )
    gated = to_owners(gated)
    blocks = gated.reshape(devices * groups, GROUP, width)[all_order]
    packed = lax.all_to_all(
        blocks.reshape(devices, rows, width), "ctx", split_axis=0, concat_axis=0, tiled=True
    )
    return pl.pallas_call(
        norm_kernel,
        out_shape=jax.ShapeDtypeStruct((rows, features), jnp.bfloat16),
        in_specs=[VM] * 2,
        out_specs=VM,
        compiler_params=limit,
        name="norm",
    )(joined(packed), norm_weight.reshape(1, -1))


def solution(mesh):
    return jax.shard_map(
        local,
        mesh=mesh,
        in_specs=(
            P(("dp", "ctx"), None),
            P(("dp", "ctx"), None),
            P(("dp", "ctx"), None),
            P(("dp", "ctx"), None),
            P(("dp", "ctx"), None),
            P(),
            P(),
            P(),
            P(),
            P(("dp", "ctx")),
            P(("dp", "ctx")),
        ),
        out_specs=P(("dp", "ctx"), None),
        check_vma=False,
    )
```
